32 devices in a mesh: dp: 16 (over z, y, core), tensor: 2 (over x).
Axes of the slice: x: 2, y: 2, z: 4, core: 2. Of those that a mesh axis runs over, the one named last changes fastest.
Arguments:
- layer_input: bfloat16 [8192, 2048], P(('dp', 'tensor')), may hold values from -6 to 6
- teacher: bfloat16 [8192, 2048], P(('dp', 'tensor')), may hold values from -6 to 6
- lengths: int32 [16], replicated, may hold values from 32 to 512, as said below
- seq_order: int32 [16], replicated, may hold values from 0 to 15, as said below
- gain_attn: bfloat16 [2048], P('dp'), may hold values from 0.5 to 1.5
- w_query: bfloat16 [2048, 2048], P('dp', 'tensor'), may hold values from -0.25 to 0.25
- key_projection_weight: bfloat16 [2048, 1024], P('dp', 'tensor'), may hold values from -0.125 to 0.125
- value_projection_weight: bfloat16 [2048, 1024], P('dp', 'tensor'), may hold values from -0.125 to 0.125
- w_out: bfloat16 [2048, 2048], P('tensor', 'dp'), may hold values from -0.375 to 0.375
- gain_mlp: bfloat16 [2048], P('dp'), may hold values from 0.5 to 1.5
- w_gate: bfloat16 [2048, 8192], P('dp', 'tensor'), may hold values from -0.125 to 0.125
- w_up: bfloat16 [2048, 8192], P('dp', 'tensor'), may hold values from -0.125 to 0.125
- w_down: bfloat16 [8192, 2048], P('tensor', 'dp'), may hold values from -0.0625 to 0.0625
Outputs:
- activations: bfloat16 [8192, 2048], P(('dp', 'tensor'))
- input_grad: bfloat16 [8192, 2048], P(('dp', 'tensor'))
- gain_attn_grad: float32 [2048], P('dp')
- w_query_grad: float32 [2048, 2048], P('dp', 'tensor')
- w_key_grad: float32 [2048, 1024], P('dp', 'tensor')
- w_value_grad: float32 [2048, 1024], P('dp', 'tensor')
- w_out_grad: float32 [2048, 2048], P('tensor', 'dp')
- gain_mlp_grad: float32 [2048], P('dp')
- w_gate_grad: float32 [2048, 8192], P('dp', 'tensor')
- w_up_grad: float32 [2048, 8192], P('dp', 'tensor')
- w_down_grad: float32 [8192, 2048], P('tensor', 'dp')
- distill_loss: float32 [], replicated
The draws below stay inside these ranges and needn't reach their ends.
Inputs may be any that keep to these rules, and one draw needn't show every extreme that they name: `lengths`: both ends are reached. `seq_order`: each number appears once.
All inputs are finite; a program needn't handle non-finite values.
Results may differ from the reference program's by a relative error of at most 0.014.
The reference program's roundings to bfloat16 on the way count: a program that leaves them out, or rounds other values in their place, can miss the bound.
Values may be sent and summed in bfloat16 or wider, within the bound.
No kernel may reach another device: no remote copies, remote signals or barrier semaphores. Data moves between devices by JAX's collectives and lax.ppermute only.
A program may use at most 256 MiB of HBM per device.

```python
import jax
import jax.numpy as jnp
from jax import lax

MODEL_WIDTH = 2048
QUERY_HEADS = 8
KEY_VALUE_HEADS = 4
HEAD_SIZE = 256
FF = 8192
GRP = 512
LMIN = 32
TOKENS = 8192
SEQS = 16


def draw_lengths(key, part):
    cut_key = jax.random.fold_in(key, 101)
    groups = SEQS
    index = jnp.arange(groups, dtype=jnp.int32)
    total = GRP * (groups - 1 + 2 * index) // (3 * (groups - 1))
    cut = jax.random.randint(cut_key, (groups,), 0, GRP // 8 + 1)
    length = jnp.maximum(total - cut, LMIN)
    length = jnp.where(index == groups - 1, GRP, length)
    length = jnp.where(index == 0, LMIN, length)
    return length.astype(jnp.int32)


def draw_seq_order(key, part):
    order_key = jax.random.fold_in(key, 202)
    return jax.random.permutation(order_key, SEQS).astype(jnp.int32)


def level_of(stream_key, extent, cuts, low, high):
    factor_of, own = 1.0, jax.random.fold_in(stream_key, 6)
    for dim, parts in cuts:
        draws = jnp.exp(jax.random.uniform(jax.random.fold_in(own, dim), (parts,), jnp.float32, low / len(cuts), high / len(cuts)))
        factor_of = factor_of * jnp.repeat(draws, extent[dim] // parts).reshape([-1 if axis == dim else 1 for axis in range(len(extent))])
    return factor_of


def normal_values(own_key, dims, scale, bound, shards=(), kind=jnp.bfloat16):
    factor_of = level_of(own_key, dims, shards, -0.22, 0.18) if shards else 1.0
    drawn = jax.random.normal(own_key, dims, jnp.float32) * scale * factor_of
    return jnp.minimum(jnp.maximum(drawn, -bound), bound).astype(kind)


def setup_inputs(seed: int = 0) -> dict:
    splits = jax.random.split(jax.random.key(seed), 14)
    return {
        "layer_input": normal_values(splits[0], (TOKENS, MODEL_WIDTH), 1.0, 6.0, ((0, 32),)),
        "teacher": normal_values(splits[1], (TOKENS, MODEL_WIDTH), 1.0, 6.0, ((0, 32),)),
        "lengths": draw_lengths(jax.random.fold_in(splits[13], 71), 0),
        "seq_order": draw_seq_order(jax.random.fold_in(splits[13], 71), 0),
        "gain_attn": jnp.clip(1.0 + 0.1 * jax.random.normal(splits[4], (MODEL_WIDTH,), jnp.float32), 0.5, 1.5).astype(jnp.bfloat16),
        "w_query": normal_values(splits[5], (MODEL_WIDTH, QUERY_HEADS * HEAD_SIZE), (MODEL_WIDTH // 4) ** -0.5, 0.25, ((0, 16), (1, 2))),
        "key_projection_weight": normal_values(splits[6], (MODEL_WIDTH, KEY_VALUE_HEADS * HEAD_SIZE), MODEL_WIDTH ** -0.5, 0.125, ((0, 16), (1, 2))),
        "value_projection_weight": normal_values(splits[7], (MODEL_WIDTH, KEY_VALUE_HEADS * HEAD_SIZE), MODEL_WIDTH ** -0.5, 0.125, ((0, 16), (1, 2))),
        "w_out": normal_values(splits[8], (QUERY_HEADS * HEAD_SIZE, MODEL_WIDTH), (QUERY_HEADS * HEAD_SIZE // 8) ** -0.5, 0.375, ((0, 2), (1, 16))),
        "gain_mlp": jnp.clip(1.0 + 0.1 * jax.random.normal(splits[9], (MODEL_WIDTH,), jnp.float32), 0.5, 1.5).astype(jnp.bfloat16),
        "w_gate": normal_values(splits[10], (MODEL_WIDTH, FF), MODEL_WIDTH ** -0.5, 0.125, ((0, 16), (1, 2))),
        "w_up": normal_values(splits[11], (MODEL_WIDTH, FF), MODEL_WIDTH ** -0.5, 0.125, ((0, 16), (1, 2))),
        "w_down": normal_values(splits[12], (FF, MODEL_WIDTH), FF ** -0.5, 0.0625, ((0, 2), (1, 16))),
    }


@jax.custom_vjp
def reduced_precision(v):
    return lax.optimization_barrier(v.astype(jnp.bfloat16)).astype(jnp.float32)

@jax.custom_vjp
def reduced_precision_backward(v):
    return v

def low_keep(v):
    return (reduced_precision(v), None)

def low_pass(kept, grad):
    return (grad,)

def back_keep(v):
    return (v, None)

def back_low(kept, grad):
    return (reduced_precision(grad),)
reduced_precision.defvjp(low_keep, low_pass)
reduced_precision_backward.defvjp(back_keep, back_low)
EPS = 1e-06
ROPE_BASE = 1000042.0
HIGH = lax.Precision.HIGHEST

def matrix_product(left, right):
    return jnp.dot(left, right, precision=HIGH)

def rms_scale(value_rows):
    return lax.rsqrt(lax.optimization_barrier(jnp.mean(value_rows * value_rows, axis=-1, keepdims=True)) + EPS)

def rope_tables(position, width):
    half = width // 2
    exponent = jnp.arange(half, dtype=jnp.float32) * (-2.0 / width)
    frequency = jnp.exp(exponent * jnp.log(jnp.float32(ROPE_BASE)))
    angle = position.astype(jnp.float32)[:, None] * frequency[None, :]
    return (jnp.cos(angle), jnp.sin(angle))

def apply_rotary(heads, cosine_table, sine_table):
    half = heads.shape[-1] // 2
    first = heads[..., :half]
    second = heads[..., half:]
    cos_b = cosine_table[:, None, :]
    sin_b = sine_table[:, None, :]
    return jnp.concatenate([first * cos_b - second * sin_b, second * cos_b + first * sin_b], axis=-1)

def layout_of(length, slots):
    place = jnp.arange(slots, dtype=jnp.int32)
    inside = place < length
    sequence = jnp.where(inside, 0, 1 + place).astype(jnp.int32)
    position = jnp.where(inside, place, 0).astype(jnp.int32)
    return (sequence, position, inside)

def block(inputs, sequence, position, params):
    gain_a, query_w, key_matrix, value_matrix, out_w, gain_m, gate_w, up_w, down_w = params
    token_rows = inputs.shape[0]
    group_portion = QUERY_HEADS // KEY_VALUE_HEADS
    normalized_rows = reduced_precision(inputs * rms_scale(inputs) * gain_a)
    query_rows = reduced_precision_backward(matrix_product(normalized_rows, query_w)).reshape(token_rows, QUERY_HEADS, HEAD_SIZE)
    key_rows = reduced_precision_backward(matrix_product(normalized_rows, key_matrix)).reshape(token_rows, KEY_VALUE_HEADS, HEAD_SIZE)
    value_rows = reduced_precision(reduced_precision_backward(matrix_product(normalized_rows, value_matrix))).reshape(token_rows, KEY_VALUE_HEADS, HEAD_SIZE)
    cosine_table, sine_table = rope_tables(position, HEAD_SIZE)
    rotated_queries = reduced_precision(apply_rotary(query_rows, cosine_table, sine_table)).reshape(token_rows, KEY_VALUE_HEADS, group_portion, HEAD_SIZE)
    krot = reduced_precision(apply_rotary(key_rows, cosine_table, sine_table))
    raw = jnp.einsum('ikgd,jkd->kgij', rotated_queries, krot, precision=HIGH) * HEAD_SIZE ** (-0.5)
    scores = reduced_precision_backward(raw)
    allowed = (sequence[:, None] == sequence[None, :]) & (position[None, :] <= position[:, None])
    masked = jnp.where(allowed, scores, -1e+30)
    probs = reduced_precision(jax.nn.softmax(masked, axis=-1))
    heads = jnp.einsum('kgij,jkd->ikgd', probs, value_rows, precision=HIGH).reshape(token_rows, QUERY_HEADS * HEAD_SIZE)
    mixed = reduced_precision(reduced_precision_backward(heads))
    middle = inputs + reduced_precision_backward(matrix_product(mixed, out_w))
    normed2 = reduced_precision(middle * rms_scale(middle) * gain_m)
    gate = reduced_precision_backward(matrix_product(normed2, gate_w))
    up = reduced_precision_backward(matrix_product(normed2, up_w))
    hidden = reduced_precision(jax.nn.silu(gate) * up)
    return middle + reduced_precision_backward(matrix_product(hidden, down_w))

def reference(layer_input, teacher, lengths, seq_order, gain_attn, w_query, key_projection_weight, value_projection_weight, w_out, gain_mlp, w_gate, w_up, w_down):
    params = tuple((w.astype(jnp.float32) for w in (gain_attn, w_query, key_projection_weight, value_projection_weight, w_out, gain_mlp, w_gate, w_up, w_down)))
    inputs = layer_input.astype(jnp.float32).reshape(SEQS, GRP, MODEL_WIDTH)
    targets = teacher.astype(jnp.float32).reshape(SEQS, GRP, MODEL_WIDTH)
    count = jnp.sum(lengths).astype(jnp.float32)
    inverse = jnp.argsort(seq_order, stable=True).astype(jnp.int32)

    def forward(inputs, params):
        dealt = jnp.take(inputs, seq_order, axis=0)
        aims = jnp.take(targets, seq_order, axis=0)

        def step(total, item):
            group_in, group_target, length = item
            sequence, position, inside = layout_of(length, GRP)
            result = block(group_in, sequence, position, params)
            error = (result - group_target) * inside[:, None].astype(jnp.float32)
            return (total + jnp.sum(error * error), result)
        squared, results = lax.scan(jax.checkpoint(step), jnp.zeros((), jnp.float32), (dealt, aims, lengths))
        return (TOKENS * squared / (2.0 * count), (results, squared))
    scaled, pullback, extras = jax.vjp(forward, inputs, params, has_aux=True)
    results, squared = extras
    input_grad, grads = pullback(jnp.ones_like(scaled))
    ordered = jnp.take(results, inverse, axis=0)
    distill_loss = squared / (2.0 * MODEL_WIDTH * count)
    return (ordered.reshape(TOKENS, MODEL_WIDTH).astype(jnp.bfloat16), input_grad.reshape(TOKENS, MODEL_WIDTH).astype(jnp.bfloat16), grads[0], grads[1], grads[2], grads[3], grads[4], grads[5], grads[6], grads[7], grads[8], distill_loss)
```

```python
import jax
import jax.numpy as jnp
from jax import lax
from jax.experimental import pallas as pl
from jax.experimental.pallas import tpu as pltpu
from jax.sharding import PartitionSpec as P

HEAD_SIZE = 256
LANES = 128
EPS = 1e-06
ROPE_BASE = 1000042.0
over_rows = (((0,), (0,)), ((), ()))
over_last = (((1,), (1,)), ((), ()))
plain = (((1,), (0,)), ((), ()))
f32 = jnp.float32
bf16 = jnp.bfloat16


def rms_scale(value_rows):
    return lax.rsqrt(jnp.mean(value_rows * value_rows, axis=-1, keepdims=True) + EPS)


def rope_tables(position, width):
    half = width // 2
    exponent = jnp.arange(half, dtype=f32) * (-2.0 / width)
    frequency = jnp.exp(exponent * jnp.log(f32(ROPE_BASE)))
    angle = position.astype(f32)[..., None] * frequency
    return (jnp.cos(angle), jnp.sin(angle))


def rotate(heads, cosine, sine):
    half = heads.shape[-1] // 2
    first, second = heads[..., :half], heads[..., half:]
    return jnp.concatenate(
        [first * cosine - second * sine, second * cosine + first * sine], axis=-1
    )


def ring_order(chips):
    column = chips // 2
    return [2 * i for i in range(column)] + [2 * i + 1 for i in reversed(range(column))]


class Ring:
    def __init__(self, chips):
        self.chips = chips
        order = ring_order(chips)
        self.place = [order.index(c) for c in range(chips)]
        hop = [(order[i], order[(i + 1) % chips]) for i in range(chips)]
        self.up = [(2 * a + c, 2 * b + c) for a, b in hop for c in range(2)]
        self.down = [(b, a) for a, b in self.up]
        self.swap = [(d, d ^ 1) for d in range(2 * chips)]

    def ahead(self, v):
        return lax.ppermute(v, "dp", self.up)

    def back(self, v):
        return lax.ppermute(v, "dp", self.down)

    def other_core(self, v):
        return lax.ppermute(v, "dp", self.swap)


def other_tensor(v):
    return lax.ppermute(v, "tensor", [(0, 1), (1, 0)])


def gather_ring(ring, low, high):
    lows, highs = [low], [high]
    for _ in range(ring.chips - 1):
        low, high = ring.ahead(low), ring.back(high)
        lows.append(low)
        highs.append(high)
    return lows, highs


def scatter_ring(ring, grads, rows):
    half = ring.chips * rows

    def block(side, k):
        start = side * half + k * rows
        return grads[start : start + rows]

    last = ring.chips - 1
    low, high = block(0, last), block(1, last)
    for k in range(last - 1, -1, -1):
        low = ring.back(low.astype(bf16)).astype(f32) + block(0, k)
        high = ring.ahead(high.astype(bf16)).astype(f32) + block(1, k)
    return low, high


def gather_group(ring, rows):
    across = other_tensor(rows)
    beside = ring.other_core(rows)
    return jnp.concatenate([rows, across, beside, ring.other_core(across)], axis=0)


def scatter_group(ring, parts):
    quarter = parts.shape[0] // 4
    near = parts[: 2 * quarter] + ring.other_core(parts[2 * quarter :].astype(bf16)).astype(f32)
    return near[:quarter] + other_tensor(near[quarter:].astype(bf16)).astype(f32)


def copy_block(table, source, target):
    target[...] = source[...]


def reorder(rows, table):
    height, width = rows.shape
    return pl.pallas_call(
        copy_block,
        out_shape=jax.ShapeDtypeStruct(rows.shape, rows.dtype),
        grid_spec=pltpu.PrefetchScalarGridSpec(
            num_scalar_prefetch=1,
            grid=(width // LANES,),
            in_specs=[pl.BlockSpec((height, LANES), lambda k, t: (0, t[k]))],
            out_specs=pl.BlockSpec((height, LANES), lambda k, t: (0, k)),
        ),
        name="reorder",
    )(table, rows)


def sum_all(ring, v):
    v = v + other_tensor(v)
    devices = 2 * ring.chips
    step = 1
    while step < devices:
        v = v + lax.ppermute(v, "dp", [(d, d ^ step) for d in range(devices)])
        step *= 2
    return v


def per_device(
    layer_input,
    teacher,
    lengths,
    seq_order,
    gain_attn,
    w_query,
    key_projection_weight,
    value_projection_weight,
    w_out,
    gain_mlp,
    w_gate,
    w_up,
    w_down,
):
    token_rows, width = layer_input.shape
    slots = token_rows * lax.axis_size("tensor")
    devices = lax.axis_size("dp")
    tokens_all = slots * devices
    chips = devices // 2
    ring = Ring(chips)
    me = lax.axis_index("dp")
    side = lax.axis_index("tensor")
    chip, core = me // 2, me % 2
    first_core = core == 0
    place = jnp.array(ring.place, dtype=jnp.int32)
    here = place[chip]
    piece = gain_attn.shape[0]

    numbers = jnp.arange(chips, dtype=jnp.int32)
    order = jnp.array(ring_order(chips), dtype=jnp.int32)
    from_low = 2 * order[(here - numbers) % chips]
    from_high = 2 * order[(here + numbers) % chips] + 1
    to_relative = jnp.concatenate([from_low, from_high])
    to_natural = jnp.stack(
        [(here - place) % chips, chips + (place - here) % chips], axis=1
    ).reshape(devices)

    def split_cores(w):
        quarter = w.shape[1] // 2
        mine = lax.dynamic_slice_in_dim(w, core * quarter, quarter, 1)
        given = lax.dynamic_slice_in_dim(w, (1 - core) * quarter, quarter, 1)
        return mine, given

    def both_rows(weights, gains=None):
        mine, given = zip(*[split_cores(w) for w in weights])
        mine, given = jnp.concatenate(mine, axis=1), jnp.concatenate(given, axis=1)
        if gains is not None:
            extra = jnp.pad(gains, ((0, 16 - gains.shape[0]), (0, mine.shape[1] - gains.shape[1])))
            mine = jnp.concatenate([mine, extra], axis=0)
            given = jnp.concatenate([given, extra], axis=0)
        taken = ring.other_core(given)
        return (
            jnp.where(first_core, mine, taken),
            jnp.where(first_core, taken, mine),
        )

    own_input = reorder(layer_input, to_relative)
    own_teacher = reorder(teacher, to_relative)
    gains = jnp.stack([gain_attn, gain_mlp])
    attn_low, attn_high = gather_ring(
        ring,
        *both_rows([w_query, key_projection_weight, value_projection_weight, w_out.T], gains),
    )
    gate_low, gate_high = gather_ring(ring, *both_rows([w_gate]))
    up_low, up_high = gather_ring(ring, *both_rows([w_up]))
    down_low, down_high = gather_ring(ring, *both_rows([w_down.T]))

    pieces = attn_low + attn_high
    q_width = w_query.shape[1] // 2
    kv_width = key_projection_weight.shape[1] // 2
    qkv_width = q_width + 2 * kv_width
    qkv_proj = jnp.concatenate([p[:piece, :qkv_width] for p in pieces], axis=0)
    out_proj_t = jnp.concatenate([p[:piece, qkv_width:] for p in pieces], axis=0)
    gain_rows = jnp.concatenate([p[piece : piece + 2, :piece] for p in pieces], axis=1).astype(f32)
    attn_gain, mlp_gain = gain_rows[:1], gain_rows[1:]
    gate_proj = jnp.concatenate(gate_low + gate_high, axis=0)
    up_proj = jnp.concatenate(up_low + up_high, axis=0)
    down_proj_t = jnp.concatenate(down_low + down_high, axis=0)

    sequence_numbers = jnp.stack([me, me + 1 - 2 * core])
    length = jnp.sum(
        jnp.where(seq_order[None, :] == sequence_numbers[:, None], lengths[None, :], 0), axis=1
    )
    offsets = jnp.arange(token_rows, dtype=jnp.int32)
    slot = jnp.concatenate([side * token_rows + offsets, (1 - side) * token_rows + offsets])
    inside = slot[None, :] < length[:, None]
    sequence = jnp.where(inside, 0, 1 + slot[None, :])
    position = jnp.where(inside, slot[None, :], 0)
    own_valid = inside[0, :token_rows].astype(f32)[:, None]
    allowed = (sequence[:, :, None] == sequence[:, None, :]) & (
        position[:, None, :] <= position[:, :, None]
    )
    allowed = allowed[:, None]
    cosine, sine = rope_tables(position, HEAD_SIZE)
    cosine, sine = cosine[:, :, None, :], sine[:, :, None, :]
    scaling = HEAD_SIZE ** (-0.5)
    query_heads = q_width // HEAD_SIZE
    all_rows = 2 * slots

    group_input = gather_group(ring, own_input).astype(f32)
    group_scale = rms_scale(group_input)
    normed = (group_input * group_scale * attn_gain).astype(bf16)
    qkv = jnp.dot(normed, qkv_proj, preferred_element_type=f32)
    query_rows = qkv[:, :q_width].reshape(2, slots, query_heads, HEAD_SIZE)
    key_rows = qkv[:, q_width : q_width + kv_width].reshape(2, slots, 1, HEAD_SIZE)
    values = qkv[:, q_width + kv_width :].astype(bf16).reshape(2, slots, HEAD_SIZE)
    rot_queries = rotate(query_rows, cosine, sine).astype(bf16)
    rot_keys = rotate(key_rows, cosine, sine).astype(bf16)[:, :, 0]
    scores = (
        jnp.einsum("bigd,bjd->bgij", rot_queries, rot_keys, preferred_element_type=f32) * scaling
    )
    scores = jnp.where(allowed, scores, -1e30)
    highest = jnp.max(scores, axis=-1, keepdims=True)
    shifted = jnp.exp(scores - highest)
    probs = shifted / jnp.sum(shifted, axis=-1, keepdims=True)
    probs_low = probs.astype(bf16)
    mixed = (
        jnp.einsum("bgij,bjd->bigd", probs_low, values, preferred_element_type=f32)
        .reshape(all_rows, q_width)
        .astype(bf16)
    )
    own_rows = own_input.astype(f32)
    attn_scale = rms_scale(own_rows)
    middle = own_rows + scatter_group(
        ring, lax.dot_general(mixed, out_proj_t, over_last, preferred_element_type=f32)
    )
    mlp_scale = rms_scale(middle)
    normed_mlp = gather_group(ring, (middle * mlp_scale * mlp_gain).astype(bf16))
    gate = jnp.dot(normed_mlp, gate_proj, preferred_element_type=f32)
    up = jnp.dot(normed_mlp, up_proj, preferred_element_type=f32)
    sigmoid_gate = jax.nn.sigmoid(gate)
    hidden = (gate * sigmoid_gate * up).astype(bf16)
    result = middle + scatter_group(
        ring, lax.dot_general(hidden, down_proj_t, over_last, preferred_element_type=f32)
    )
    activations = reorder(result.astype(bf16), to_natural)
    error = (result - own_teacher.astype(f32)) * own_valid
    count = jnp.sum(lengths).astype(f32)
    delta_result = error * (tokens_all / count)
    branch = gather_group(ring, delta_result.astype(bf16))
    grad_down_t = lax.dot_general(branch, hidden, over_rows, preferred_element_type=f32)
    down_sum = scatter_ring(ring, grad_down_t, piece)
    delta_hidden = jnp.dot(branch, down_proj_t, preferred_element_type=f32)
    delta_gate = (delta_hidden * up * sigmoid_gate * (1.0 + gate * (1.0 - sigmoid_gate))).astype(
        bf16
    )
    delta_up = (delta_hidden * gate * sigmoid_gate).astype(bf16)
    grad_gate = lax.dot_general(normed_mlp, delta_gate, over_rows, preferred_element_type=f32)
    gate_sum = scatter_ring(ring, grad_gate, piece)
    grad_up = lax.dot_general(normed_mlp, delta_up, over_rows, preferred_element_type=f32)
    up_sum = scatter_ring(ring, grad_up, piece)
    delta_normed_mlp = scatter_group(
        ring,
        lax.dot_general(delta_gate, gate_proj, over_last, preferred_element_type=f32)
        + lax.dot_general(delta_up, up_proj, over_last, preferred_element_type=f32),
    )
    gain_mlp_part = jnp.sum(delta_normed_mlp * middle * mlp_scale, axis=0)
    weighted_mlp = mlp_gain * delta_normed_mlp
    delta_middle = (
        delta_result
        + mlp_scale * weighted_mlp
        - middle * mlp_scale**3 * jnp.mean(middle * weighted_mlp, axis=-1, keepdims=True)
    )
    attn_low_rows = gather_group(ring, delta_middle.astype(bf16))
    grad_out_t = lax.dot_general(attn_low_rows, mixed, over_rows, preferred_element_type=f32)
    delta_mixed = (
        jnp.dot(attn_low_rows, out_proj_t, preferred_element_type=f32)
        .astype(bf16)
        .reshape(2, slots, query_heads, HEAD_SIZE)
    )
    delta_probs = jnp.einsum("bigd,bjd->bgij", delta_mixed, values, preferred_element_type=f32)
    inner = jnp.sum(probs * delta_probs, axis=-1, keepdims=True)
    delta_scores = (probs * (delta_probs - inner)).astype(bf16)
    delta_values = jnp.einsum("bgij,bigd->bjd", probs_low, delta_mixed, preferred_element_type=f32)
    delta_qrot = (
        jnp.einsum("bgij,bjd->bigd", delta_scores, rot_keys, preferred_element_type=f32) * scaling
    )
    delta_krot = (
        jnp.einsum("bgij,bigd->bjd", delta_scores, rot_queries, preferred_element_type=f32)
        * scaling
    )
    delta_queries = rotate(delta_qrot, cosine, -sine).reshape(all_rows, q_width)
    delta_keys = rotate(delta_krot[:, :, None], cosine, -sine).reshape(all_rows, kv_width)
    delta_qkv = jnp.concatenate(
        [
            delta_queries.astype(bf16),
            delta_keys.astype(bf16),
            delta_values.astype(bf16).reshape(all_rows, kv_width),
        ],
        axis=1,
    )
    grad_qkv = lax.dot_general(normed, delta_qkv, over_rows, preferred_element_type=f32)
    attn_sum = scatter_ring(ring, jnp.concatenate([grad_qkv, grad_out_t], axis=1), piece)
    delta_normed = scatter_group(
        ring, lax.dot_general(delta_qkv, qkv_proj, over_last, preferred_element_type=f32)
    )
    gain_attn_part = jnp.sum(delta_normed * own_rows * attn_scale, axis=0)
    weighted_attn = attn_gain * delta_normed
    input_grad = (
        delta_middle
        + attn_scale * weighted_attn
        - own_rows * attn_scale**3 * jnp.mean(own_rows * weighted_attn, axis=-1, keepdims=True)
    )
    input_grad = reorder(input_grad.astype(bf16), to_natural)

    squared = jnp.sum(error * error)
    natural = jnp.stack([gain_mlp_part, gain_attn_part], axis=0).reshape(2, devices, piece)[
        :, to_natural
    ]
    totals = sum_all(
        ring,
        jnp.concatenate(
            [natural.reshape(2 * devices, piece), jnp.full((8, piece), squared)], axis=0
        ),
    )
    gain_mlp_grad = lax.dynamic_slice_in_dim(totals, me, 1, 0)[0]
    gain_attn_grad = lax.dynamic_slice_in_dim(totals, devices + me, 1, 0)[0]
    distill_loss = totals[2 * devices, 0] / (2.0 * width * count)

    def finish(sums):
        low, high = sums
        kept = jnp.where(first_core, low, high)
        taken = ring.other_core(jnp.where(first_core, high, low).astype(bf16)).astype(f32)
        return kept, taken

    def whole(kept, taken):
        return jnp.concatenate(
            [jnp.where(first_core, kept, taken), jnp.where(first_core, taken, kept)], axis=1
        )

    attn_kept, attn_taken = finish(attn_sum)
    cuts = [0, q_width, q_width + kv_width, qkv_width, attn_kept.shape[1]]
    query_grad, key_grad, value_grad, out_grad_t = [
        whole(attn_kept[:, a:b], attn_taken[:, a:b]) for a, b in zip(cuts[:-1], cuts[1:])
    ]
    return (
        activations,
        input_grad,
        gain_attn_grad,
        query_grad,
        key_grad,
        value_grad,
        out_grad_t.T,
        gain_mlp_grad,
        whole(*finish(gate_sum)),
        whole(*finish(up_sum)),
        whole(*finish(down_sum)).T,
        distill_loss,
    )


def solution(mesh):
    placed = (
        P(("dp", "tensor"), None),
        P(("dp", "tensor"), None),
        P(),
        P(),
        P("dp"),
        P("dp", "tensor"),
        P("dp", "tensor"),
        P("dp", "tensor"),
        P("tensor", "dp"),
        P("dp"),
        P("dp", "tensor"),
        P("dp", "tensor"),
        P("tensor", "dp"),
    )
    return jax.shard_map(
        per_device,
        mesh=mesh,
        in_specs=placed,
        out_specs=(
            P(("dp", "tensor"), None),
            P(("dp", "tensor"), None),
            P("dp"),
            P("dp", "tensor"),
            P("dp", "tensor"),
            P("dp", "tensor"),
            P("tensor", "dp"),
            P("dp"),
            P("dp", "tensor"),
            P("dp", "tensor"),
            P("tensor", "dp"),
            P(),
        ),
        check_vma=False,
    )
```

```python
import jax
import jax.numpy as jnp
from jax import lax
from jax.experimental import pallas as pl
from jax.experimental.pallas import tpu as pltpu
from jax.sharding import PartitionSpec as P

HEAD_SIZE = 256
LANES = 128
EPS = 1e-06
ROPE_BASE = 1000042.0
over_rows = (((0,), (0,)), ((), ()))
over_last = (((1,), (1,)), ((), ()))
plain = (((1,), (0,)), ((), ()))
f32 = jnp.float32
bf16 = jnp.bfloat16


def rms_scale(value_rows):
    return lax.rsqrt(jnp.mean(value_rows * value_rows, axis=-1, keepdims=True) + EPS)


def rope_tables(position, width):
    half = width // 2
    exponent = jnp.arange(half, dtype=f32) * (-2.0 / width)
    frequency = jnp.exp(exponent * jnp.log(f32(ROPE_BASE)))
    angle = position.astype(f32)[..., None] * frequency
    return (jnp.cos(angle), jnp.sin(angle))


def rotate(heads, cosine, sine):
    half = heads.shape[-1] // 2
    first, second = heads[..., :half], heads[..., half:]
    return jnp.concatenate(
        [first * cosine - second * sine, second * cosine + first * sine], axis=-1
    )


def ring_order(chips):
    column = chips // 2
    return [2 * i for i in range(column)] + [2 * i + 1 for i in reversed(range(column))]


class Ring:
    def __init__(self, chips):
        self.chips = chips
        order = ring_order(chips)
        self.place = [order.index(c) for c in range(chips)]
        hop = [(order[i], order[(i + 1) % chips]) for i in range(chips)]
        self.up = [(2 * a + c, 2 * b + c) for a, b in hop for c in range(2)]
        self.down = [(b, a) for a, b in self.up]
        self.swap = [(d, d ^ 1) for d in range(2 * chips)]

    def ahead(self, v):
        return lax.ppermute(v, "dp", self.up)

    def back(self, v):
        return lax.ppermute(v, "dp", self.down)

    def other_core(self, v):
        return lax.ppermute(v, "dp", self.swap)


def other_tensor(v):
    return lax.ppermute(v, "tensor", [(0, 1), (1, 0)])


def together(values):
    return lax.optimization_barrier(values)


class Gather:
    def __init__(self, ring, low, high):
        self.ring = ring
        self.now = (low, high)
        self.lows, self.highs = [low], [high]

    def move(self):
        return self.ring.ahead(self.now[0]), self.ring.back(self.now[1])

    def take(self, moved):
        self.now = moved
        self.lows.append(moved[0])
        self.highs.append(moved[1])

    def rows(self):
        return self.lows + self.highs


class Scatter:
    def __init__(self, ring, grads, rows):
        self.ring, self.grads, self.size = ring, grads, rows
        self.left = ring.chips - 1
        self.now = (self.block(0), self.block(1))

    def block(self, half):
        start = (half * self.ring.chips + self.left) * self.size
        return jnp.concatenate([g[start : start + self.size] for g in self.grads], axis=1)

    def move(self):
        return self.ring.back(self.now[0]), self.ring.ahead(self.now[1])

    def take(self, moved):
        self.left -= 1
        sums = [m.astype(f32) + self.block(half).astype(f32) for half, m in enumerate(moved)]
        self.now = tuple(sums if self.left == 0 else [v.astype(bf16) for v in sums])


def turn(lane, other=None, values=()):
    moved, _, values = together((lane.move(), other.now if other else (), values))
    lane.take(moved)
    return values


class Stages:
    def __init__(self, generator):
        self.generator = generator
        self.result = None
        self.value = ()
        self.over = False
        self.advance(None)

    def advance(self, value):
        if not self.over:
            try:
                self.value = self.generator.send(value)
            except StopIteration as end:
                self.result, self.over, self.value = end.value, True, ()

    def turn(self, lane, other=None):
        self.advance(turn(lane, other, self.value))

    def finish(self):
        while not self.over:
            self.advance(self.value)
        return self.result


def gather_group(ring, rows):
    across = other_tensor(rows)
    beside = ring.other_core(rows)
    return jnp.concatenate([rows, across, beside, ring.other_core(across)], axis=0)


def scatter_group(ring, parts):
    quarter = parts.shape[0] // 4
    near = parts[: 2 * quarter] + ring.other_core(parts[2 * quarter :].astype(bf16)).astype(f32)
    return near[:quarter] + other_tensor(near[quarter:].astype(bf16)).astype(f32)


def copy_blocks(table, source, target):
    for k in range(target.shape[1] // LANES):
        start = pl.multiple_of(table[k] * LANES, LANES)
        target[:, k * LANES : (k + 1) * LANES] = source[:, pl.ds(start, LANES)]


def reorder(rows, table):
    height, width = rows.shape
    step = height // 4
    return pl.pallas_call(
        copy_blocks,
        out_shape=jax.ShapeDtypeStruct(rows.shape, rows.dtype),
        grid_spec=pltpu.PrefetchScalarGridSpec(
            num_scalar_prefetch=1,
            grid=(height // step,),
            in_specs=[pl.BlockSpec((step, width), lambda k, t: (k, 0))],
            out_specs=pl.BlockSpec((step, width), lambda k, t: (k, 0)),
        ),
        name="reorder",
    )(table, rows)


def sum_all(ring, v):
    v = v + other_tensor(v)
    devices = 2 * ring.chips
    step = 1
    while step < devices:
        v = v + lax.ppermute(v, "dp", [(d, d ^ step) for d in range(devices)])
        step *= 2
    return v


def per_device(
    layer_input,
    teacher,
    lengths,
    seq_order,
    gain_attn,
    w_query,
    key_projection_weight,
    value_projection_weight,
    w_out,
    gain_mlp,
    w_gate,
    w_up,
    w_down,
):
    token_rows, width = layer_input.shape
    slots = token_rows * lax.axis_size("tensor")
    devices = lax.axis_size("dp")
    tokens_all = slots * devices
    chips = devices // 2
    ring = Ring(chips)
    me = lax.axis_index("dp")
    side = lax.axis_index("tensor")
    chip, core = me // 2, me % 2
    first_core = core == 0
    place = jnp.array(ring.place, dtype=jnp.int32)
    here = place[chip]
    piece = gain_attn.shape[0]

    numbers = jnp.arange(chips, dtype=jnp.int32)
    order = jnp.array(ring_order(chips), dtype=jnp.int32)
    from_low = 2 * order[(here - numbers) % chips]
    from_high = 2 * order[(here + numbers) % chips] + 1
    to_relative = jnp.concatenate([from_low, from_high])
    to_natural = jnp.stack(
        [(here - place) % chips, chips + (place - here) % chips], axis=1
    ).reshape(devices)

    def split_cores(w):
        quarter = w.shape[1] // 2
        mine = lax.dynamic_slice_in_dim(w, core * quarter, quarter, 1)
        given = lax.dynamic_slice_in_dim(w, (1 - core) * quarter, quarter, 1)
        return mine, given

    def both_rows(weights, gains=None):
        mine, given = zip(*[split_cores(w) for w in weights])
        mine, given = jnp.concatenate(mine, axis=1), jnp.concatenate(given, axis=1)
        if gains is not None:
            extra = jnp.pad(gains, ((0, 16 - gains.shape[0]), (0, mine.shape[1] - gains.shape[1])))
            mine = jnp.concatenate([mine, extra], axis=0)
            given = jnp.concatenate([given, extra], axis=0)
        taken = ring.other_core(given)
        return (
            jnp.where(first_core, mine, taken),
            jnp.where(first_core, taken, mine),
        )

    gains = jnp.stack([gain_attn, gain_mlp])
    hops = ring.chips - 1
    attn_weights = Gather(
        ring,
        *both_rows([w_query, key_projection_weight, value_projection_weight, w_out.T], gains),
    )
    gate_weights = Gather(ring, *both_rows([w_gate]))
    own_input = reorder(layer_input, to_relative)
    group_rows = gather_group(ring, own_input)
    for k in range(hops):
        turn(attn_weights, gate_weights)
        turn(gate_weights, attn_weights)
    up_weights = Gather(ring, *together((both_rows([w_up]), attn_weights.now))[0])
    down_weights = Gather(ring, *together((both_rows([w_down.T]), gate_weights.now))[0])

    sequence_numbers = jnp.stack([me, me + 1 - 2 * core])
    length = jnp.sum(
        jnp.where(seq_order[None, :] == sequence_numbers[:, None], lengths[None, :], 0), axis=1
    )
    offsets = jnp.arange(token_rows, dtype=jnp.int32)
    slot = jnp.concatenate([side * token_rows + offsets, (1 - side) * token_rows + offsets])
    inside = slot[None, :] < length[:, None]
    sequence = jnp.where(inside, 0, 1 + slot[None, :])
    position = jnp.where(inside, slot[None, :], 0)
    own_valid = inside[0, :token_rows].astype(f32)[:, None]
    allowed = (sequence[:, :, None] == sequence[:, None, :]) & (
        position[:, None, :] <= position[:, :, None]
    )
    allowed = allowed[:, None]
    cosine, sine = rope_tables(position, HEAD_SIZE)
    cosine, sine = cosine[:, :, None, :], sine[:, :, None, :]
    scaling = HEAD_SIZE ** (-0.5)
    q_width = w_query.shape[1] // 2
    kv_width = key_projection_weight.shape[1] // 2
    qkv_width = q_width + 2 * kv_width
    query_heads = q_width // HEAD_SIZE
    all_rows = 2 * slots
    own_rows = own_input.astype(f32)
    attn_scale = rms_scale(own_rows)

    pieces = attn_weights.rows()
    qkv_proj = jnp.concatenate([p[:piece, :qkv_width] for p in pieces], axis=0)
    out_proj_t = jnp.concatenate([p[:piece, qkv_width:] for p in pieces], axis=0)
    gain_rows = jnp.concatenate([p[piece : piece + 2, :piece] for p in pieces], axis=1).astype(f32)
    attn_gain, mlp_gain = gain_rows[:1], gain_rows[1:]
    gate_proj = jnp.concatenate(gate_weights.rows(), axis=0)

    def forward():
        group_input = group_rows.astype(f32)
        normed = (group_input * rms_scale(group_input) * attn_gain).astype(bf16)
        qkv = jnp.dot(normed, qkv_proj, preferred_element_type=f32)
        normed, qkv = yield normed, qkv
        query_rows = qkv[:, :q_width].reshape(2, slots, query_heads, HEAD_SIZE)
        key_rows = qkv[:, q_width : q_width + kv_width].reshape(2, slots, 1, HEAD_SIZE)
        values = qkv[:, q_width + kv_width :].astype(bf16).reshape(2, slots, HEAD_SIZE)
        rot_queries = rotate(query_rows, cosine, sine).astype(bf16)
        rot_keys = rotate(key_rows, cosine, sine).astype(bf16)[:, :, 0]
        rot_queries, rot_keys, values = yield rot_queries, rot_keys, values
        scores = (
            jnp.einsum("bigd,bjd->bgij", rot_queries, rot_keys, preferred_element_type=f32)
            * scaling
        )
        scores = jnp.where(allowed, scores, -1e30)
        shifted = jnp.exp(scores - jnp.max(scores, axis=-1, keepdims=True))
        probs = shifted / jnp.sum(shifted, axis=-1, keepdims=True)
        probs = yield probs
        mixed = (
            jnp.einsum("bgij,bjd->bigd", probs.astype(bf16), values, preferred_element_type=f32)
            .reshape(all_rows, q_width)
            .astype(bf16)
        )
        parts = lax.dot_general(mixed, out_proj_t, over_last, preferred_element_type=f32)
        mixed, parts = yield mixed, parts
        shared = scatter_group(ring, parts)
        yield ()
        yield ()
        shared = yield shared
        middle = own_rows + shared
        mlp_scale = rms_scale(middle)
        normed_mlp = gather_group(ring, (middle * mlp_scale * mlp_gain).astype(bf16))
        yield ()
        yield ()
        normed_mlp = yield normed_mlp
        gate = jnp.dot(normed_mlp, gate_proj, preferred_element_type=f32)
        gate = yield gate
        return normed, rot_queries, rot_keys, values, probs, mixed, middle, mlp_scale, normed_mlp, gate

    stages = Stages(forward())
    for k in range(hops):
        stages.turn(up_weights, down_weights)
        stages.turn(down_weights, up_weights)
    (normed, rot_queries, rot_keys, values, probs, mixed, middle, mlp_scale, normed_mlp, gate) = (
        stages.finish()
    )
    up_proj = jnp.concatenate(up_weights.rows(), axis=0)
    down_proj_t = jnp.concatenate(down_weights.rows(), axis=0)
    own_teacher = reorder(teacher, to_relative)

    up = jnp.dot(normed_mlp, up_proj, preferred_element_type=f32)
    sigmoid_gate = jax.nn.sigmoid(gate)
    hidden = (gate * sigmoid_gate * up).astype(bf16)
    result = middle + scatter_group(
        ring, lax.dot_general(hidden, down_proj_t, over_last, preferred_element_type=f32)
    )
    error = (result - own_teacher.astype(f32)) * own_valid
    count = jnp.sum(lengths).astype(f32)
    delta_result = error * (tokens_all / count)
    branch = gather_group(ring, delta_result.astype(bf16))
    grad_down_t = lax.dot_general(branch, hidden, over_rows, preferred_element_type=f32)
    down_sums = Scatter(ring, [grad_down_t.astype(bf16)], piece)

    def backward():
        activations = reorder(result.astype(bf16), to_natural)
        delta_hidden = jnp.dot(branch, down_proj_t, preferred_element_type=f32)
        delta_gate = (
            delta_hidden * up * sigmoid_gate * (1.0 + gate * (1.0 - sigmoid_gate))
        ).astype(bf16)
        delta_up = (delta_hidden * gate * sigmoid_gate).astype(bf16)
        activations, delta_gate, delta_up = yield activations, delta_gate, delta_up
        grad_gate = lax.dot_general(
            normed_mlp, delta_gate, over_rows, preferred_element_type=f32
        ).astype(bf16)
        grad_gate, delta_gate = yield grad_gate, delta_gate
        grad_up = lax.dot_general(
            normed_mlp, delta_up, over_rows, preferred_element_type=f32
        ).astype(bf16)
        grad_up, delta_up = yield grad_up, delta_up
        gate_up.append(grad_gate)
        gate_up.append(grad_up)
        from_gate = lax.dot_general(delta_gate, gate_proj, over_last, preferred_element_type=f32)
        from_gate, delta_up = yield from_gate, delta_up
        parts = from_gate + lax.dot_general(
            delta_up, up_proj, over_last, preferred_element_type=f32
        )
        parts = yield parts
        delta_normed_mlp = scatter_group(ring, parts)
        yield ()
        delta_normed_mlp = yield delta_normed_mlp
        gain_mlp_part = jnp.sum(delta_normed_mlp * middle * mlp_scale, axis=0)
        weighted_mlp = mlp_gain * delta_normed_mlp
        delta_middle = (
            delta_result
            + mlp_scale * weighted_mlp
            - middle * mlp_scale**3 * jnp.mean(middle * weighted_mlp, axis=-1, keepdims=True)
        )
        attn_low_rows = gather_group(ring, delta_middle.astype(bf16))
        yield ()
        attn_low_rows = yield attn_low_rows
        grad_out_t = lax.dot_general(attn_low_rows, mixed, over_rows, preferred_element_type=f32)
        delta_mixed = (
            jnp.dot(attn_low_rows, out_proj_t, preferred_element_type=f32)
            .astype(bf16)
            .reshape(2, slots, query_heads, HEAD_SIZE)
        )
        grad_out_t, delta_mixed = yield grad_out_t.astype(bf16), delta_mixed
        probs_low = probs.astype(bf16)
        delta_probs = jnp.einsum("bigd,bjd->bgij", delta_mixed, values, preferred_element_type=f32)
        inner = jnp.sum(probs * delta_probs, axis=-1, keepdims=True)
        delta_scores = (probs * (delta_probs - inner)).astype(bf16)
        delta_values = jnp.einsum(
            "bgij,bigd->bjd", probs_low, delta_mixed, preferred_element_type=f32
        )
        delta_scores, delta_values = yield delta_scores, delta_values
        delta_qrot = (
            jnp.einsum("bgij,bjd->bigd", delta_scores, rot_keys, preferred_element_type=f32)
            * scaling
        )
        delta_krot = (
            jnp.einsum("bgij,bigd->bjd", delta_scores, rot_queries, preferred_element_type=f32)
            * scaling
        )
        delta_queries = rotate(delta_qrot, cosine, -sine).reshape(all_rows, q_width)
        delta_keys = rotate(delta_krot[:, :, None], cosine, -sine).reshape(all_rows, kv_width)
        delta_qkv = jnp.concatenate(
            [
                delta_queries.astype(bf16),
                delta_keys.astype(bf16),
                delta_values.astype(bf16).reshape(all_rows, kv_width),
            ],
            axis=1,
        )
        delta_qkv = yield delta_qkv
        grad_qkv = lax.dot_general(normed, delta_qkv, over_rows, preferred_element_type=f32)
        return (
            activations,
            gain_mlp_part,
            delta_middle,
            delta_qkv,
            [grad_qkv.astype(bf16), grad_out_t],
        )

    gate_up = []
    stages = Stages(backward())
    for k in range(3):
        stages.turn(down_sums)
    gate_up_sums = Scatter(ring, gate_up, piece)
    for k in range(hops):
        stages.turn(gate_up_sums, down_sums)
        if down_sums.left:
            stages.turn(down_sums, gate_up_sums)
    activations, gain_mlp_part, delta_middle, delta_qkv, attn_grads = stages.finish()
    attn_sums = Scatter(ring, attn_grads, piece)
    squared = jnp.sum(error * error)

    def finish(sums):
        low, high = sums.now
        kept = jnp.where(first_core, low, high)
        taken = ring.other_core(jnp.where(first_core, high, low).astype(bf16)).astype(f32)
        return kept, taken

    def whole(kept, taken):
        return jnp.concatenate(
            [jnp.where(first_core, kept, taken), jnp.where(first_core, taken, kept)], axis=1
        )

    def closing():
        delta_normed = scatter_group(
            ring, lax.dot_general(delta_qkv, qkv_proj, over_last, preferred_element_type=f32)
        )
        down_grad = whole(*finish(down_sums)).T
        down_grad = yield down_grad
        kept, taken = finish(gate_up_sums)
        gate_width = w_gate.shape[1] // 2
        gate_grad = whole(kept[:, :gate_width], taken[:, :gate_width])
        up_grad = whole(kept[:, gate_width:], taken[:, gate_width:])
        gate_grad, up_grad, delta_normed = yield gate_grad, up_grad, delta_normed
        gain_attn_part = jnp.sum(delta_normed * own_rows * attn_scale, axis=0)
        weighted_attn = attn_gain * delta_normed
        input_grad = (
            delta_middle
            + attn_scale * weighted_attn
            - own_rows * attn_scale**3 * jnp.mean(own_rows * weighted_attn, axis=-1, keepdims=True)
        )
        input_grad = reorder(input_grad.astype(bf16), to_natural)
        natural = jnp.stack([gain_mlp_part, gain_attn_part], axis=0).reshape(2, devices, piece)[
            :, to_natural
        ]
        sums = jnp.concatenate(
            [natural.reshape(2 * devices, piece), jnp.full((8, piece), squared)], axis=0
        )
        input_grad, sums = yield input_grad, sums
        totals = yield sum_all(ring, sums)
        return down_grad, gate_grad, up_grad, input_grad, totals

    stages = Stages(closing())
    for k in range(hops):
        stages.turn(attn_sums)
    down_grad, gate_grad, up_grad, input_grad, totals = stages.finish()
    gain_mlp_grad = lax.dynamic_slice_in_dim(totals, me, 1, 0)[0]
    gain_attn_grad = lax.dynamic_slice_in_dim(totals, devices + me, 1, 0)[0]
    distill_loss = totals[2 * devices, 0] / (2.0 * width * count)
    attn_kept, attn_taken = finish(attn_sums)
    cuts = [0, q_width, q_width + kv_width, qkv_width, attn_kept.shape[1]]
    query_grad, key_grad, value_grad, out_grad_t = [
        whole(attn_kept[:, a:b], attn_taken[:, a:b]) for a, b in zip(cuts[:-1], cuts[1:])
    ]
    return (
        activations,
        input_grad,
        gain_attn_grad,
        query_grad,
        key_grad,
        value_grad,
        out_grad_t.T,
        gain_mlp_grad,
        gate_grad,
        up_grad,
        down_grad,
        distill_loss,
    )


def solution(mesh):
    placed = (
        P(("dp", "tensor"), None),
        P(("dp", "tensor"), None),
        P(),
        P(),
        P("dp"),
        P("dp", "tensor"),
        P("dp", "tensor"),
        P("dp", "tensor"),
        P("tensor", "dp"),
        P("dp"),
        P("dp", "tensor"),
        P("dp", "tensor"),
        P("tensor", "dp"),
    )
    return jax.shard_map(
        per_device,
        mesh=mesh,
        in_specs=placed,
        out_specs=(
            P(("dp", "tensor"), None),
            P(("dp", "tensor"), None),
            P("dp"),
            P("dp", "tensor"),
            P("dp", "tensor"),
            P("dp", "tensor"),
            P("tensor", "dp"),
            P("dp"),
            P("dp", "tensor"),
            P("dp", "tensor"),
            P("tensor", "dp"),
            P(),
        ),
        check_vma=False,
    )
```

```python
import jax
import jax.numpy as jnp
from jax import lax
from jax.experimental import pallas as pl
from jax.experimental.pallas import tpu as pltpu
from jax.sharding import PartitionSpec as P

HEAD_SIZE = 256
LANES = 128
EPS = 1e-06
ROPE_BASE = 1000042.0
over_rows = (((0,), (0,)), ((), ()))
over_last = (((1,), (1,)), ((), ()))
plain = (((1,), (0,)), ((), ()))
f32 = jnp.float32
bf16 = jnp.bfloat16


def rms_scale(value_rows):
    return lax.rsqrt(jnp.mean(value_rows * value_rows, axis=-1, keepdims=True) + EPS)


def rope_tables(position, width):
    half = width // 2
    exponent = jnp.arange(half, dtype=f32) * (-2.0 / width)
    frequency = jnp.exp(exponent * jnp.log(f32(ROPE_BASE)))
    angle = position.astype(f32)[..., None] * frequency
    return (jnp.cos(angle), jnp.sin(angle))


def rotate(heads, cosine, sine):
    half = heads.shape[-1] // 2
    first, second = heads[..., :half], heads[..., half:]
    return jnp.concatenate(
        [first * cosine - second * sine, second * cosine + first * sine], axis=-1
    )


def ring_order(chips):
    column = chips // 2
    return [2 * i for i in range(column)] + [2 * i + 1 for i in reversed(range(column))]


class Ring:
    def __init__(self, chips):
        self.chips = chips
        order = ring_order(chips)
        self.place = [order.index(c) for c in range(chips)]
        hop = [(order[i], order[(i + 1) % chips]) for i in range(chips)]
        self.up = [(2 * a + c, 2 * b + c) for a, b in hop for c in range(2)]
        self.down = [(b, a) for a, b in self.up]
        self.swap = [(d, d ^ 1) for d in range(2 * chips)]

    def ahead(self, v):
        return lax.ppermute(v, "dp", self.up)

    def back(self, v):
        return lax.ppermute(v, "dp", self.down)

    def other_core(self, v):
        return lax.ppermute(v, "dp", self.swap)


def other_tensor(v):
    return lax.ppermute(v, "tensor", [(0, 1), (1, 0)])


def together(values):
    return lax.optimization_barrier(values)


class Gather:
    def __init__(self, ring, low, high):
        self.ring = ring
        self.now = (low, high)
        self.lows, self.highs = [low], [high]

    def move(self):
        return self.ring.ahead(self.now[0]), self.ring.back(self.now[1])

    def take(self, moved):
        self.now = moved
        self.lows.append(moved[0])
        self.highs.append(moved[1])

    def far(self):
        half = self.ring.chips // 2
        return jnp.concatenate(self.lows[half:] + self.highs[half:], axis=0)

    def near(self):
        half = self.ring.chips // 2
        return jnp.concatenate(self.lows[:half] + self.highs[:half], axis=0)

    def rows(self):
        half = self.ring.chips // 2
        return self.lows[half:] + self.highs[half:] + self.lows[:half] + self.highs[:half]


class Scatter:
    def __init__(self, ring, far, near, rows):
        self.ring, self.parts, self.size = ring, (near, far), rows
        self.left = ring.chips - 1
        self.now = (self.block(0), self.block(1))

    def block(self, side):
        half = self.ring.chips // 2
        grads = self.parts[self.left // half]
        start = (side * half + self.left % half) * self.size
        return jnp.concatenate([g[start : start + self.size] for g in grads], axis=1)

    def move(self):
        return self.ring.back(self.now[0]), self.ring.ahead(self.now[1])

    def take(self, moved):
        self.left -= 1
        sums = [m.astype(f32) + self.block(side).astype(f32) for side, m in enumerate(moved)]
        self.now = tuple(sums if self.left == 0 else [v.astype(bf16) for v in sums])


class Held:
    def __init__(self, *value):
        self.value = value if len(value) > 1 else value[0]


def turn(lane, other=None, values=(), held=()):
    moved, _, held = together((lane.move(), other.now if other else (), held))
    values = together((values, moved))[0]
    lane.take(moved)
    return values, held


class Stages:
    def __init__(self, generator):
        self.generator = generator
        self.result = None
        self.value = ()
        self.over = False
        self.advance(None)

    def advance(self, value):
        if not self.over:
            try:
                self.value = self.generator.send(value)
            except StopIteration as end:
                self.result, self.over, self.value = end.value, True, ()

    def turn(self, lane, other=None, extra=()):
        if isinstance(self.value, Held):
            extra, value = turn(lane, other, extra, self.value.value)
        else:
            (value, extra), _ = turn(lane, other, (self.value, extra))
        self.advance(value)
        return extra

    def finish(self):
        while not self.over:
            self.advance(self.value.value if isinstance(self.value, Held) else self.value)
        return self.result


def gather_group(ring, rows):
    across = other_tensor(rows)
    beside = ring.other_core(rows)
    return jnp.concatenate([rows, across, beside, ring.other_core(across)], axis=0)


def scatter_group(ring, parts):
    quarter = parts.shape[0] // 4
    near = parts[: 2 * quarter] + ring.other_core(parts[2 * quarter :].astype(bf16)).astype(f32)
    return near[:quarter] + other_tensor(near[quarter:].astype(bf16)).astype(f32)


def copy_blocks(table, source, target):
    for k in range(target.shape[1] // LANES):
        start = pl.multiple_of(table[k] * LANES, LANES)
        target[:, k * LANES : (k + 1) * LANES] = source[:, pl.ds(start, LANES)]


def reorder(rows, table):
    height, width = rows.shape
    step = height // 4
    return pl.pallas_call(
        copy_blocks,
        out_shape=jax.ShapeDtypeStruct(rows.shape, rows.dtype),
        grid_spec=pltpu.PrefetchScalarGridSpec(
            num_scalar_prefetch=1,
            grid=(height // step,),
            in_specs=[pl.BlockSpec((step, width), lambda k, t: (k, 0))],
            out_specs=pl.BlockSpec((step, width), lambda k, t: (k, 0)),
        ),
        name="reorder",
    )(table, rows)


def sum_all(ring, v):
    v = v + other_tensor(v)
    devices = 2 * ring.chips
    step = 1
    while step < devices:
        v = v + lax.ppermute(v, "dp", [(d, d ^ step) for d in range(devices)])
        step *= 2
    return v


def per_device(
    layer_input,
    teacher,
    lengths,
    seq_order,
    gain_attn,
    w_query,
    key_projection_weight,
    value_projection_weight,
    w_out,
    gain_mlp,
    w_gate,
    w_up,
    w_down,
):
    token_rows, width = layer_input.shape
    slots = token_rows * lax.axis_size("tensor")
    devices = lax.axis_size("dp")
    tokens_all = slots * devices
    chips = devices // 2
    ring = Ring(chips)
    me = lax.axis_index("dp")
    side = lax.axis_index("tensor")
    chip, core = me // 2, me % 2
    first_core = core == 0
    place = jnp.array(ring.place, dtype=jnp.int32)
    here = place[chip]
    piece = gain_attn.shape[0]

    numbers = jnp.arange(chips, dtype=jnp.int32)
    order = jnp.array(ring_order(chips), dtype=jnp.int32)
    from_low = 2 * order[(here - numbers) % chips]
    from_high = 2 * order[(here + numbers) % chips] + 1
    half = chips // 2
    to_relative = jnp.concatenate(
        [from_low[half:], from_high[half:], from_low[:half], from_high[:half]]
    )
    behind, before = (here - place) % chips, (place - here) % chips
    to_natural = jnp.stack(
        [
            jnp.where(behind < half, behind + 2 * half, behind - half),
            jnp.where(before < half, before + 3 * half, before),
        ],
        axis=1,
    ).reshape(devices)

    def split_cores(w):
        quarter = w.shape[1] // 2
        mine = lax.dynamic_slice_in_dim(w, core * quarter, quarter, 1)
        given = lax.dynamic_slice_in_dim(w, (1 - core) * quarter, quarter, 1)
        return mine, given

    def both_rows(weights, gains=None):
        mine, given = zip(*[split_cores(w) for w in weights])
        mine, given = jnp.concatenate(mine, axis=1), jnp.concatenate(given, axis=1)
        if gains is not None:
            extra = jnp.pad(gains, ((0, 16 - gains.shape[0]), (0, mine.shape[1] - gains.shape[1])))
            mine = jnp.concatenate([mine, extra], axis=0)
            given = jnp.concatenate([given, extra], axis=0)
        taken = ring.other_core(given)
        return (
            jnp.where(first_core, mine, taken),
            jnp.where(first_core, taken, mine),
        )

    gains = jnp.stack([gain_attn, gain_mlp])
    hops = ring.chips - 1
    attn_weights = Gather(
        ring,
        *both_rows([w_query, key_projection_weight, value_projection_weight, w_out.T], gains),
    )
    gate_weights = Gather(ring, *both_rows([w_gate]))
    own_input = reorder(layer_input, to_relative)
    group_rows = gather_group(ring, own_input)
    for k in range(hops):
        turn(attn_weights, gate_weights)
        turn(gate_weights, attn_weights)
    up_weights = Gather(ring, *together((both_rows([w_up]), attn_weights.now))[0])
    down_weights = Gather(ring, *together((both_rows([w_down.T]), gate_weights.now))[0])

    sequence_numbers = jnp.stack([me, me + 1 - 2 * core])
    length = jnp.sum(
        jnp.where(seq_order[None, :] == sequence_numbers[:, None], lengths[None, :], 0), axis=1
    )
    offsets = jnp.arange(token_rows, dtype=jnp.int32)
    slot = jnp.concatenate([side * token_rows + offsets, (1 - side) * token_rows + offsets])
    inside = slot[None, :] < length[:, None]
    sequence = jnp.where(inside, 0, 1 + slot[None, :])
    position = jnp.where(inside, slot[None, :], 0)
    own_valid = inside[0, :token_rows].astype(f32)[:, None]
    allowed = (sequence[:, :, None] == sequence[:, None, :]) & (
        position[:, None, :] <= position[:, :, None]
    )
    allowed = allowed[:, None]
    cosine, sine = rope_tables(position, HEAD_SIZE)
    cosine, sine = cosine[:, :, None, :], sine[:, :, None, :]
    scaling = HEAD_SIZE ** (-0.5)
    q_width = w_query.shape[1] // 2
    kv_width = key_projection_weight.shape[1] // 2
    qkv_width = q_width + 2 * kv_width
    query_heads = q_width // HEAD_SIZE
    all_rows = 2 * slots
    own_rows = own_input.astype(f32)
    attn_scale = rms_scale(own_rows)

    pieces = attn_weights.rows()
    qkv_proj = jnp.concatenate([p[:piece, :qkv_width] for p in pieces], axis=0)
    out_proj_t = jnp.concatenate([p[:piece, qkv_width:] for p in pieces], axis=0)
    gain_rows = jnp.concatenate([p[piece : piece + 2, :piece] for p in pieces], axis=1).astype(f32)
    attn_gain, mlp_gain = gain_rows[:1], gain_rows[1:]
    gate_proj = jnp.concatenate(gate_weights.rows(), axis=0)

    def forward():
        group_input = group_rows.astype(f32)
        normed = (group_input * rms_scale(group_input) * attn_gain).astype(bf16)
        qkv = jnp.dot(normed, qkv_proj, preferred_element_type=f32)
        normed, qkv = yield normed, qkv
        query_rows = qkv[:, :q_width].reshape(2, slots, query_heads, HEAD_SIZE)
        key_rows = qkv[:, q_width : q_width + kv_width].reshape(2, slots, 1, HEAD_SIZE)
        values = qkv[:, q_width + kv_width :].astype(bf16).reshape(2, slots, HEAD_SIZE)
        rot_queries = rotate(query_rows, cosine, sine).astype(bf16)
        rot_keys = rotate(key_rows, cosine, sine).astype(bf16)[:, :, 0]
        rot_queries, rot_keys, values = yield rot_queries, rot_keys, values
        scores = (
            jnp.einsum("bigd,bjd->bgij", rot_queries, rot_keys, preferred_element_type=f32)
            * scaling
        )
        scores = jnp.where(allowed, scores, -1e30)
        shifted = jnp.exp(scores - jnp.max(scores, axis=-1, keepdims=True))
        probs = shifted / jnp.sum(shifted, axis=-1, keepdims=True)
        probs = yield probs
        mixed = (
            jnp.einsum("bgij,bjd->bigd", probs.astype(bf16), values, preferred_element_type=f32)
            .reshape(all_rows, q_width)
            .astype(bf16)
        )
        parts = lax.dot_general(mixed, out_proj_t, over_last, preferred_element_type=f32)
        mixed, parts = yield mixed, parts
        shared = scatter_group(ring, parts)
        yield ()
        yield ()
        shared = yield shared
        middle = own_rows + shared
        mlp_scale = rms_scale(middle)
        normed_mlp = gather_group(ring, (middle * mlp_scale * mlp_gain).astype(bf16))
        yield ()
        yield ()
        normed_mlp = yield normed_mlp
        gate = jnp.dot(normed_mlp, gate_proj, preferred_element_type=f32)
        gate = yield gate
        return normed, rot_queries, rot_keys, values, probs, mixed, middle, mlp_scale, normed_mlp, gate

    stages = Stages(forward())
    for k in range(hops):
        stages.turn(up_weights, down_weights)
        stages.turn(down_weights, up_weights)
    (normed, rot_queries, rot_keys, values, probs, mixed, middle, mlp_scale, normed_mlp, gate) = (
        stages.finish()
    )
    up_proj = jnp.concatenate(up_weights.rows(), axis=0)
    down_far, down_near = down_weights.far(), down_weights.near()
    own_teacher = reorder(teacher, to_relative)
    count = jnp.sum(lengths).astype(f32)

    up = jnp.dot(normed_mlp, up_proj, preferred_element_type=f32)
    sigmoid_gate = jax.nn.sigmoid(gate)
    hidden = (gate * sigmoid_gate * up).astype(bf16)
    cut = width // 2

    def output(proj_t, columns, before=()):
        parts = lax.dot_general(hidden, proj_t, over_last, preferred_element_type=f32)
        shared = together((scatter_group(ring, parts), before))[0]
        result = middle[:, columns] + shared
        error = (result - own_teacher[:, columns].astype(f32)) * own_valid
        delta = error * (tokens_all / count)
        return result, error, delta, gather_group(ring, delta.astype(bf16))

    def down_grad_of(branch):
        return lax.dot_general(branch, hidden, over_rows, preferred_element_type=f32).astype(bf16)

    result_far, error_far, delta_far, branch_far = output(down_far, slice(0, cut))
    result_near, error_near, delta_near, branch_near = output(down_near, slice(cut, width), delta_far)
    down_sums = Scatter(ring, [down_grad_of(branch_far)], [down_grad_of(branch_near)], piece)
    result = jnp.concatenate([result_far, result_near], axis=1)
    delta_result = jnp.concatenate([delta_far, delta_near], axis=1)
    squared = jnp.sum(error_far * error_far) + jnp.sum(error_near * error_near)

    def backward():
        activations = reorder(result.astype(bf16), to_natural)
        delta_hidden = jnp.dot(branch_far, down_far, preferred_element_type=f32) + jnp.dot(
            branch_near, down_near, preferred_element_type=f32
        )
        delta_gate = (
            delta_hidden * up * sigmoid_gate * (1.0 + gate * (1.0 - sigmoid_gate))
        ).astype(bf16)
        delta_up = (delta_hidden * gate * sigmoid_gate).astype(bf16)
        activations, delta_gate, delta_up, near = (
            yield activations, delta_gate, delta_up, down_sums.parts[0]
        )
        down_sums.parts = (near, down_sums.parts[1])
        grad_gate = lax.dot_general(
            normed_mlp, delta_gate, over_rows, preferred_element_type=f32
        ).astype(bf16)
        grad_gate, delta_gate = yield grad_gate, delta_gate
        grad_up = lax.dot_general(
            normed_mlp, delta_up, over_rows, preferred_element_type=f32
        ).astype(bf16)
        grad_up, delta_up = yield grad_up, delta_up
        gate_up.append(grad_gate)
        gate_up.append(grad_up)
        parts = lax.dot_general(
            delta_gate, gate_proj, over_last, preferred_element_type=f32
        ) + lax.dot_general(delta_up, up_proj, over_last, preferred_element_type=f32)
        parts = yield parts
        delta_normed_mlp = scatter_group(ring, parts)
        yield ()
        delta_normed_mlp = yield Held(delta_normed_mlp)
        gain_mlp_part = jnp.sum(delta_normed_mlp * middle * mlp_scale, axis=0)
        weighted_mlp = mlp_gain * delta_normed_mlp
        delta_middle = (
            delta_result
            + mlp_scale * weighted_mlp
            - middle * mlp_scale**3 * jnp.mean(middle * weighted_mlp, axis=-1, keepdims=True)
        )
        attn_low_rows = gather_group(ring, delta_middle.astype(bf16))
        yield ()
        attn_low_rows = yield Held(attn_low_rows)
        grad_out_t = lax.dot_general(attn_low_rows, mixed, over_rows, preferred_element_type=f32)
        delta_mixed = (
            jnp.dot(attn_low_rows, out_proj_t, preferred_element_type=f32)
            .astype(bf16)
            .reshape(2, slots, query_heads, HEAD_SIZE)
        )
        grad_out_t, delta_mixed = yield Held(grad_out_t.astype(bf16), delta_mixed)
        probs_low = probs.astype(bf16)
        delta_probs = jnp.einsum("bigd,bjd->bgij", delta_mixed, values, preferred_element_type=f32)
        inner = jnp.sum(probs * delta_probs, axis=-1, keepdims=True)
        delta_scores = (probs * (delta_probs - inner)).astype(bf16)
        delta_values = jnp.einsum(
            "bgij,bigd->bjd", probs_low, delta_mixed, preferred_element_type=f32
        )
        delta_scores, delta_values = yield Held(delta_scores, delta_values)
        delta_qrot = (
            jnp.einsum("bgij,bjd->bigd", delta_scores, rot_keys, preferred_element_type=f32)
            * scaling
        )
        delta_krot = (
            jnp.einsum("bgij,bigd->bjd", delta_scores, rot_queries, preferred_element_type=f32)
            * scaling
        )
        delta_queries = rotate(delta_qrot, cosine, -sine).reshape(all_rows, q_width)
        delta_keys = rotate(delta_krot[:, :, None], cosine, -sine).reshape(all_rows, kv_width)
        delta_qkv = jnp.concatenate(
            [
                delta_queries.astype(bf16),
                delta_keys.astype(bf16),
                delta_values.astype(bf16).reshape(all_rows, kv_width),
            ],
            axis=1,
        )
        delta_qkv = yield delta_qkv
        grad_qkv = lax.dot_general(normed, delta_qkv, over_rows, preferred_element_type=f32)
        return (
            activations,
            gain_mlp_part,
            delta_middle,
            delta_qkv,
            [grad_qkv.astype(bf16), grad_out_t],
        )

    def finish(sums):
        low, high = sums.now
        kept = jnp.where(first_core, low, high)
        taken = ring.other_core(jnp.where(first_core, high, low).astype(bf16)).astype(f32)
        return kept, taken

    def whole(kept, taken):
        return jnp.concatenate(
            [jnp.where(first_core, kept, taken), jnp.where(first_core, taken, kept)], axis=1
        )

    def halves(grads):
        return [g[: width // 2] for g in grads], [g[width // 2 :] for g in grads]

    gate_up = []
    stages = Stages(backward())
    for k in range(3):
        stages.turn(down_sums)
    gate_up_sums = Scatter(ring, *halves(gate_up), piece)
    while down_sums.left:
        if gate_up_sums.left:
            stages.turn(gate_up_sums, down_sums)
        stages.turn(down_sums, gate_up_sums)
    down_grad = whole(*finish(down_sums)).T
    while not stages.over and gate_up_sums.left:
        down_grad = stages.turn(gate_up_sums, None, down_grad)
    assert stages.over
    activations, gain_mlp_part, delta_middle, delta_qkv, attn_grads = stages.finish()
    attn_sums = Scatter(ring, *halves(attn_grads), piece)

    def closing():
        delta_normed = scatter_group(
            ring, lax.dot_general(delta_qkv, qkv_proj, over_last, preferred_element_type=f32)
        )
        yield ()
        delta_normed = yield delta_normed
        gain_attn_part = jnp.sum(delta_normed * own_rows * attn_scale, axis=0)
        weighted_attn = attn_gain * delta_normed
        input_grad = (
            delta_middle
            + attn_scale * weighted_attn
            - own_rows * attn_scale**3 * jnp.mean(own_rows * weighted_attn, axis=-1, keepdims=True)
        )
        input_grad = reorder(input_grad.astype(bf16), to_natural)
        natural = jnp.stack([gain_mlp_part, gain_attn_part], axis=0).reshape(2, devices, piece)[
            :, to_natural
        ]
        sums = jnp.concatenate(
            [natural.reshape(2 * devices, piece), jnp.full((8, piece), squared)], axis=0
        )
        input_grad, sums = yield input_grad, sums
        totals = yield sum_all(ring, sums)
        return input_grad, totals

    stages = Stages(closing())
    while gate_up_sums.left:
        down_grad = stages.turn(gate_up_sums, attn_sums, down_grad)
        stages.turn(attn_sums, gate_up_sums)
    kept, taken = finish(gate_up_sums)
    gate_width = w_gate.shape[1] // 2
    gate_grad = whole(kept[:, :gate_width], taken[:, :gate_width])
    up_grad = whole(kept[:, gate_width:], taken[:, gate_width:])
    stages.turn(attn_sums)
    while attn_sums.left:
        gate_grad, up_grad = stages.turn(attn_sums, None, (gate_grad, up_grad))
    input_grad, totals = stages.finish()
    gain_mlp_grad = lax.dynamic_slice_in_dim(totals, me, 1, 0)[0]
    gain_attn_grad = lax.dynamic_slice_in_dim(totals, devices + me, 1, 0)[0]
    distill_loss = totals[2 * devices, 0] / (2.0 * width * count)
    attn_kept, attn_taken = finish(attn_sums)
    cuts = [0, q_width, q_width + kv_width, qkv_width, attn_kept.shape[1]]
    query_grad, key_grad, value_grad, out_grad_t = [
        whole(attn_kept[:, a:b], attn_taken[:, a:b]) for a, b in zip(cuts[:-1], cuts[1:])
    ]
    return (
        activations,
        input_grad,
        gain_attn_grad,
        query_grad,
        key_grad,
        value_grad,
        out_grad_t.T,
        gain_mlp_grad,
        gate_grad,
        up_grad,
        down_grad,
        distill_loss,
    )


def solution(mesh):
    placed = (
        P(("dp", "tensor"), None),
        P(("dp", "tensor"), None),
        P(),
        P(),
        P("dp"),
        P("dp", "tensor"),
        P("dp", "tensor"),
        P("dp", "tensor"),
        P("tensor", "dp"),
        P("dp"),
        P("dp", "tensor"),
        P("dp", "tensor"),
        P("tensor", "dp"),
    )
    return jax.shard_map(
        per_device,
        mesh=mesh,
        in_specs=placed,
        out_specs=(
            P(("dp", "tensor"), None),
            P(("dp", "tensor"), None),
            P("dp"),
            P("dp", "tensor"),
            P("dp", "tensor"),
            P("dp", "tensor"),
            P("tensor", "dp"),
            P("dp"),
            P("dp", "tensor"),
            P("dp", "tensor"),
            P("tensor", "dp"),
            P(),
        ),
        check_vma=False,
    )
```

```python
import jax
import jax.numpy as jnp
from jax import lax
from jax.experimental import pallas as pl
from jax.experimental.pallas import tpu as pltpu
from jax.sharding import PartitionSpec as P

HEAD_SIZE = 256
LANES = 128
EPS = 1e-06
ROPE_BASE = 1000042.0
over_rows = (((0,), (0,)), ((), ()))
over_last = (((1,), (1,)), ((), ()))
plain = (((1,), (0,)), ((), ()))
f32 = jnp.float32
bf16 = jnp.bfloat16


def rms_scale(value_rows):
    return lax.rsqrt(jnp.mean(value_rows * value_rows, axis=-1, keepdims=True) + EPS)


def rope_tables(position, width):
    half = width // 2
    exponent = jnp.arange(half, dtype=f32) * (-2.0 / width)
    frequency = jnp.exp(exponent * jnp.log(f32(ROPE_BASE)))
    angle = position.astype(f32)[..., None] * frequency
    return (jnp.cos(angle), jnp.sin(angle))


def rotate(heads, cosine, sine):
    half = heads.shape[-1] // 2
    first, second = heads[..., :half], heads[..., half:]
    return jnp.concatenate(
        [first * cosine - second * sine, second * cosine + first * sine], axis=-1
    )


def ring_order(chips):
    column = chips // 2
    return [2 * i for i in range(column)] + [2 * i + 1 for i in reversed(range(column))]


class Ring:
    def __init__(self, chips):
        self.chips = chips
        order = ring_order(chips)
        self.place = [order.index(c) for c in range(chips)]
        hop = [(order[i], order[(i + 1) % chips]) for i in range(chips)]
        self.up = [(2 * a + c, 2 * b + c) for a, b in hop for c in range(2)]
        self.down = [(b, a) for a, b in self.up]
        self.swap = [(d, d ^ 1) for d in range(2 * chips)]

    def ahead(self, v):
        return lax.ppermute(v, "dp", self.up)

    def back(self, v):
        return lax.ppermute(v, "dp", self.down)

    def other_core(self, v):
        return lax.ppermute(v, "dp", self.swap)


def other_tensor(v):
    return lax.ppermute(v, "tensor", [(0, 1), (1, 0)])


def together(values):
    return lax.optimization_barrier(values)


class Gather:
    def __init__(self, ring, low, high, rows, cuts=None, split=False, below=0):
        self.ring, self.size, self.split, self.below = ring, rows, split, below
        self.now = (low, high)
        self.cuts = cuts or [(0, low.shape[1])]
        height = 2 * ring.chips * rows
        if split:
            self.buffers = [jnp.zeros((height // 2, low.shape[1]), bf16)] * 2
        else:
            self.buffers = [jnp.zeros((height, b - a), bf16) for a, b in self.cuts]
        if below:
            self.buffers.append(jnp.zeros((below, height), bf16))
        self.hops = 0
        self.store()

    def store(self):
        half = self.ring.chips // 2
        k, self.hops = self.hops, self.hops + 1
        for side, rows in enumerate(self.now):
            at = k + (side - 1) * half if k >= half else k + (side + 2) * half
            if self.split:
                which = int(k < half)
                start = (at - which * 2 * half) * self.size
                self.buffers[which] = lax.dynamic_update_slice(
                    self.buffers[which], rows[: self.size], (start, 0)
                )
                continue
            for i, (a, b) in enumerate(self.cuts):
                self.buffers[i] = lax.dynamic_update_slice(
                    self.buffers[i], rows[: self.size, a:b], (at * self.size, 0)
                )
            if self.below:
                self.buffers[-1] = lax.dynamic_update_slice(
                    self.buffers[-1],
                    rows[self.size : self.size + self.below, : self.size],
                    (0, at * self.size),
                )

    def move(self):
        return self.ring.ahead(self.now[0]), self.ring.back(self.now[1])

    def take(self, moved):
        self.now = moved
        self.store()


class Scatter:
    def __init__(self, ring, far, near, rows):
        self.ring, self.parts, self.size = ring, (near, far), rows
        self.buffers = []
        self.left = ring.chips - 1
        self.now = (self.block(0), self.block(1))

    def block(self, side):
        half = self.ring.chips // 2
        grads = self.parts[self.left // half]
        start = (side * half + self.left % half) * self.size
        return jnp.concatenate([g[start : start + self.size] for g in grads], axis=1)

    def move(self):
        return self.ring.back(self.now[0]), self.ring.ahead(self.now[1])

    def take(self, moved):
        self.left -= 1
        sums = [m.astype(f32) + self.block(side).astype(f32) for side, m in enumerate(moved)]
        self.now = tuple(sums if self.left == 0 else [v.astype(bf16) for v in sums])


class Held:
    def __init__(self, *value):
        self.value = value if len(value) > 1 else value[0]


def turn(lane, other=None, values=(), held=()):
    moved, _, held, lane.buffers = together(
        (lane.move(), other.now if other else (), held, lane.buffers)
    )
    lane.take(moved)
    values, held, _ = together((values, held, lane.now))
    return values, held


class Stages:
    def __init__(self, generator):
        self.generator = generator
        self.result = None
        self.value = ()
        self.over = False
        self.advance(None)

    def advance(self, value):
        if not self.over:
            try:
                self.value = self.generator.send(value)
            except StopIteration as end:
                self.result, self.over, self.value = end.value, True, ()

    def turn(self, lane, other=None, extra=()):
        if isinstance(self.value, Held):
            extra, value = turn(lane, other, extra, self.value.value)
        else:
            (value, extra), _ = turn(lane, other, (self.value, extra))
        self.advance(value)
        return extra

    def finish(self):
        while not self.over:
            self.advance(self.value.value if isinstance(self.value, Held) else self.value)
        return self.result


def gather_group(ring, rows):
    across = other_tensor(rows)
    beside = ring.other_core(rows)
    return jnp.concatenate([rows, across, beside, ring.other_core(across)], axis=0)


def scatter_group(ring, parts, before=()):
    quarter = parts.shape[0] // 4
    near = parts[: 2 * quarter] + ring.other_core(parts[2 * quarter :].astype(bf16)).astype(f32)
    near = together((near, before))[0]
    return near[:quarter] + other_tensor(near[quarter:].astype(bf16)).astype(f32)


def copy_blocks(table, source, target):
    for k in range(target.shape[1] // LANES):
        start = pl.multiple_of(table[k] * LANES, LANES)
        target[:, k * LANES : (k + 1) * LANES] = source[:, pl.ds(start, LANES)]


def reorder(rows, table):
    height, width = rows.shape
    step = height // 4
    return pl.pallas_call(
        copy_blocks,
        out_shape=jax.ShapeDtypeStruct(rows.shape, rows.dtype),
        grid_spec=pltpu.PrefetchScalarGridSpec(
            num_scalar_prefetch=1,
            grid=(height // step,),
            in_specs=[pl.BlockSpec((step, width), lambda k, t: (k, 0))],
            out_specs=pl.BlockSpec((step, width), lambda k, t: (k, 0)),
        ),
        name="reorder",
    )(table, rows)


def sum_all(ring, v):
    v = v + other_tensor(v)
    devices = 2 * ring.chips
    step = 1
    while step < devices:
        v = v + lax.ppermute(v, "dp", [(d, d ^ step) for d in range(devices)])
        step *= 2
    return v


def per_device(
    layer_input,
    teacher,
    lengths,
    seq_order,
    gain_attn,
    w_query,
    key_projection_weight,
    value_projection_weight,
    w_out,
    gain_mlp,
    w_gate,
    w_up,
    w_down,
):
    token_rows, width = layer_input.shape
    slots = token_rows * lax.axis_size("tensor")
    devices = lax.axis_size("dp")
    tokens_all = slots * devices
    chips = devices // 2
    ring = Ring(chips)
    me = lax.axis_index("dp")
    side = lax.axis_index("tensor")
    chip, core = me // 2, me % 2
    first_core = core == 0
    place = jnp.array(ring.place, dtype=jnp.int32)
    here = place[chip]
    piece = gain_attn.shape[0]

    numbers = jnp.arange(chips, dtype=jnp.int32)
    order = jnp.array(ring_order(chips), dtype=jnp.int32)
    from_low = 2 * order[(here - numbers) % chips]
    from_high = 2 * order[(here + numbers) % chips] + 1
    half = chips // 2
    to_relative = jnp.concatenate(
        [from_low[half:], from_high[half:], from_low[:half], from_high[:half]]
    )
    behind, before = (here - place) % chips, (place - here) % chips
    to_natural = jnp.stack(
        [
            jnp.where(behind < half, behind + 2 * half, behind - half),
            jnp.where(before < half, before + 3 * half, before),
        ],
        axis=1,
    ).reshape(devices)

    def split_cores(w):
        quarter = w.shape[1] // 2
        mine = lax.dynamic_slice_in_dim(w, core * quarter, quarter, 1)
        given = lax.dynamic_slice_in_dim(w, (1 - core) * quarter, quarter, 1)
        return mine, given

    def both_rows(weights, gains=None):
        mine, given = zip(*[split_cores(w) for w in weights])
        mine, given = jnp.concatenate(mine, axis=1), jnp.concatenate(given, axis=1)
        if gains is not None:
            extra = jnp.pad(gains, ((0, 16 - gains.shape[0]), (0, mine.shape[1] - gains.shape[1])))
            mine = jnp.concatenate([mine, extra], axis=0)
            given = jnp.concatenate([given, extra], axis=0)
        taken = ring.other_core(given)
        return (
            jnp.where(first_core, mine, taken),
            jnp.where(first_core, taken, mine),
        )

    gains = jnp.stack([gain_attn, gain_mlp])
    hops = ring.chips - 1
    q_width = w_query.shape[1] // 2
    kv_width = key_projection_weight.shape[1] // 2
    qkv_width = q_width + 2 * kv_width
    out_width = w_out.shape[0] // 2
    attn_weights = Gather(
        ring,
        *both_rows([w_query, key_projection_weight, value_projection_weight, w_out.T], gains),
        piece,
        [(0, qkv_width), (qkv_width, qkv_width + out_width)],
        below=16,
    )
    gate_weights = Gather(ring, *both_rows([w_gate]), piece)
    own_input = reorder(layer_input, to_relative)
    group_rows = gather_group(ring, own_input)
    for k in range(hops):
        turn(attn_weights, gate_weights)
        turn(gate_weights, attn_weights)
    up_weights = Gather(ring, *together((both_rows([w_up]), attn_weights.now))[0], piece)
    down_weights = Gather(
        ring, *together((both_rows([w_down.T]), gate_weights.now))[0], piece, split=True
    )

    sequence_numbers = jnp.stack([me, me + 1 - 2 * core])
    length = jnp.sum(
        jnp.where(seq_order[None, :] == sequence_numbers[:, None], lengths[None, :], 0), axis=1
    )
    offsets = jnp.arange(token_rows, dtype=jnp.int32)
    slot = jnp.concatenate([side * token_rows + offsets, (1 - side) * token_rows + offsets])
    inside = slot[None, :] < length[:, None]
    sequence = jnp.where(inside, 0, 1 + slot[None, :])
    position = jnp.where(inside, slot[None, :], 0)
    own_valid = inside[0, :token_rows].astype(f32)[:, None]
    allowed = (sequence[:, :, None] == sequence[:, None, :]) & (
        position[:, None, :] <= position[:, :, None]
    )
    allowed = allowed[:, None]
    cosine, sine = rope_tables(position, HEAD_SIZE)
    cosine, sine = cosine[:, :, None, :], sine[:, :, None, :]
    scaling = HEAD_SIZE ** (-0.5)
    query_heads = q_width // HEAD_SIZE
    all_rows = 2 * slots
    own_rows = own_input.astype(f32)
    attn_scale = rms_scale(own_rows)

    qkv_proj, out_proj_t, gain_rows = attn_weights.buffers
    gain_rows = gain_rows[:2].astype(f32)
    attn_gain, mlp_gain = gain_rows[:1], gain_rows[1:]
    gate_proj = gate_weights.buffers[0]

    def forward():
        group_input = group_rows.astype(f32)
        normed = (group_input * rms_scale(group_input) * attn_gain).astype(bf16)
        qkv = jnp.dot(normed, qkv_proj, preferred_element_type=f32)
        normed, qkv = yield Held(normed, qkv)
        query_rows = qkv[:, :q_width].reshape(2, slots, query_heads, HEAD_SIZE)
        key_rows = qkv[:, q_width : q_width + kv_width].reshape(2, slots, 1, HEAD_SIZE)
        values = qkv[:, q_width + kv_width :].astype(bf16).reshape(2, slots, HEAD_SIZE)
        rot_queries = rotate(query_rows, cosine, sine).astype(bf16)
        rot_keys = rotate(key_rows, cosine, sine).astype(bf16)[:, :, 0]
        rot_queries, rot_keys, values = yield Held(rot_queries, rot_keys, values)
        scores = (
            jnp.einsum("bigd,bjd->bgij", rot_queries, rot_keys, preferred_element_type=f32)
            * scaling
        )
        scores = jnp.where(allowed, scores, -1e30)
        shifted = jnp.exp(scores - jnp.max(scores, axis=-1, keepdims=True))
        probs = shifted / jnp.sum(shifted, axis=-1, keepdims=True)
        probs = yield Held(probs)
        mixed = (
            jnp.einsum("bgij,bjd->bigd", probs.astype(bf16), values, preferred_element_type=f32)
            .reshape(all_rows, q_width)
            .astype(bf16)
        )
        parts = lax.dot_general(mixed, out_proj_t, over_last, preferred_element_type=f32)
        mixed, parts = yield Held(mixed, parts)
        shared = scatter_group(ring, parts)
        own_teacher = yield Held(reorder(teacher, to_relative))
        yield ()
        shared = yield Held(shared)
        middle = own_rows + shared
        mlp_scale = rms_scale(middle)
        normed_mlp = gather_group(ring, (middle * mlp_scale * mlp_gain).astype(bf16))
        yield ()
        yield ()
        normed_mlp = yield Held(normed_mlp)
        gate = jnp.dot(normed_mlp, gate_proj, preferred_element_type=f32)
        gate = yield Held(gate)
        return (
            own_teacher,
            (normed, rot_queries, rot_keys, values, probs, mixed),
            (middle, mlp_scale, normed_mlp, gate),
        )

    stages = Stages(forward())
    for k in range(hops):
        stages.turn(up_weights, down_weights)
        stages.turn(down_weights, up_weights)
    own_teacher, attn_kept, mlp_kept = stages.finish()
    normed, rot_queries, rot_keys, values, probs, mixed = attn_kept
    middle, mlp_scale, normed_mlp, gate = mlp_kept
    up_proj = up_weights.buffers[0]
    down_far, down_near = down_weights.buffers
    count = jnp.sum(lengths).astype(f32)

    up = jnp.dot(normed_mlp, up_proj, preferred_element_type=f32)
    sigmoid_gate = jax.nn.sigmoid(gate)
    hidden = (gate * sigmoid_gate * up).astype(bf16)
    cut = width // 2

    def output(proj_t, columns, before=()):
        parts = lax.dot_general(hidden, proj_t, over_last, preferred_element_type=f32)
        result = middle[:, columns] + scatter_group(ring, parts, before)
        error = (result - own_teacher[:, columns].astype(f32)) * own_valid
        delta = error * (tokens_all / count)
        return result, error, delta, gather_group(ring, delta.astype(bf16))

    def down_grad_of(branch):
        return lax.dot_general(branch, hidden, over_rows, preferred_element_type=f32).astype(bf16)

    result_far, error_far, delta_far, branch_far = output(down_far, slice(0, cut))
    result_near, error_near, delta_near, branch_near = output(down_near, slice(cut, width), delta_far)
    down_sums = Scatter(ring, [down_grad_of(branch_far)], None, piece)
    result = jnp.concatenate([result_far, result_near], axis=1)
    delta_result = jnp.concatenate([delta_far, delta_near], axis=1)
    squared = jnp.sum(error_far * error_far) + jnp.sum(error_near * error_near)

    def backward():
        first = jnp.dot(branch_far, down_far, preferred_element_type=f32)
        first = yield Held(first)
        delta_hidden = first + jnp.dot(branch_near, down_near, preferred_element_type=f32)
        delta_gate = (
            delta_hidden * up * sigmoid_gate * (1.0 + gate * (1.0 - sigmoid_gate))
        ).astype(bf16)
        delta_up = (delta_hidden * gate * sigmoid_gate).astype(bf16)
        delta_gate, delta_up = yield Held(delta_gate, delta_up)
        near = yield Held(down_grad_of(branch_near))
        down_sums.parts = ([near], down_sums.parts[1])
        grad_gate = lax.dot_general(
            normed_mlp, delta_gate, over_rows, preferred_element_type=f32
        ).astype(bf16)
        grad_gate = yield Held(grad_gate)
        grad_up = lax.dot_general(
            normed_mlp, delta_up, over_rows, preferred_element_type=f32
        ).astype(bf16)
        grad_up = yield Held(grad_up)
        gate_up.append(grad_gate)
        gate_up.append(grad_up)
        parts = lax.dot_general(
            delta_gate, gate_proj, over_last, preferred_element_type=f32
        ) + lax.dot_general(delta_up, up_proj, over_last, preferred_element_type=f32)
        parts = yield Held(parts)
        delta_normed_mlp = scatter_group(ring, parts)
        placed = together((result.astype(bf16), parts))[0]
        activations = yield Held(reorder(placed, to_natural))
        delta_normed_mlp = yield Held(delta_normed_mlp)
        gain_mlp_part = jnp.sum(delta_normed_mlp * middle * mlp_scale, axis=0)
        weighted_mlp = mlp_gain * delta_normed_mlp
        delta_middle = (
            delta_result
            + mlp_scale * weighted_mlp
            - middle * mlp_scale**3 * jnp.mean(middle * weighted_mlp, axis=-1, keepdims=True)
        )
        attn_low_rows = gather_group(ring, delta_middle.astype(bf16))
        yield ()
        attn_low_rows = yield Held(attn_low_rows)
        grad_out_t = lax.dot_general(attn_low_rows, mixed, over_rows, preferred_element_type=f32)
        delta_mixed = (
            jnp.dot(attn_low_rows, out_proj_t, preferred_element_type=f32)
            .astype(bf16)
            .reshape(2, slots, query_heads, HEAD_SIZE)
        )
        grad_out_t = grad_out_t.astype(bf16)
        probs_low = probs.astype(bf16)
        delta_probs = jnp.einsum("bigd,bjd->bgij", delta_mixed, values, preferred_element_type=f32)
        inner = jnp.sum(probs * delta_probs, axis=-1, keepdims=True)
        delta_scores = (probs * (delta_probs - inner)).astype(bf16)
        delta_values = jnp.einsum(
            "bgij,bigd->bjd", probs_low, delta_mixed, preferred_element_type=f32
        )
        grad_out_t, delta_scores, delta_values = yield Held(grad_out_t, delta_scores, delta_values)
        delta_qrot = (
            jnp.einsum("bgij,bjd->bigd", delta_scores, rot_keys, preferred_element_type=f32)
            * scaling
        )
        delta_krot = (
            jnp.einsum("bgij,bigd->bjd", delta_scores, rot_queries, preferred_element_type=f32)
            * scaling
        )
        delta_queries = rotate(delta_qrot, cosine, -sine).reshape(all_rows, q_width)
        delta_keys = rotate(delta_krot[:, :, None], cosine, -sine).reshape(all_rows, kv_width)
        delta_qkv = jnp.concatenate(
            [
                delta_queries.astype(bf16),
                delta_keys.astype(bf16),
                delta_values.astype(bf16).reshape(all_rows, kv_width),
            ],
            axis=1,
        )
        delta_qkv = yield Held(delta_qkv)
        grad_qkv = lax.dot_general(normed, delta_qkv, over_rows, preferred_element_type=f32)
        return (
            activations,
            gain_mlp_part,
            delta_middle,
            delta_qkv,
            [jnp.concatenate([grad_qkv.astype(bf16), grad_out_t], axis=1)],
        )

    def finish(sums):
        low, high = sums.now
        kept = jnp.where(first_core, low, high)
        taken = ring.other_core(jnp.where(first_core, high, low).astype(bf16)).astype(f32)
        return kept, taken

    def whole(kept, taken):
        return jnp.concatenate(
            [jnp.where(first_core, kept, taken), jnp.where(first_core, taken, kept)], axis=1
        )

    def halves(grads):
        return [g[: width // 2] for g in grads], [g[width // 2 :] for g in grads]

    gate_up = []
    stages = Stages(backward())
    for k in range(5):
        stages.turn(down_sums)
    gate_up_sums = Scatter(ring, *halves(gate_up), piece)
    while down_sums.left:
        if gate_up_sums.left:
            stages.turn(gate_up_sums, down_sums)
        stages.turn(down_sums, gate_up_sums)
    down_grad = whole(*finish(down_sums)).T
    while not stages.over and gate_up_sums.left:
        down_grad = stages.turn(gate_up_sums, None, down_grad)
    assert stages.over
    activations, gain_mlp_part, delta_middle, delta_qkv, attn_grads = stages.finish()
    attn_sums = Scatter(ring, *halves(attn_grads), piece)

    def closing():
        delta_normed = scatter_group(
            ring, lax.dot_general(delta_qkv, qkv_proj, over_last, preferred_element_type=f32)
        )
        yield ()
        delta_normed = yield delta_normed
        gain_attn_part = jnp.sum(delta_normed * own_rows * attn_scale, axis=0)
        weighted_attn = attn_gain * delta_normed
        input_grad = (
            delta_middle
            + attn_scale * weighted_attn
            - own_rows * attn_scale**3 * jnp.mean(own_rows * weighted_attn, axis=-1, keepdims=True)
        )
        input_grad = reorder(input_grad.astype(bf16), to_natural)
        natural = jnp.stack([gain_mlp_part, gain_attn_part], axis=0).reshape(2, devices, piece)[
            :, to_natural
        ]
        sums = jnp.concatenate(
            [natural.reshape(2 * devices, piece), jnp.full((8, piece), squared)], axis=0
        )
        input_grad, sums = yield input_grad, sums
        totals = yield sum_all(ring, sums)
        return input_grad, totals

    stages = Stages(closing())
    while gate_up_sums.left:
        down_grad = stages.turn(gate_up_sums, attn_sums, down_grad)
        stages.turn(attn_sums, gate_up_sums)
    kept, taken = finish(gate_up_sums)
    gate_width = w_gate.shape[1] // 2
    gate_grad = whole(kept[:, :gate_width], taken[:, :gate_width])
    up_grad = whole(kept[:, gate_width:], taken[:, gate_width:])
    stages.turn(attn_sums)
    while attn_sums.left:
        gate_grad, up_grad = stages.turn(attn_sums, None, (gate_grad, up_grad))
    input_grad, totals = stages.finish()
    gain_mlp_grad = lax.dynamic_slice_in_dim(totals, me, 1, 0)[0]
    gain_attn_grad = lax.dynamic_slice_in_dim(totals, devices + me, 1, 0)[0]
    distill_loss = totals[2 * devices, 0] / (2.0 * width * count)
    attn_kept, attn_taken = finish(attn_sums)
    cuts = [0, q_width, q_width + kv_width, qkv_width, attn_kept.shape[1]]
    query_grad, key_grad, value_grad, out_grad_t = [
        whole(attn_kept[:, a:b], attn_taken[:, a:b]) for a, b in zip(cuts[:-1], cuts[1:])
    ]
    return (
        activations,
        input_grad,
        gain_attn_grad,
        query_grad,
        key_grad,
        value_grad,
        out_grad_t.T,
        gain_mlp_grad,
        gate_grad,
        up_grad,
        down_grad,
        distill_loss,
    )


def solution(mesh):
    placed = (
        P(("dp", "tensor"), None),
        P(("dp", "tensor"), None),
        P(),
        P(),
        P("dp"),
        P("dp", "tensor"),
        P("dp", "tensor"),
        P("dp", "tensor"),
        P("tensor", "dp"),
        P("dp"),
        P("dp", "tensor"),
        P("dp", "tensor"),
        P("tensor", "dp"),
    )
    return jax.shard_map(
        per_device,
        mesh=mesh,
        in_specs=placed,
        out_specs=(
            P(("dp", "tensor"), None),
            P(("dp", "tensor"), None),
            P("dp"),
            P("dp", "tensor"),
            P("dp", "tensor"),
            P("dp", "tensor"),
            P("tensor", "dp"),
            P("dp"),
            P("dp", "tensor"),
            P("dp", "tensor"),
            P("tensor", "dp"),
            P(),
        ),
        check_vma=False,
    )
```

```python
import jax
import jax.numpy as jnp
from jax import lax
from jax.experimental import pallas as pl
from jax.experimental.pallas import tpu as pltpu
from jax.sharding import PartitionSpec as P

HEAD_SIZE = 256
LANES = 128
EPS = 1e-06
ROPE_BASE = 1000042.0
over_rows = (((0,), (0,)), ((), ()))
over_last = (((1,), (1,)), ((), ()))
plain = (((1,), (0,)), ((), ()))
f32 = jnp.float32
bf16 = jnp.bfloat16


def rms_scale(value_rows):
    return lax.rsqrt(jnp.mean(value_rows * value_rows, axis=-1, keepdims=True) + EPS)


def rope_tables(position, width):
    half = width // 2
    exponent = jnp.arange(half, dtype=f32) * (-2.0 / width)
    frequency = jnp.exp(exponent * jnp.log(f32(ROPE_BASE)))
    angle = position.astype(f32)[..., None] * frequency
    return (jnp.cos(angle), jnp.sin(angle))


def ring_order(chips):
    column = chips // 2
    return [2 * i for i in range(column)] + [2 * i + 1 for i in reversed(range(column))]


class Ring:
    def __init__(self, chips):
        self.chips = chips
        order = ring_order(chips)
        self.place = [order.index(c) for c in range(chips)]
        hop = [(order[i], order[(i + 1) % chips]) for i in range(chips)]
        self.up = [(2 * a + c, 2 * b + c) for a, b in hop for c in range(2)]
        self.down = [(b, a) for a, b in self.up]
        self.swap = [(d, d ^ 1) for d in range(2 * chips)]

    def ahead(self, v):
        return lax.ppermute(v, "dp", self.up)

    def back(self, v):
        return lax.ppermute(v, "dp", self.down)

    def other_core(self, v):
        return lax.ppermute(v, "dp", self.swap)


def other_tensor(v):
    return lax.ppermute(v, "tensor", [(0, 1), (1, 0)])


def together(values):
    return lax.optimization_barrier(values)


def unfilled(shape, name):
    return pl.pallas_call(
        lambda out: None,
        out_shape=jax.ShapeDtypeStruct(shape, bf16),
        out_specs=pl.BlockSpec(memory_space=pl.ANY),
        name=name,
    )()


class Gather:
    def __init__(self, ring, name, low, high, rows, cuts=None, split=False, below=0):
        self.ring, self.size, self.split, self.below = ring, rows, split, below
        self.now = (low, high)
        self.cuts = cuts or [(0, low.shape[1])]
        height = 2 * ring.chips * rows
        shapes = [(height, b - a) for a, b in self.cuts]
        if split:
            shapes = [(height // 2, low.shape[1])] * 2
        if below:
            shapes.append((below, height))
        self.buffers = [unfilled(v, f"{name}_{i}") for i, v in enumerate(shapes)]
        self.hops = 0
        self.store()

    def store(self):
        half = self.ring.chips // 2
        k, self.hops = self.hops, self.hops + 1
        for side, rows in enumerate(self.now):
            at = k + (side - 1) * half if k >= half else k + (side + 2) * half
            if self.split:
                which = int(k < half)
                start = (at - which * 2 * half) * self.size
                self.buffers[which] = lax.dynamic_update_slice(
                    self.buffers[which], rows[: self.size], (start, 0)
                )
                continue
            for i, (a, b) in enumerate(self.cuts):
                self.buffers[i] = lax.dynamic_update_slice(
                    self.buffers[i], rows[: self.size, a:b], (at * self.size, 0)
                )
            if self.below:
                self.buffers[-1] = lax.dynamic_update_slice(
                    self.buffers[-1],
                    rows[self.size : self.size + self.below, : self.size],
                    (0, at * self.size),
                )

    def move(self):
        return self.ring.ahead(self.now[0]), self.ring.back(self.now[1])

    def take(self, moved):
        self.now = moved
        self.store()


class Scatter:
    def __init__(self, ring, far, near, rows):
        self.ring, self.parts, self.size = ring, (near, far), rows
        self.buffers = []
        self.left = ring.chips - 1
        self.now = (self.block(0), self.block(1))

    def block(self, side):
        half = self.ring.chips // 2
        grads = self.parts[self.left // half]
        start = (side * half + self.left % half) * self.size
        return jnp.concatenate([g[start : start + self.size] for g in grads], axis=1)

    def move(self):
        return self.ring.back(self.now[0]), self.ring.ahead(self.now[1])

    def take(self, moved):
        self.left -= 1
        sums = [m.astype(f32) + self.block(side).astype(f32) for side, m in enumerate(moved)]
        self.now = tuple(sums if self.left == 0 else [v.astype(bf16) for v in sums])


class Held:
    def __init__(self, *value):
        self.value = value if len(value) > 1 else value[0]


def turn(lane, other=None, values=(), held=()):
    moved, _, held, lane.buffers = together(
        (lane.move(), other.now if other else (), held, lane.buffers)
    )
    lane.take(moved)
    values, held, _ = together((values, held, lane.now))
    return values, held


class Stages:
    def __init__(self, generator):
        self.generator = generator
        self.result = None
        self.value = ()
        self.over = False
        self.advance(None)

    def advance(self, value):
        if not self.over:
            try:
                self.value = self.generator.send(value)
            except StopIteration as end:
                self.result, self.over, self.value = end.value, True, ()

    def turn(self, lane, other=None, extra=()):
        if isinstance(self.value, Held):
            extra, value = turn(lane, other, extra, self.value.value)
        else:
            (value, extra), _ = turn(lane, other, (self.value, extra))
        self.advance(value)
        return extra

    def finish(self):
        while not self.over:
            self.advance(self.value.value if isinstance(self.value, Held) else self.value)
        return self.result


def gather_group(ring, rows):
    across = other_tensor(rows)
    beside = ring.other_core(rows)
    return jnp.concatenate([rows, across, beside, ring.other_core(across)], axis=0)


def scatter_group(ring, parts, before=()):
    quarter = parts.shape[0] // 4
    near = parts[: 2 * quarter] + ring.other_core(parts[2 * quarter :].astype(bf16)).astype(f32)
    near = together((near, before))[0]
    return near[:quarter] + other_tensor(near[quarter:].astype(bf16)).astype(f32)


def copy_blocks(table, source, target):
    for k in range(target.shape[1] // LANES):
        start = pl.multiple_of(table[k] * LANES, LANES)
        target[:, k * LANES : (k + 1) * LANES] = source[:, pl.ds(start, LANES)]


def reorder(rows, table):
    height, width = rows.shape
    step = height // 4
    return pl.pallas_call(
        copy_blocks,
        out_shape=jax.ShapeDtypeStruct(rows.shape, rows.dtype),
        grid_spec=pltpu.PrefetchScalarGridSpec(
            num_scalar_prefetch=1,
            grid=(height // step,),
            in_specs=[pl.BlockSpec((step, width), lambda k, t: (k, 0))],
            out_specs=pl.BlockSpec((step, width), lambda k, t: (k, 0)),
        ),
        name="reorder",
    )(table, rows)


def visible(numbers, shape):
    def slot(axis):
        offset = lax.broadcasted_iota(jnp.int32, shape, axis)
        start = numbers[2] * (shape[0] // 2)
        return jnp.where(offset < shape[0] // 2, offset + start, offset - start)

    query, key = slot(0), slot(1)
    inside = query < numbers[pl.program_id(0)]
    return jnp.where(inside, key - query, jnp.abs(key - query)) <= 0


def turned(heads, cosine, sine):
    half = heads.shape[1] // 2
    first, second = heads[:, :half], heads[:, half:]
    return first * cosine - second * sine, second * cosine + first * sine


def weights_of(queries, keys, allowed):
    scores = lax.dot_general(queries, keys, over_last, preferred_element_type=f32)
    scores = jnp.where(allowed, scores * HEAD_SIZE ** (-0.5), -1e30)
    shifted = jnp.exp(scores - jnp.max(scores, axis=-1, keepdims=True))
    return shifted / jnp.sum(shifted, axis=-1, keepdims=True)


def attend_body(numbers, qkv, cosine, sine, queries, keys, values, mixed):
    rows, width = queries.shape
    half = HEAD_SIZE // 2
    cosine, sine = cosine[...], sine[...]
    key_low, key_high = turned(qkv[:, width : width + HEAD_SIZE], cosine, sine)
    keys[:, :half] = key_low.astype(bf16)
    keys[:, half:] = key_high.astype(bf16)
    values[...] = qkv[:, width + HEAD_SIZE :].astype(bf16)
    allowed = visible(numbers, (rows, rows))
    for start in range(0, width, HEAD_SIZE):
        low, high = turned(qkv[:, start : start + HEAD_SIZE], cosine, sine)
        queries[:, start : start + half] = low.astype(bf16)
        queries[:, start + half : start + HEAD_SIZE] = high.astype(bf16)
        probs = weights_of(queries[:, start : start + HEAD_SIZE], keys[...], allowed)
        mixed[:, start : start + HEAD_SIZE] = jnp.dot(
            probs.astype(bf16), values[...], preferred_element_type=f32
        ).astype(bf16)


def attend_back_body(numbers, queries, keys, values, delta, cosine, sine, out):
    rows, width = queries.shape
    half = HEAD_SIZE // 2
    scaling = HEAD_SIZE ** (-0.5)
    cosine, sine = cosine[...], sine[...]
    allowed = visible(numbers, (rows, rows))
    delta_keys = jnp.zeros((rows, HEAD_SIZE), f32)
    delta_values = jnp.zeros((rows, HEAD_SIZE), f32)
    for start in range(0, width, HEAD_SIZE):
        head = queries[:, start : start + HEAD_SIZE]
        delta_mixed = delta[:, start : start + HEAD_SIZE]
        probs = weights_of(head, keys[...], allowed)
        delta_probs = lax.dot_general(
            delta_mixed, values[...], over_last, preferred_element_type=f32
        )
        inner = jnp.sum(probs * delta_probs, axis=-1, keepdims=True)
        delta_scores = (probs * (delta_probs - inner)).astype(bf16)
        delta_values += lax.dot_general(
            probs.astype(bf16), delta_mixed, over_rows, preferred_element_type=f32
        )
        delta_keys += lax.dot_general(delta_scores, head, over_rows, preferred_element_type=f32)
        delta_head = jnp.dot(delta_scores, keys[...], preferred_element_type=f32) * scaling
        low, high = turned(delta_head, cosine, -sine)
        out[:, start : start + half] = low.astype(bf16)
        out[:, start + half : start + HEAD_SIZE] = high.astype(bf16)
    low, high = turned(delta_keys * scaling, cosine, -sine)
    out[:, width : width + half] = low.astype(bf16)
    out[:, width + half : width + HEAD_SIZE] = high.astype(bf16)
    out[:, width + HEAD_SIZE :] = delta_values.astype(bf16)


def by_sequence(body, numbers, arrays, widths, name):
    rows = arrays[0].shape[0] // 2

    def spec(columns):
        return pl.BlockSpec((rows, columns), lambda b, n: (b, 0))

    return pl.pallas_call(
        body,
        out_shape=[jax.ShapeDtypeStruct((2 * rows, w), bf16) for w in widths],
        grid_spec=pltpu.PrefetchScalarGridSpec(
            num_scalar_prefetch=1,
            grid=(2,),
            in_specs=[spec(v.shape[1]) for v in arrays],
            out_specs=[spec(w) for w in widths],
        ),
        name=name,
    )(numbers, *arrays)


def sum_all(ring, v):
    v = v + other_tensor(v)
    devices = 2 * ring.chips
    step = 1
    while step < devices:
        v = v + lax.ppermute(v, "dp", [(d, d ^ step) for d in range(devices)])
        step *= 2
    return v


def per_device(
    layer_input,
    teacher,
    lengths,
    seq_order,
    gain_attn,
    w_query,
    key_projection_weight,
    value_projection_weight,
    w_out,
    gain_mlp,
    w_gate,
    w_up,
    w_down,
):
    token_rows, width = layer_input.shape
    slots = token_rows * lax.axis_size("tensor")
    devices = lax.axis_size("dp")
    tokens_all = slots * devices
    chips = devices // 2
    ring = Ring(chips)
    me = lax.axis_index("dp")
    side = lax.axis_index("tensor")
    chip, core = me // 2, me % 2
    first_core = core == 0
    place = jnp.array(ring.place, dtype=jnp.int32)
    here = place[chip]
    piece = gain_attn.shape[0]

    numbers = jnp.arange(chips, dtype=jnp.int32)
    order = jnp.array(ring_order(chips), dtype=jnp.int32)
    from_low = 2 * order[(here - numbers) % chips]
    from_high = 2 * order[(here + numbers) % chips] + 1
    half = chips // 2
    to_relative = jnp.concatenate(
        [from_low[half:], from_high[half:], from_low[:half], from_high[:half]]
    )
    behind, before = (here - place) % chips, (place - here) % chips
    to_natural = jnp.stack(
        [
            jnp.where(behind < half, behind + 2 * half, behind - half),
            jnp.where(before < half, before + 3 * half, before),
        ],
        axis=1,
    ).reshape(devices)

    def split_cores(w):
        quarter = w.shape[1] // 2
        mine = lax.dynamic_slice_in_dim(w, core * quarter, quarter, 1)
        given = lax.dynamic_slice_in_dim(w, (1 - core) * quarter, quarter, 1)
        return mine, given

    def both_rows(weights, gains=None):
        mine, given = zip(*[split_cores(w) for w in weights])
        mine, given = jnp.concatenate(mine, axis=1), jnp.concatenate(given, axis=1)
        if gains is not None:
            extra = jnp.pad(gains, ((0, 16 - gains.shape[0]), (0, mine.shape[1] - gains.shape[1])))
            mine = jnp.concatenate([mine, extra], axis=0)
            given = jnp.concatenate([given, extra], axis=0)
        taken = ring.other_core(given)
        return (
            jnp.where(first_core, mine, taken),
            jnp.where(first_core, taken, mine),
        )

    gains = jnp.stack([gain_attn, gain_mlp])
    hops = ring.chips - 1
    q_width = w_query.shape[1] // 2
    kv_width = key_projection_weight.shape[1] // 2
    qkv_width = q_width + 2 * kv_width
    out_width = w_out.shape[0] // 2
    attn_weights = Gather(
        ring,
        "attn_rows",
        *both_rows([w_query, key_projection_weight, value_projection_weight, w_out.T], gains),
        piece,
        [(0, qkv_width), (qkv_width, qkv_width + out_width)],
        below=16,
    )
    w_gate, layer_input, to_relative, lengths, _ = together(
        (w_gate, layer_input, to_relative, lengths, attn_weights.now)
    )
    gate_weights = Gather(ring, "gate_rows", *both_rows([w_gate]), piece)
    own_input = reorder(layer_input, to_relative)
    group_rows = gather_group(ring, own_input)
    for k in range(hops):
        turn(attn_weights, gate_weights)
        turn(gate_weights, attn_weights)
    up_weights = Gather(
        ring, "up_rows", *together((both_rows([w_up]), attn_weights.now))[0], piece
    )
    down_weights = Gather(
        ring, "down_rows", *together((both_rows([w_down.T]), gate_weights.now))[0], piece, split=True
    )

    sequence_numbers = jnp.stack([me, me + 1 - 2 * core])
    length = jnp.sum(
        jnp.where(seq_order[None, :] == sequence_numbers[:, None], lengths[None, :], 0), axis=1
    )
    offsets = jnp.arange(token_rows, dtype=jnp.int32)
    slot = jnp.concatenate([side * token_rows + offsets, (1 - side) * token_rows + offsets])
    inside = slot[None, :] < length[:, None]
    position = jnp.where(inside, slot[None, :], 0)
    own_valid = inside[0, :token_rows].astype(f32)[:, None]
    cosine, sine = rope_tables(position.reshape(-1), HEAD_SIZE)
    numbers = jnp.concatenate([length, side[None]]).astype(jnp.int32)
    own_rows = own_input.astype(f32)
    attn_scale = rms_scale(own_rows)

    qkv_proj, out_proj_t, gain_rows = attn_weights.buffers
    gain_rows = gain_rows[:2].astype(f32)
    attn_gain, mlp_gain = gain_rows[:1], gain_rows[1:]
    gate_proj = gate_weights.buffers[0]

    def forward():
        group_input = group_rows.astype(f32)
        normed = (group_input * rms_scale(group_input) * attn_gain).astype(bf16)
        qkv = jnp.dot(normed, qkv_proj, preferred_element_type=f32)
        normed, qkv = yield Held(normed, qkv)
        attended = by_sequence(
            attend_body,
            numbers,
            [qkv, cosine, sine],
            [q_width, kv_width, kv_width, q_width],
            "attend",
        )
        attended = yield Held(attended)
        parts = lax.dot_general(attended[3], out_proj_t, over_last, preferred_element_type=f32)
        parts = yield Held(parts)
        shared = scatter_group(ring, parts)
        own_teacher = yield Held(reorder(teacher, to_relative))
        yield ()
        shared = yield Held(shared)
        middle = own_rows + shared
        mlp_scale = rms_scale(middle)
        normed_mlp = gather_group(ring, (middle * mlp_scale * mlp_gain).astype(bf16))
        yield ()
        yield ()
        normed_mlp = yield Held(normed_mlp)
        gate = jnp.dot(normed_mlp, gate_proj, preferred_element_type=f32)
        gate = yield Held(gate)
        return (
            own_teacher,
            (normed, *attended),
            (middle, mlp_scale, normed_mlp, gate),
        )

    stages = Stages(forward())
    for k in range(hops):
        stages.turn(up_weights, down_weights)
        stages.turn(down_weights, up_weights)
    own_teacher, attn_kept, mlp_kept = stages.finish()
    normed, rot_queries, rot_keys, values, mixed = attn_kept
    middle, mlp_scale, normed_mlp, gate = mlp_kept
    up_proj = up_weights.buffers[0]
    down_far, down_near = down_weights.buffers
    count = jnp.sum(lengths).astype(f32)

    up = jnp.dot(normed_mlp, up_proj, preferred_element_type=f32)
    sigmoid_gate = jax.nn.sigmoid(gate)
    hidden = (gate * sigmoid_gate * up).astype(bf16)
    cut = width // 2

    def output(proj_t, columns, before=()):
        parts = lax.dot_general(hidden, proj_t, over_last, preferred_element_type=f32)
        result = middle[:, columns] + scatter_group(ring, parts, before)
        error = (result - own_teacher[:, columns].astype(f32)) * own_valid
        delta = error * (tokens_all / count)
        return result, error, delta, gather_group(ring, delta.astype(bf16))

    def down_grad_of(branch):
        return lax.dot_general(branch, hidden, over_rows, preferred_element_type=f32).astype(bf16)

    result_far, error_far, delta_far, branch_far = output(down_far, slice(0, cut))
    result_near, error_near, delta_near, branch_near = output(down_near, slice(cut, width), delta_far)
    down_sums = Scatter(ring, [down_grad_of(branch_far)], None, piece)
    result = jnp.concatenate([result_far, result_near], axis=1)
    delta_result = jnp.concatenate([delta_far, delta_near], axis=1)
    squared = jnp.sum(error_far * error_far) + jnp.sum(error_near * error_near)

    def backward():
        first = jnp.dot(branch_far, down_far, preferred_element_type=f32)
        first = yield Held(first)
        delta_hidden = first + jnp.dot(branch_near, down_near, preferred_element_type=f32)
        delta_gate = (
            delta_hidden * up * sigmoid_gate * (1.0 + gate * (1.0 - sigmoid_gate))
        ).astype(bf16)
        delta_up = (delta_hidden * gate * sigmoid_gate).astype(bf16)
        delta_gate, delta_up = yield Held(delta_gate, delta_up)
        near = yield Held(down_grad_of(branch_near))
        down_sums.parts = ([near], down_sums.parts[1])
        grad_gate = lax.dot_general(
            normed_mlp, delta_gate, over_rows, preferred_element_type=f32
        ).astype(bf16)
        grad_gate = yield Held(grad_gate)
        grad_up = lax.dot_general(
            normed_mlp, delta_up, over_rows, preferred_element_type=f32
        ).astype(bf16)
        grad_up = yield Held(grad_up)
        gate_up.append(grad_gate)
        gate_up.append(grad_up)
        parts = lax.dot_general(
            delta_gate, gate_proj, over_last, preferred_element_type=f32
        ) + lax.dot_general(delta_up, up_proj, over_last, preferred_element_type=f32)
        parts = yield Held(parts)
        delta_normed_mlp = scatter_group(ring, parts)
        placed = together((result.astype(bf16), parts))[0]
        activations = yield Held(reorder(placed, to_natural))
        delta_normed_mlp = yield Held(delta_normed_mlp)
        gain_mlp_part = jnp.sum(delta_normed_mlp * middle * mlp_scale, axis=0)
        weighted_mlp = mlp_gain * delta_normed_mlp
        delta_middle = (
            delta_result
            + mlp_scale * weighted_mlp
            - middle * mlp_scale**3 * jnp.mean(middle * weighted_mlp, axis=-1, keepdims=True)
        )
        attn_low_rows = gather_group(ring, delta_middle.astype(bf16))
        yield ()
        attn_low_rows = yield Held(attn_low_rows)
        grad_out_t = lax.dot_general(attn_low_rows, mixed, over_rows, preferred_element_type=f32)
        delta_mixed = jnp.dot(attn_low_rows, out_proj_t, preferred_element_type=f32).astype(bf16)
        grad_out_t = grad_out_t.astype(bf16)
        delta_qkv = by_sequence(
            attend_back_body,
            numbers,
            [rot_queries, rot_keys, values, delta_mixed, cosine, sine],
            [qkv_width],
            "attend_back",
        )[0]
        delta_qkv, grad_out_t = yield Held(delta_qkv, grad_out_t)
        grad_qkv = lax.dot_general(normed, delta_qkv, over_rows, preferred_element_type=f32)
        return (
            activations,
            gain_mlp_part,
            delta_middle,
            delta_qkv,
            [jnp.concatenate([grad_qkv.astype(bf16), grad_out_t], axis=1)],
        )

    def finish(sums):
        low, high = sums.now
        kept = jnp.where(first_core, low, high)
        taken = ring.other_core(jnp.where(first_core, high, low).astype(bf16)).astype(f32)
        return kept, taken

    def whole(kept, taken):
        return jnp.concatenate(
            [jnp.where(first_core, kept, taken), jnp.where(first_core, taken, kept)], axis=1
        )

    def halves(grads):
        return [g[: width // 2] for g in grads], [g[width // 2 :] for g in grads]

    gate_up = []
    stages = Stages(backward())
    for k in range(5):
        stages.turn(down_sums)
    gate_up_sums = Scatter(ring, *halves(gate_up), piece)
    while down_sums.left:
        if gate_up_sums.left:
            stages.turn(gate_up_sums, down_sums)
        stages.turn(down_sums, gate_up_sums)
    down_grad = whole(*finish(down_sums)).T
    while not stages.over and gate_up_sums.left:
        down_grad = stages.turn(gate_up_sums, None, down_grad)
    assert stages.over
    activations, gain_mlp_part, delta_middle, delta_qkv, attn_grads = stages.finish()
    attn_sums = Scatter(ring, *halves(attn_grads), piece)

    def closing():
        delta_normed = scatter_group(
            ring, lax.dot_general(delta_qkv, qkv_proj, over_last, preferred_element_type=f32)
        )
        yield ()
        delta_normed = yield delta_normed
        gain_attn_part = jnp.sum(delta_normed * own_rows * attn_scale, axis=0)
        weighted_attn = attn_gain * delta_normed
        input_grad = (
            delta_middle
            + attn_scale * weighted_attn
            - own_rows * attn_scale**3 * jnp.mean(own_rows * weighted_attn, axis=-1, keepdims=True)
        )
        input_grad = reorder(input_grad.astype(bf16), to_natural)
        natural = jnp.stack([gain_mlp_part, gain_attn_part], axis=0).reshape(2, devices, piece)[
            :, to_natural
        ]
        sums = jnp.concatenate(
            [natural.reshape(2 * devices, piece), jnp.full((8, piece), squared)], axis=0
        )
        input_grad, sums = yield input_grad, sums
        totals = yield sum_all(ring, sums)
        return input_grad, totals

    stages = Stages(closing())
    while gate_up_sums.left:
        down_grad = stages.turn(gate_up_sums, attn_sums, down_grad)
        stages.turn(attn_sums, gate_up_sums)
    kept, taken = finish(gate_up_sums)
    gate_width = w_gate.shape[1] // 2
    gate_grad = whole(kept[:, :gate_width], taken[:, :gate_width])
    up_grad = whole(kept[:, gate_width:], taken[:, gate_width:])
    stages.turn(attn_sums)
    while attn_sums.left:
        gate_grad, up_grad = stages.turn(attn_sums, None, (gate_grad, up_grad))
    input_grad, totals = stages.finish()
    gain_mlp_grad = lax.dynamic_slice_in_dim(totals, me, 1, 0)[0]
    gain_attn_grad = lax.dynamic_slice_in_dim(totals, devices + me, 1, 0)[0]
    distill_loss = totals[2 * devices, 0] / (2.0 * width * count)
    attn_kept, attn_taken = finish(attn_sums)
    cuts = [0, q_width, q_width + kv_width, qkv_width, attn_kept.shape[1]]
    query_grad, key_grad, value_grad, out_grad_t = [
        whole(attn_kept[:, a:b], attn_taken[:, a:b]) for a, b in zip(cuts[:-1], cuts[1:])
    ]
    return (
        activations,
        input_grad,
        gain_attn_grad,
        query_grad,
        key_grad,
        value_grad,
        out_grad_t.T,
        gain_mlp_grad,
        gate_grad,
        up_grad,
        down_grad,
        distill_loss,
    )


def solution(mesh):
    placed = (
        P(("dp", "tensor"), None),
        P(("dp", "tensor"), None),
        P(),
        P(),
        P("dp"),
        P("dp", "tensor"),
        P("dp", "tensor"),
        P("dp", "tensor"),
        P("tensor", "dp"),
        P("dp"),
        P("dp", "tensor"),
        P("dp", "tensor"),
        P("tensor", "dp"),
    )
    return jax.shard_map(
        per_device,
        mesh=mesh,
        in_specs=placed,
        out_specs=(
            P(("dp", "tensor"), None),
            P(("dp", "tensor"), None),
            P("dp"),
            P("dp", "tensor"),
            P("dp", "tensor"),
            P("dp", "tensor"),
            P("tensor", "dp"),
            P("dp"),
            P("dp", "tensor"),
            P("dp", "tensor"),
            P("tensor", "dp"),
            P(),
        ),
        check_vma=False,
    )
```

```python
import jax
import jax.numpy as jnp
from jax import lax
from jax.experimental import pallas as pl
from jax.experimental.pallas import tpu as pltpu
from jax.sharding import PartitionSpec as P

HEAD_SIZE = 256
LANES = 128
EPS = 1e-06
ROPE_BASE = 1000042.0
over_rows = (((0,), (0,)), ((), ()))
over_last = (((1,), (1,)), ((), ()))
plain = (((1,), (0,)), ((), ()))
f32 = jnp.float32
bf16 = jnp.bfloat16


def rms_scale(value_rows):
    return lax.rsqrt(jnp.mean(value_rows * value_rows, axis=-1, keepdims=True) + EPS)


def rope_tables(position, width):
    half = width // 2
    exponent = jnp.arange(half, dtype=f32) * (-2.0 / width)
    frequency = jnp.exp(exponent * jnp.log(f32(ROPE_BASE)))
    angle = position.astype(f32)[..., None] * frequency
    return (jnp.cos(angle), jnp.sin(angle))


def ring_order(chips):
    column = chips // 2
    return [2 * i for i in range(column)] + [2 * i + 1 for i in reversed(range(column))]


class Ring:
    def __init__(self, chips):
        self.chips = chips
        order = ring_order(chips)
        self.place = [order.index(c) for c in range(chips)]
        hop = [(order[i], order[(i + 1) % chips]) for i in range(chips)]
        self.up = [(2 * a + c, 2 * b + c) for a, b in hop for c in range(2)]
        self.down = [(b, a) for a, b in self.up]
        self.swap = [(d, d ^ 1) for d in range(2 * chips)]

    def ahead(self, v):
        return lax.ppermute(v, "dp", self.up)

    def back(self, v):
        return lax.ppermute(v, "dp", self.down)

    def other_core(self, v):
        return lax.ppermute(v, "dp", self.swap)


def other_tensor(v):
    return lax.ppermute(v, "tensor", [(0, 1), (1, 0)])


def together(values):
    return lax.optimization_barrier(values)


def unfilled(shape, name):
    return pl.pallas_call(
        lambda out: None,
        out_shape=jax.ShapeDtypeStruct(shape, bf16),
        out_specs=pl.BlockSpec(memory_space=pl.ANY),
        name=name,
    )()


class Gather:
    def __init__(self, ring, name, low, high, rows, cuts=None, split=False, below=0):
        self.ring, self.size, self.split, self.below = ring, rows, split, below
        self.now = (low, high)
        self.cuts = cuts or [(0, low.shape[1])]
        height = 2 * ring.chips * rows
        shapes = [(height, b - a) for a, b in self.cuts]
        if split:
            shapes = [(height // 2, low.shape[1])] * 2
        if below:
            shapes.append((below, height))
        self.buffers = [unfilled(v, f"{name}_{i}") for i, v in enumerate(shapes)]
        self.hops = 0
        self.store()

    def store(self):
        half = self.ring.chips // 2
        k, self.hops = self.hops, self.hops + 1
        for side, rows in enumerate(self.now):
            at = k + (side - 1) * half if k >= half else k + (side + 2) * half
            if self.split:
                which = int(k < half)
                start = (at - which * 2 * half) * self.size
                self.buffers[which] = lax.dynamic_update_slice(
                    self.buffers[which], rows[: self.size], (start, 0)
                )
                continue
            for i, (a, b) in enumerate(self.cuts):
                self.buffers[i] = lax.dynamic_update_slice(
                    self.buffers[i], rows[: self.size, a:b], (at * self.size, 0)
                )
            if self.below:
                self.buffers[-1] = lax.dynamic_update_slice(
                    self.buffers[-1],
                    rows[self.size : self.size + self.below, : self.size],
                    (0, at * self.size),
                )

    def move(self):
        return self.ring.ahead(self.now[0]), self.ring.back(self.now[1])

    def take(self, moved):
        self.now = moved
        self.store()


class Scatter:
    def __init__(self, ring, far, near, rows):
        self.ring, self.parts, self.size = ring, (near, far), rows
        self.buffers = []
        self.left = ring.chips - 1
        self.now = (self.block(0), self.block(1))

    def block(self, side):
        half = self.ring.chips // 2
        grads = self.parts[self.left // half]
        start = (side * half + self.left % half) * self.size
        return jnp.concatenate([g[start : start + self.size] for g in grads], axis=1)

    def move(self):
        return self.ring.back(self.now[0]), self.ring.ahead(self.now[1])

    def take(self, moved):
        self.left -= 1
        sums = [m.astype(f32) + self.block(side).astype(f32) for side, m in enumerate(moved)]
        self.now = tuple(sums if self.left == 0 else [v.astype(bf16) for v in sums])


class Held:
    def __init__(self, *value):
        self.value = value if len(value) > 1 else value[0]


def turn(lane, other=None, values=(), held=()):
    moved, _, held, lane.buffers = together(
        (lane.move(), other.now if other else (), held, lane.buffers)
    )
    lane.take(moved)
    values, held, _ = together((values, held, lane.now))
    return values, held


class Stages:
    def __init__(self, generator):
        self.generator = generator
        self.result = None
        self.value = ()
        self.over = False
        self.advance(None)

    def advance(self, value):
        if not self.over:
            try:
                self.value = self.generator.send(value)
            except StopIteration as end:
                self.result, self.over, self.value = end.value, True, ()

    def turn(self, lane, other=None, extra=()):
        if isinstance(self.value, Held):
            extra, value = turn(lane, other, extra, self.value.value)
        else:
            (value, extra), _ = turn(lane, other, (self.value, extra))
        self.advance(value)
        return extra

    def finish(self):
        while not self.over:
            self.advance(self.value.value if isinstance(self.value, Held) else self.value)
        return self.result


def gather_group(ring, rows):
    across = other_tensor(rows)
    beside = ring.other_core(rows)
    return jnp.concatenate([rows, across, beside, ring.other_core(across)], axis=0)


def core_sum(ring, parts):
    half = parts.shape[0] // 2
    return parts[:half] + ring.other_core(parts[half:].astype(bf16)).astype(f32)


def tensor_sum(rows):
    half = rows.shape[0] // 2
    return rows[:half] + other_tensor(rows[half:].astype(bf16)).astype(f32)


def scatter_group(ring, parts):
    return tensor_sum(core_sum(ring, parts))


def copy_blocks(table, source, target):
    for k in range(target.shape[1] // LANES):
        start = pl.multiple_of(table[k] * LANES, LANES)
        target[:, k * LANES : (k + 1) * LANES] = source[:, pl.ds(start, LANES)]


def reorder(rows, table):
    height, width = rows.shape
    step = height // 4
    return pl.pallas_call(
        copy_blocks,
        out_shape=jax.ShapeDtypeStruct(rows.shape, rows.dtype),
        grid_spec=pltpu.PrefetchScalarGridSpec(
            num_scalar_prefetch=1,
            grid=(height // step,),
            in_specs=[pl.BlockSpec((step, width), lambda k, t: (k, 0))],
            out_specs=pl.BlockSpec((step, width), lambda k, t: (k, 0)),
        ),
        name="reorder",
    )(table, rows)


def visible(numbers, shape):
    def slot(axis):
        offset = lax.broadcasted_iota(jnp.int32, shape, axis)
        start = numbers[2] * (shape[0] // 2)
        return jnp.where(offset < shape[0] // 2, offset + start, offset - start)

    query, key = slot(0), slot(1)
    inside = query < numbers[pl.program_id(0)]
    return jnp.where(inside, key - query, jnp.abs(key - query)) <= 0


def turned(heads, cosine, sine):
    half = heads.shape[1] // 2
    first, second = heads[:, :half], heads[:, half:]
    return first * cosine - second * sine, second * cosine + first * sine


def weights_of(queries, keys, allowed):
    scores = lax.dot_general(queries, keys, over_last, preferred_element_type=f32)
    scores = jnp.where(allowed, scores * HEAD_SIZE ** (-0.5), -1e30)
    shifted = jnp.exp(scores - jnp.max(scores, axis=-1, keepdims=True))
    return shifted / jnp.sum(shifted, axis=-1, keepdims=True)


def attend_body(numbers, qkv, cosine, sine, queries, keys, values, mixed):
    rows, width = queries.shape
    half = HEAD_SIZE // 2
    cosine, sine = cosine[...], sine[...]
    key_low, key_high = turned(qkv[:, width : width + HEAD_SIZE], cosine, sine)
    keys[:, :half] = key_low.astype(bf16)
    keys[:, half:] = key_high.astype(bf16)
    values[...] = qkv[:, width + HEAD_SIZE :].astype(bf16)
    allowed = visible(numbers, (rows, rows))
    for start in range(0, width, HEAD_SIZE):
        low, high = turned(qkv[:, start : start + HEAD_SIZE], cosine, sine)
        queries[:, start : start + half] = low.astype(bf16)
        queries[:, start + half : start + HEAD_SIZE] = high.astype(bf16)
        probs = weights_of(queries[:, start : start + HEAD_SIZE], keys[...], allowed)
        mixed[:, start : start + HEAD_SIZE] = jnp.dot(
            probs.astype(bf16), values[...], preferred_element_type=f32
        ).astype(bf16)


def attend_back_body(numbers, queries, keys, values, delta, cosine, sine, out):
    rows, width = queries.shape
    half = HEAD_SIZE // 2
    scaling = HEAD_SIZE ** (-0.5)
    cosine, sine = cosine[...], sine[...]
    allowed = visible(numbers, (rows, rows))
    delta_keys = jnp.zeros((rows, HEAD_SIZE), f32)
    delta_values = jnp.zeros((rows, HEAD_SIZE), f32)
    for start in range(0, width, HEAD_SIZE):
        head = queries[:, start : start + HEAD_SIZE]
        delta_mixed = delta[:, start : start + HEAD_SIZE]
        probs = weights_of(head, keys[...], allowed)
        delta_probs = lax.dot_general(
            delta_mixed, values[...], over_last, preferred_element_type=f32
        )
        inner = jnp.sum(probs * delta_probs, axis=-1, keepdims=True)
        delta_scores = (probs * (delta_probs - inner)).astype(bf16)
        delta_values += lax.dot_general(
            probs.astype(bf16), delta_mixed, over_rows, preferred_element_type=f32
        )
        delta_keys += lax.dot_general(delta_scores, head, over_rows, preferred_element_type=f32)
        delta_head = jnp.dot(delta_scores, keys[...], preferred_element_type=f32) * scaling
        low, high = turned(delta_head, cosine, -sine)
        out[:, start : start + half] = low.astype(bf16)
        out[:, start + half : start + HEAD_SIZE] = high.astype(bf16)
    low, high = turned(delta_keys * scaling, cosine, -sine)
    out[:, width : width + half] = low.astype(bf16)
    out[:, width + half : width + HEAD_SIZE] = high.astype(bf16)
    out[:, width + HEAD_SIZE :] = delta_values.astype(bf16)


def by_sequence(body, numbers, arrays, widths, name):
    rows = arrays[0].shape[0] // 2

    def spec(columns):
        return pl.BlockSpec((rows, columns), lambda b, n: (b, 0))

    return pl.pallas_call(
        body,
        out_shape=[jax.ShapeDtypeStruct((2 * rows, w), bf16) for w in widths],
        grid_spec=pltpu.PrefetchScalarGridSpec(
            num_scalar_prefetch=1,
            grid=(2,),
            in_specs=[spec(v.shape[1]) for v in arrays],
            out_specs=[spec(w) for w in widths],
        ),
        name=name,
    )(numbers, *arrays)


def per_device(
    layer_input,
    teacher,
    lengths,
    seq_order,
    gain_attn,
    w_query,
    key_projection_weight,
    value_projection_weight,
    w_out,
    gain_mlp,
    w_gate,
    w_up,
    w_down,
):
    token_rows, width = layer_input.shape
    slots = token_rows * lax.axis_size("tensor")
    devices = lax.axis_size("dp")
    tokens_all = slots * devices
    chips = devices // 2
    ring = Ring(chips)
    me = lax.axis_index("dp")
    side = lax.axis_index("tensor")
    chip, core = me // 2, me % 2
    first_core = core == 0
    place = jnp.array(ring.place, dtype=jnp.int32)
    here = place[chip]
    piece = gain_attn.shape[0]

    numbers = jnp.arange(chips, dtype=jnp.int32)
    order = jnp.array(ring_order(chips), dtype=jnp.int32)
    from_low = 2 * order[(here - numbers) % chips]
    from_high = 2 * order[(here + numbers) % chips] + 1
    half = chips // 2
    to_relative = jnp.concatenate(
        [from_low[half:], from_high[half:], from_low[:half], from_high[:half]]
    )
    behind, before = (here - place) % chips, (place - here) % chips
    to_natural = jnp.stack(
        [
            jnp.where(behind < half, behind + 2 * half, behind - half),
            jnp.where(before < half, before + 3 * half, before),
        ],
        axis=1,
    ).reshape(devices)

    def split_cores(w):
        quarter = w.shape[1] // 2
        mine = lax.dynamic_slice_in_dim(w, core * quarter, quarter, 1)
        given = lax.dynamic_slice_in_dim(w, (1 - core) * quarter, quarter, 1)
        return mine, given

    def both_rows(weights, gains=None):
        mine, given = zip(*[split_cores(w) for w in weights])
        mine, given = jnp.concatenate(mine, axis=1), jnp.concatenate(given, axis=1)
        if gains is not None:
            extra = jnp.pad(gains, ((0, 16 - gains.shape[0]), (0, mine.shape[1] - gains.shape[1])))
            mine = jnp.concatenate([mine, extra], axis=0)
            given = jnp.concatenate([given, extra], axis=0)
        taken = ring.other_core(given)
        return (
            jnp.where(first_core, mine, taken),
            jnp.where(first_core, taken, mine),
        )

    gains = jnp.stack([gain_attn, gain_mlp])
    hops = ring.chips - 1
    q_width = w_query.shape[1] // 2
    kv_width = key_projection_weight.shape[1] // 2
    qkv_width = q_width + 2 * kv_width
    out_width = w_out.shape[0] // 2
    attn_weights = Gather(
        ring,
        "attn_rows",
        *both_rows([w_query, key_projection_weight, value_projection_weight, w_out.T], gains),
        piece,
        [(0, qkv_width), (qkv_width, qkv_width + out_width)],
        below=16,
    )
    w_gate, layer_input, to_relative, lengths, _ = together(
        (w_gate, layer_input, to_relative, lengths, attn_weights.now)
    )
    gate_weights = Gather(ring, "gate_rows", *both_rows([w_gate]), piece)
    own_input = reorder(layer_input, to_relative)
    group_rows = gather_group(ring, own_input)
    for k in range(hops):
        turn(attn_weights, gate_weights)
        turn(gate_weights, attn_weights)
    up_weights = Gather(
        ring, "up_rows", *together((both_rows([w_up]), attn_weights.now))[0], piece
    )
    down_weights = Gather(
        ring, "down_rows", *together((both_rows([w_down.T]), gate_weights.now))[0], piece, split=True
    )

    sequence_numbers = jnp.stack([me, me + 1 - 2 * core])
    length = jnp.sum(
        jnp.where(seq_order[None, :] == sequence_numbers[:, None], lengths[None, :], 0), axis=1
    )
    offsets = jnp.arange(token_rows, dtype=jnp.int32)
    slot = jnp.concatenate([side * token_rows + offsets, (1 - side) * token_rows + offsets])
    inside = slot[None, :] < length[:, None]
    position = jnp.where(inside, slot[None, :], 0)
    own_valid = inside[0, :token_rows].astype(f32)[:, None]
    cosine, sine = rope_tables(position.reshape(-1), HEAD_SIZE)
    numbers = jnp.concatenate([length, side[None]]).astype(jnp.int32)
    own_rows = own_input.astype(f32)
    attn_scale = rms_scale(own_rows)

    qkv_proj, out_proj_t, gain_rows = attn_weights.buffers
    gain_rows = gain_rows[:2].astype(f32)
    attn_gain, mlp_gain = gain_rows[:1], gain_rows[1:]
    gate_proj = gate_weights.buffers[0]

    def forward():
        group_input = group_rows.astype(f32)
        normed = (group_input * rms_scale(group_input) * attn_gain).astype(bf16)
        qkv = jnp.dot(normed, qkv_proj, preferred_element_type=f32)
        normed, qkv = yield Held(normed, qkv)
        attended = by_sequence(
            attend_body,
            numbers,
            [qkv, cosine, sine],
            [q_width, kv_width, kv_width, q_width],
            "attend",
        )
        attended = yield Held(attended)
        parts = lax.dot_general(attended[3], out_proj_t, over_last, preferred_element_type=f32)
        parts = yield Held(parts)
        shared = scatter_group(ring, parts)
        own_teacher = yield Held(reorder(teacher, to_relative))
        yield ()
        shared = yield Held(shared)
        middle = own_rows + shared
        mlp_scale = rms_scale(middle)
        normed_mlp = gather_group(ring, (middle * mlp_scale * mlp_gain).astype(bf16))
        yield ()
        yield ()
        normed_mlp = yield Held(normed_mlp)
        gate = jnp.dot(normed_mlp, gate_proj, preferred_element_type=f32)
        gate = yield Held(gate)
        return (
            own_teacher,
            (normed, *attended),
            (middle, mlp_scale, normed_mlp, gate),
        )

    stages = Stages(forward())
    for k in range(hops):
        stages.turn(up_weights, down_weights)
        stages.turn(down_weights, up_weights)
    own_teacher, attn_kept, mlp_kept = stages.finish()
    normed, rot_queries, rot_keys, values, mixed = attn_kept
    middle, mlp_scale, normed_mlp, gate = mlp_kept
    up_proj = up_weights.buffers[0]
    down_far, down_near = down_weights.buffers
    count = jnp.sum(lengths).astype(f32)

    up = jnp.dot(normed_mlp, up_proj, preferred_element_type=f32)
    sigmoid_gate = jax.nn.sigmoid(gate)
    hidden = (gate * sigmoid_gate * up).astype(bf16)
    cut = width // 2

    def half_sum(rows, proj_t):
        parts = lax.dot_general(rows, proj_t, over_last, preferred_element_type=f32)
        return core_sum(ring, parts)

    def output(shared, columns):
        result = middle[:, columns] + shared
        error = (result - own_teacher[:, columns].astype(f32)) * own_valid
        delta = error * (tokens_all / count)
        return result, error, delta, delta.astype(bf16)

    def down_grad_of(branch):
        return lax.dot_general(branch, hidden, over_rows, preferred_element_type=f32).astype(bf16)

    half_far = half_sum(hidden, down_far)
    half_near = half_sum(together((hidden, half_far))[0], down_near)
    result_far, error_far, delta_far, low_far = output(tensor_sum(half_far), slice(0, cut))
    half_near, low_far = together((half_near, low_far))
    branch_far = gather_group(ring, low_far)
    grad_far = down_grad_of(branch_far)
    shared_near, branch_far, _ = together((tensor_sum(half_near), branch_far, grad_far))
    result_near, error_near, delta_near, low_near = output(shared_near, slice(cut, width))
    branch_near = gather_group(ring, low_near)
    down_sums = Scatter(ring, [grad_far], None, piece)
    result = jnp.concatenate([result_far, result_near], axis=1)
    delta_result = jnp.concatenate([delta_far, delta_near], axis=1)
    squared = jnp.sum(error_far * error_far) + jnp.sum(error_near * error_near)

    def backward():
        first = jnp.dot(branch_far, down_far, preferred_element_type=f32)
        first = yield Held(first)
        delta_hidden = first + jnp.dot(branch_near, down_near, preferred_element_type=f32)
        delta_gate = (
            delta_hidden * up * sigmoid_gate * (1.0 + gate * (1.0 - sigmoid_gate))
        ).astype(bf16)
        delta_up = (delta_hidden * gate * sigmoid_gate).astype(bf16)
        delta_gate, delta_up, branch = yield Held(delta_gate, delta_up, branch_near)
        near, delta_gate = yield Held(down_grad_of(branch), delta_gate)
        down_sums.parts = ([near], down_sums.parts[1])
        grad_gate = lax.dot_general(
            normed_mlp, delta_gate, over_rows, preferred_element_type=f32
        ).astype(bf16)
        grad_gate, delta_up = yield Held(grad_gate, delta_up)
        grad_up = lax.dot_general(
            normed_mlp, delta_up, over_rows, preferred_element_type=f32
        ).astype(bf16)
        grad_up, delta_gate, delta_up = yield Held(grad_up, delta_gate, delta_up)
        gate_up.append(grad_gate)
        gate_up.append(grad_up)
        parts = lax.dot_general(
            delta_gate, gate_proj, over_last, preferred_element_type=f32
        ) + lax.dot_general(delta_up, up_proj, over_last, preferred_element_type=f32)
        parts = yield Held(parts)
        delta_normed_mlp = scatter_group(ring, parts)
        placed = together((result.astype(bf16), parts))[0]
        activations = yield Held(reorder(placed, to_natural))
        delta_normed_mlp = yield Held(delta_normed_mlp)
        gain_mlp_part = jnp.sum(delta_normed_mlp * middle * mlp_scale, axis=0)
        weighted_mlp = mlp_gain * delta_normed_mlp
        delta_middle = (
            delta_result
            + mlp_scale * weighted_mlp
            - middle * mlp_scale**3 * jnp.mean(middle * weighted_mlp, axis=-1, keepdims=True)
        )
        attn_low_rows = gather_group(ring, delta_middle.astype(bf16))
        yield ()
        attn_low_rows = yield Held(attn_low_rows)
        grad_out_t = lax.dot_general(attn_low_rows, mixed, over_rows, preferred_element_type=f32)
        delta_mixed = jnp.dot(attn_low_rows, out_proj_t, preferred_element_type=f32).astype(bf16)
        grad_out_t = grad_out_t.astype(bf16)
        delta_qkv = by_sequence(
            attend_back_body,
            numbers,
            [rot_queries, rot_keys, values, delta_mixed, cosine, sine],
            [qkv_width],
            "attend_back",
        )[0]
        delta_qkv, grad_out_t = yield Held(delta_qkv, grad_out_t)
        grad_qkv = lax.dot_general(normed, delta_qkv, over_rows, preferred_element_type=f32)
        return (
            activations,
            gain_mlp_part,
            delta_middle,
            delta_qkv,
            [jnp.concatenate([grad_qkv.astype(bf16), grad_out_t], axis=1)],
        )

    def finish(sums):
        low, high = sums.now
        kept = jnp.where(first_core, low, high)
        taken = ring.other_core(jnp.where(first_core, high, low).astype(bf16)).astype(f32)
        return kept, taken

    def whole(kept, taken):
        return jnp.concatenate(
            [jnp.where(first_core, kept, taken), jnp.where(first_core, taken, kept)], axis=1
        )

    def halves(grads):
        return [g[: width // 2] for g in grads], [g[width // 2 :] for g in grads]

    gate_up = []
    stages = Stages(backward())
    for k in range(5):
        stages.turn(down_sums)
    gate_up_sums = Scatter(ring, *halves(gate_up), piece)
    while down_sums.left:
        if gate_up_sums.left:
            stages.turn(gate_up_sums, down_sums)
        stages.turn(down_sums, gate_up_sums)
    down_grad = whole(*finish(down_sums)).T
    while not stages.over and gate_up_sums.left:
        down_grad = stages.turn(gate_up_sums, None, down_grad)
    assert stages.over
    activations, gain_mlp_part, delta_middle, delta_qkv, attn_grads = stages.finish()
    attn_sums = Scatter(ring, *halves(attn_grads), piece)

    def closing():
        delta_normed = scatter_group(
            ring, lax.dot_general(delta_qkv, qkv_proj, over_last, preferred_element_type=f32)
        )
        yield ()
        delta_normed = yield Held(delta_normed)
        gain_attn_part = jnp.sum(delta_normed * own_rows * attn_scale, axis=0)
        weighted_attn = attn_gain * delta_normed
        input_grad = (
            delta_middle
            + attn_scale * weighted_attn
            - own_rows * attn_scale**3 * jnp.mean(own_rows * weighted_attn, axis=-1, keepdims=True)
        )
        natural = jnp.stack([gain_mlp_part, gain_attn_part], axis=0).reshape(2, devices, piece)[
            :, to_natural
        ]
        sums = jnp.concatenate(
            [natural.reshape(2 * devices, piece), jnp.full((8, piece), squared)], axis=0
        )
        input_grad, sums = yield Held(input_grad.astype(bf16), sums)
        sums = yield Held(sums + other_tensor(sums))
        step = 1
        while step < devices:
            pairs = [(d, d ^ step) for d in range(devices)]
            sums = yield Held(sums + lax.ppermute(sums, "dp", pairs))
            step *= 2
        return reorder(input_grad, to_natural), sums

    stages = Stages(closing())
    while gate_up_sums.left:
        down_grad = stages.turn(gate_up_sums, attn_sums, down_grad)
        stages.turn(attn_sums, gate_up_sums)
    kept, taken = finish(gate_up_sums)
    gate_width = w_gate.shape[1] // 2
    gate_grad = whole(kept[:, :gate_width], taken[:, :gate_width])
    up_grad = whole(kept[:, gate_width:], taken[:, gate_width:])
    stages.turn(attn_sums)
    while attn_sums.left:
        gate_grad, up_grad = stages.turn(attn_sums, None, (gate_grad, up_grad))
    input_grad, totals = stages.finish()
    gain_mlp_grad = lax.dynamic_slice_in_dim(totals, me, 1, 0)[0]
    gain_attn_grad = lax.dynamic_slice_in_dim(totals, devices + me, 1, 0)[0]
    distill_loss = totals[2 * devices, 0] / (2.0 * width * count)
    attn_kept, attn_taken = finish(attn_sums)
    cuts = [0, q_width, q_width + kv_width, qkv_width, attn_kept.shape[1]]
    query_grad, key_grad, value_grad, out_grad_t = [
        whole(attn_kept[:, a:b], attn_taken[:, a:b]) for a, b in zip(cuts[:-1], cuts[1:])
    ]
    return (
        activations,
        input_grad,
        gain_attn_grad,
        query_grad,
        key_grad,
        value_grad,
        out_grad_t.T,
        gain_mlp_grad,
        gate_grad,
        up_grad,
        down_grad,
        distill_loss,
    )


def solution(mesh):
    placed = (
        P(("dp", "tensor"), None),
        P(("dp", "tensor"), None),
        P(),
        P(),
        P("dp"),
        P("dp", "tensor"),
        P("dp", "tensor"),
        P("dp", "tensor"),
        P("tensor", "dp"),
        P("dp"),
        P("dp", "tensor"),
        P("dp", "tensor"),
        P("tensor", "dp"),
    )
    return jax.shard_map(
        per_device,
        mesh=mesh,
        in_specs=placed,
        out_specs=(
            P(("dp", "tensor"), None),
            P(("dp", "tensor"), None),
            P("dp"),
            P("dp", "tensor"),
            P("dp", "tensor"),
            P("dp", "tensor"),
            P("tensor", "dp"),
            P("dp"),
            P("dp", "tensor"),
            P("dp", "tensor"),
            P("tensor", "dp"),
            P(),
        ),
        check_vma=False,
    )
```

```python
import jax
import jax.numpy as jnp
from jax import lax
from jax.experimental import pallas as pl
from jax.experimental.pallas import tpu as pltpu
from jax.sharding import PartitionSpec as P

HEAD_SIZE = 256
LANES = 128
EPS = 1e-06
ROPE_BASE = 1000042.0
over_rows = (((0,), (0,)), ((), ()))
over_last = (((1,), (1,)), ((), ()))
plain = (((1,), (0,)), ((), ()))
f32 = jnp.float32
bf16 = jnp.bfloat16


def rms_scale(value_rows):
    return lax.rsqrt(jnp.mean(value_rows * value_rows, axis=-1, keepdims=True) + EPS)


def rope_tables(position, width):
    half = width // 2
    exponent = jnp.arange(half, dtype=f32) * (-2.0 / width)
    frequency = jnp.exp(exponent * jnp.log(f32(ROPE_BASE)))
    angle = position.astype(f32)[..., None] * frequency
    return (jnp.cos(angle), jnp.sin(angle))


def ring_order(chips):
    column = chips // 2
    return [2 * i for i in range(column)] + [2 * i + 1 for i in reversed(range(column))]


class Ring:
    def __init__(self, chips):
        self.chips = chips
        order = ring_order(chips)
        self.place = [order.index(c) for c in range(chips)]
        hop = [(order[i], order[(i + 1) % chips]) for i in range(chips)]
        self.up = [(2 * a + c, 2 * b + c) for a, b in hop for c in range(2)]
        self.down = [(b, a) for a, b in self.up]
        self.swap = [(d, d ^ 1) for d in range(2 * chips)]

    def ahead(self, v):
        return lax.ppermute(v, "dp", self.up)

    def back(self, v):
        return lax.ppermute(v, "dp", self.down)

    def other_core(self, v):
        return lax.ppermute(v, "dp", self.swap)


def other_tensor(v):
    return lax.ppermute(v, "tensor", [(0, 1), (1, 0)])


def together(values):
    return lax.optimization_barrier(values)


def unfilled(shape, name):
    return pl.pallas_call(
        lambda out: None,
        out_shape=jax.ShapeDtypeStruct(shape, bf16),
        out_specs=pl.BlockSpec(memory_space=pl.ANY),
        name=name,
    )()


class Gather:
    def __init__(self, ring, name, low, high, rows, cuts=None, split=False, below=0):
        self.ring, self.size, self.split, self.below = ring, rows, split, below
        self.now = (low, high)
        self.cuts = cuts or [(0, low.shape[1])]
        height = 2 * ring.chips * rows
        shapes = [(height, b - a) for a, b in self.cuts]
        if split:
            shapes = [(height // 2, low.shape[1])] * 2
        if below:
            shapes.append((below, height))
        self.buffers = [unfilled(v, f"{name}_{i}") for i, v in enumerate(shapes)]
        self.hops = 0
        self.store()

    def store(self):
        half = self.ring.chips // 2
        k, self.hops = self.hops, self.hops + 1
        for side, rows in enumerate(self.now):
            at = k + (side - 1) * half if k >= half else k + (side + 2) * half
            if self.split:
                which = int(k < half)
                start = (at - which * 2 * half) * self.size
                self.buffers[which] = lax.dynamic_update_slice(
                    self.buffers[which], rows[: self.size], (start, 0)
                )
                continue
            for i, (a, b) in enumerate(self.cuts):
                self.buffers[i] = lax.dynamic_update_slice(
                    self.buffers[i], rows[: self.size, a:b], (at * self.size, 0)
                )
            if self.below:
                self.buffers[-1] = lax.dynamic_update_slice(
                    self.buffers[-1],
                    rows[self.size : self.size + self.below, : self.size],
                    (0, at * self.size),
                )

    def move(self):
        return self.ring.ahead(self.now[0]), self.ring.back(self.now[1])

    def take(self, moved):
        self.now = moved
        self.store()


class Scatter:
    def __init__(self, ring, far, near, rows):
        self.ring, self.parts, self.size = ring, (near, far), rows
        self.buffers = []
        self.left = ring.chips - 1
        self.now = (self.block(0), self.block(1))

    def block(self, side):
        half = self.ring.chips // 2
        grads = self.parts[self.left // half]
        start = (side * half + self.left % half) * self.size
        return jnp.concatenate([g[start : start + self.size] for g in grads], axis=1)

    def move(self):
        return self.ring.back(self.now[0]), self.ring.ahead(self.now[1])

    def take(self, moved):
        self.left -= 1
        sums = [m.astype(f32) + self.block(side).astype(f32) for side, m in enumerate(moved)]
        self.now = tuple(sums if self.left == 0 else [v.astype(bf16) for v in sums])


class Held:
    def __init__(self, *value):
        self.value = value if len(value) > 1 else value[0]


def turn(lane, other=None, values=(), held=()):
    moved, _, held, lane.buffers = together(
        (lane.move(), other.now if other else (), held, lane.buffers)
    )
    lane.take(moved)
    values, held, _ = together((values, held, lane.now))
    return values, held


class Stages:
    def __init__(self, generator):
        self.generator = generator
        self.result = None
        self.value = ()
        self.over = False
        self.advance(None)

    def advance(self, value):
        if not self.over:
            try:
                self.value = self.generator.send(value)
            except StopIteration as end:
                self.result, self.over, self.value = end.value, True, ()

    def turn(self, lane, other=None, extra=()):
        if isinstance(self.value, Held):
            extra, value = turn(lane, other, extra, self.value.value)
        else:
            (value, extra), _ = turn(lane, other, (self.value, extra))
        self.advance(value)
        return extra

    def finish(self):
        while not self.over:
            self.advance(self.value.value if isinstance(self.value, Held) else self.value)
        return self.result


def gather_group(ring, rows):
    across = other_tensor(rows)
    beside = ring.other_core(rows)
    return jnp.concatenate([rows, across, beside, ring.other_core(across)], axis=0)


def core_sum(ring, parts):
    half = parts.shape[0] // 2
    return parts[:half] + ring.other_core(parts[half:].astype(bf16)).astype(f32)


def tensor_sum(rows):
    half = rows.shape[0] // 2
    return rows[:half] + other_tensor(rows[half:].astype(bf16)).astype(f32)


def scatter_group(ring, parts):
    return tensor_sum(core_sum(ring, parts))


def copy_blocks(table, source, target):
    for k in range(target.shape[1] // LANES):
        start = pl.multiple_of(table[k] * LANES, LANES)
        target[:, k * LANES : (k + 1) * LANES] = source[:, pl.ds(start, LANES)]


def reorder(rows, table):
    height, width = rows.shape
    step = height // 4
    return pl.pallas_call(
        copy_blocks,
        out_shape=jax.ShapeDtypeStruct(rows.shape, rows.dtype),
        grid_spec=pltpu.PrefetchScalarGridSpec(
            num_scalar_prefetch=1,
            grid=(height // step,),
            in_specs=[pl.BlockSpec((step, width), lambda k, t: (k, 0))],
            out_specs=pl.BlockSpec((step, width), lambda k, t: (k, 0)),
        ),
        name="reorder",
    )(table, rows)


def visible(numbers, shape):
    def slot(axis):
        offset = lax.broadcasted_iota(jnp.int32, shape, axis)
        start = numbers[2] * (shape[0] // 2)
        return jnp.where(offset < shape[0] // 2, offset + start, offset - start)

    query, key = slot(0), slot(1)
    inside = query < numbers[pl.program_id(0)]
    return jnp.where(inside, key - query, jnp.abs(key - query)) <= 0


def turned(heads, cosine, sine):
    half = heads.shape[1] // 2
    first, second = heads[:, :half], heads[:, half:]
    return first * cosine - second * sine, second * cosine + first * sine


def weights_of(queries, keys, allowed):
    scores = lax.dot_general(queries, keys, over_last, preferred_element_type=f32)
    scores = jnp.where(allowed, scores * HEAD_SIZE ** (-0.5), -1e30)
    shifted = jnp.exp(scores - jnp.max(scores, axis=-1, keepdims=True))
    return shifted / jnp.sum(shifted, axis=-1, keepdims=True)


def attend_body(numbers, qkv, cosine, sine, queries, keys, values, mixed):
    rows, width = queries.shape
    half = HEAD_SIZE // 2
    cosine, sine = cosine[...], sine[...]
    key_low, key_high = turned(qkv[:, width : width + HEAD_SIZE], cosine, sine)
    keys[:, :half] = key_low.astype(bf16)
    keys[:, half:] = key_high.astype(bf16)
    values[...] = qkv[:, width + HEAD_SIZE :].astype(bf16)
    allowed = visible(numbers, (rows, rows))
    for start in range(0, width, HEAD_SIZE):
        low, high = turned(qkv[:, start : start + HEAD_SIZE], cosine, sine)
        queries[:, start : start + half] = low.astype(bf16)
        queries[:, start + half : start + HEAD_SIZE] = high.astype(bf16)
        probs = weights_of(queries[:, start : start + HEAD_SIZE], keys[...], allowed)
        mixed[:, start : start + HEAD_SIZE] = jnp.dot(
            probs.astype(bf16), values[...], preferred_element_type=f32
        ).astype(bf16)


def attend_back_body(numbers, queries, keys, values, delta, cosine, sine, out):
    rows, width = queries.shape
    half = HEAD_SIZE // 2
    scaling = HEAD_SIZE ** (-0.5)
    cosine, sine = cosine[...], sine[...]
    allowed = visible(numbers, (rows, rows))
    delta_keys = jnp.zeros((rows, HEAD_SIZE), f32)
    delta_values = jnp.zeros((rows, HEAD_SIZE), f32)
    for start in range(0, width, HEAD_SIZE):
        head = queries[:, start : start + HEAD_SIZE]
        delta_mixed = delta[:, start : start + HEAD_SIZE]
        probs = weights_of(head, keys[...], allowed)
        delta_probs = lax.dot_general(
            delta_mixed, values[...], over_last, preferred_element_type=f32
        )
        inner = jnp.sum(probs * delta_probs, axis=-1, keepdims=True)
        delta_scores = (probs * (delta_probs - inner)).astype(bf16)
        delta_values += lax.dot_general(
            probs.astype(bf16), delta_mixed, over_rows, preferred_element_type=f32
        )
        delta_keys += lax.dot_general(delta_scores, head, over_rows, preferred_element_type=f32)
        delta_head = jnp.dot(delta_scores, keys[...], preferred_element_type=f32) * scaling
        low, high = turned(delta_head, cosine, -sine)
        out[:, start : start + half] = low.astype(bf16)
        out[:, start + half : start + HEAD_SIZE] = high.astype(bf16)
    low, high = turned(delta_keys * scaling, cosine, -sine)
    out[:, width : width + half] = low.astype(bf16)
    out[:, width + half : width + HEAD_SIZE] = high.astype(bf16)
    out[:, width + HEAD_SIZE :] = delta_values.astype(bf16)


def by_sequence(body, numbers, arrays, widths, name):
    rows = arrays[0].shape[0] // 2

    def spec(columns):
        return pl.BlockSpec((rows, columns), lambda b, n: (b, 0))

    return pl.pallas_call(
        body,
        out_shape=[jax.ShapeDtypeStruct((2 * rows, w), bf16) for w in widths],
        grid_spec=pltpu.PrefetchScalarGridSpec(
            num_scalar_prefetch=1,
            grid=(2,),
            in_specs=[spec(v.shape[1]) for v in arrays],
            out_specs=[spec(w) for w in widths],
        ),
        name=name,
    )(numbers, *arrays)


def per_device(
    layer_input,
    teacher,
    lengths,
    seq_order,
    gain_attn,
    w_query,
    key_projection_weight,
    value_projection_weight,
    w_out,
    gain_mlp,
    w_gate,
    w_up,
    w_down,
):
    token_rows, width = layer_input.shape
    slots = token_rows * lax.axis_size("tensor")
    devices = lax.axis_size("dp")
    tokens_all = slots * devices
    chips = devices // 2
    ring = Ring(chips)
    me = lax.axis_index("dp")
    side = lax.axis_index("tensor")
    chip, core = me // 2, me % 2
    first_core = core == 0
    place = jnp.array(ring.place, dtype=jnp.int32)
    here = place[chip]
    piece = gain_attn.shape[0]

    numbers = jnp.arange(chips, dtype=jnp.int32)
    order = jnp.array(ring_order(chips), dtype=jnp.int32)
    from_low = 2 * order[(here - numbers) % chips]
    from_high = 2 * order[(here + numbers) % chips] + 1
    half = chips // 2
    to_relative = jnp.concatenate(
        [from_low[half:], from_high[half:], from_low[:half], from_high[:half]]
    )
    behind, before = (here - place) % chips, (place - here) % chips
    to_natural = jnp.stack(
        [
            jnp.where(behind < half, behind + 2 * half, behind - half),
            jnp.where(before < half, before + 3 * half, before),
        ],
        axis=1,
    ).reshape(devices)

    def split_cores(w):
        quarter = w.shape[1] // 2
        mine = lax.dynamic_slice_in_dim(w, core * quarter, quarter, 1)
        given = lax.dynamic_slice_in_dim(w, (1 - core) * quarter, quarter, 1)
        return mine, given

    def both_rows(weights, gains=None):
        mine, given = zip(*[split_cores(w) for w in weights])
        mine, given = jnp.concatenate(mine, axis=1), jnp.concatenate(given, axis=1)
        if gains is not None:
            extra = jnp.pad(gains, ((0, 16 - gains.shape[0]), (0, mine.shape[1] - gains.shape[1])))
            mine = jnp.concatenate([mine, extra], axis=0)
            given = jnp.concatenate([given, extra], axis=0)
        taken = ring.other_core(given)
        return (
            jnp.where(first_core, mine, taken),
            jnp.where(first_core, taken, mine),
        )

    gains = jnp.stack([gain_attn, gain_mlp])
    hops = ring.chips - 1
    q_width = w_query.shape[1] // 2
    kv_width = key_projection_weight.shape[1] // 2
    qkv_width = q_width + 2 * kv_width
    out_width = w_out.shape[0] // 2
    attn_weights = Gather(
        ring,
        "attn_rows",
        *both_rows([w_query, key_projection_weight, value_projection_weight, w_out.T], gains),
        piece,
        [(0, qkv_width), (qkv_width, qkv_width + out_width)],
        below=16,
    )
    w_gate, layer_input, to_relative, lengths, _ = together(
        (w_gate, layer_input, to_relative, lengths, attn_weights.now)
    )
    gate_weights = Gather(ring, "gate_rows", *both_rows([w_gate]), piece)
    own_input = reorder(layer_input, to_relative)
    group_rows = gather_group(ring, own_input)
    for k in range(hops):
        turn(attn_weights, gate_weights)
        turn(gate_weights, attn_weights)
    up_weights = Gather(
        ring, "up_rows", *together((both_rows([w_up]), attn_weights.now))[0], piece
    )
    down_weights = Gather(
        ring, "down_rows", *together((both_rows([w_down.T]), gate_weights.now))[0], piece, split=True
    )

    sequence_numbers = jnp.stack([me, me + 1 - 2 * core])
    length = jnp.sum(
        jnp.where(seq_order[None, :] == sequence_numbers[:, None], lengths[None, :], 0), axis=1
    )
    offsets = jnp.arange(token_rows, dtype=jnp.int32)
    slot = jnp.concatenate([side * token_rows + offsets, (1 - side) * token_rows + offsets])
    inside = slot[None, :] < length[:, None]
    position = jnp.where(inside, slot[None, :], 0)
    own_valid = inside[0, :token_rows].astype(f32)[:, None]
    cosine, sine = rope_tables(position.reshape(-1), HEAD_SIZE)
    numbers = jnp.concatenate([length, side[None]]).astype(jnp.int32)
    own_rows = own_input.astype(f32)
    attn_scale = rms_scale(own_rows)

    qkv_proj, out_proj_t, gain_rows = attn_weights.buffers
    gain_rows = gain_rows[:2].astype(f32)
    attn_gain, mlp_gain = gain_rows[:1], gain_rows[1:]
    gate_proj = gate_weights.buffers[0]

    def forward():
        group_input = group_rows.astype(f32)
        normed = (group_input * rms_scale(group_input) * attn_gain).astype(bf16)
        qkv = jnp.dot(normed, qkv_proj, preferred_element_type=f32)
        normed, qkv = yield Held(normed, qkv)
        attended = by_sequence(
            attend_body,
            numbers,
            [qkv, cosine, sine],
            [q_width, kv_width, kv_width, q_width],
            "attend",
        )
        attended = yield Held(attended)
        parts = lax.dot_general(attended[3], out_proj_t, over_last, preferred_element_type=f32)
        parts = yield Held(parts)
        shared = scatter_group(ring, parts)
        own_teacher = yield Held(reorder(teacher, to_relative))
        yield ()
        shared = yield Held(shared)
        middle = own_rows + shared
        mlp_scale = rms_scale(middle)
        normed_mlp = gather_group(ring, (middle * mlp_scale * mlp_gain).astype(bf16))
        yield ()
        yield ()
        normed_mlp = yield Held(normed_mlp)
        gate = jnp.dot(normed_mlp, gate_proj, preferred_element_type=f32)
        gate = yield Held(gate)
        return (
            own_teacher,
            (normed, *attended),
            (middle, mlp_scale, normed_mlp, gate),
        )

    stages = Stages(forward())
    for k in range(hops):
        stages.turn(up_weights, down_weights)
        stages.turn(down_weights, up_weights)
    own_teacher, attn_kept, mlp_kept = stages.finish()
    normed, rot_queries, rot_keys, values, mixed = attn_kept
    middle, mlp_scale, normed_mlp, gate = mlp_kept
    up_proj = up_weights.buffers[0]
    down_far, down_near = down_weights.buffers
    count = jnp.sum(lengths).astype(f32)

    up = jnp.dot(normed_mlp, up_proj, preferred_element_type=f32)
    sigmoid_gate = jax.nn.sigmoid(gate)
    hidden = (gate * sigmoid_gate * up).astype(bf16)
    cut = width // 2

    def half_sum(rows, proj_t):
        parts = lax.dot_general(rows, proj_t, over_last, preferred_element_type=f32)
        return core_sum(ring, parts)

    def output(shared, columns):
        result = middle[:, columns] + shared
        error = (result - own_teacher[:, columns].astype(f32)) * own_valid
        delta = error * (tokens_all / count)
        return result, error, delta, delta.astype(bf16)

    def down_grad_of(branch):
        return lax.dot_general(branch, hidden, over_rows, preferred_element_type=f32).astype(bf16)

    half_far = half_sum(hidden, down_far)
    half_near = half_sum(together((hidden, half_far))[0], down_near)
    result_far, error_far, delta_far, low_far = output(tensor_sum(half_far), slice(0, cut))
    branch_far = gather_group(ring, low_far)
    grad_far = down_grad_of(branch_far)
    shared_near = together((tensor_sum(half_near), low_far))[0]
    result_near, error_near, delta_near, low_near = output(shared_near, slice(cut, width))
    branch_near = gather_group(ring, low_near)
    down_sums = Scatter(ring, [grad_far], None, piece)
    result = jnp.concatenate([result_far, result_near], axis=1)
    delta_result = jnp.concatenate([delta_far, delta_near], axis=1)
    squared = jnp.sum(error_far * error_far) + jnp.sum(error_near * error_near)

    def backward():
        branch = together((branch_far, grad_far))[0]
        first = jnp.dot(branch, down_far, preferred_element_type=f32)
        first = yield Held(first)
        delta_hidden = first + jnp.dot(branch_near, down_near, preferred_element_type=f32)
        delta_gate = (
            delta_hidden * up * sigmoid_gate * (1.0 + gate * (1.0 - sigmoid_gate))
        ).astype(bf16)
        delta_up = (delta_hidden * gate * sigmoid_gate).astype(bf16)
        delta_gate, delta_up, branch = yield Held(delta_gate, delta_up, branch_near)
        near, delta_gate = yield Held(down_grad_of(branch), delta_gate)
        down_sums.parts = ([near], down_sums.parts[1])
        grad_gate = lax.dot_general(
            normed_mlp, delta_gate, over_rows, preferred_element_type=f32
        ).astype(bf16)
        grad_gate, delta_up = yield Held(grad_gate, delta_up)
        grad_up = lax.dot_general(
            normed_mlp, delta_up, over_rows, preferred_element_type=f32
        ).astype(bf16)
        grad_up, delta_gate, delta_up = yield Held(grad_up, delta_gate, delta_up)
        gate_up.append(grad_gate)
        gate_up.append(grad_up)
        def from_hidden(rows):
            return lax.dot_general(
                delta_gate[rows], gate_proj, over_last, preferred_element_type=f32
            ) + lax.dot_general(delta_up[rows], up_proj, over_last, preferred_element_type=f32)

        given, delta_gate, delta_up = yield Held(
            from_hidden(slice(slots, None)).astype(bf16), delta_gate, delta_up
        )
        taken = ring.other_core(given)
        parts = yield Held(from_hidden(slice(0, slots)))
        delta_normed_mlp = tensor_sum(parts + taken.astype(f32))
        placed = together((result.astype(bf16), parts))[0]
        activations = yield Held(reorder(placed, to_natural))
        delta_normed_mlp = yield Held(delta_normed_mlp)
        gain_mlp_part = jnp.sum(delta_normed_mlp * middle * mlp_scale, axis=0)
        weighted_mlp = mlp_gain * delta_normed_mlp
        delta_middle = (
            delta_result
            + mlp_scale * weighted_mlp
            - middle * mlp_scale**3 * jnp.mean(middle * weighted_mlp, axis=-1, keepdims=True)
        )
        attn_low_rows = gather_group(ring, delta_middle.astype(bf16))
        yield ()
        attn_low_rows = yield Held(attn_low_rows)
        grad_out_t = lax.dot_general(attn_low_rows, mixed, over_rows, preferred_element_type=f32)
        delta_mixed = jnp.dot(attn_low_rows, out_proj_t, preferred_element_type=f32).astype(bf16)
        grad_out_t = grad_out_t.astype(bf16)
        delta_qkv = by_sequence(
            attend_back_body,
            numbers,
            [rot_queries, rot_keys, values, delta_mixed, cosine, sine],
            [qkv_width],
            "attend_back",
        )[0]
        delta_qkv, grad_out_t = yield Held(delta_qkv, grad_out_t)
        grad_qkv = lax.dot_general(normed, delta_qkv, over_rows, preferred_element_type=f32)
        return (
            activations,
            gain_mlp_part,
            delta_middle,
            delta_qkv,
            [jnp.concatenate([grad_qkv.astype(bf16), grad_out_t], axis=1)],
        )

    def finish(sums):
        low, high = sums.now
        kept = jnp.where(first_core, low, high)
        taken = ring.other_core(jnp.where(first_core, high, low).astype(bf16)).astype(f32)
        return kept, taken

    def whole(kept, taken):
        return jnp.concatenate(
            [jnp.where(first_core, kept, taken), jnp.where(first_core, taken, kept)], axis=1
        )

    def halves(grads):
        return [g[: width // 2] for g in grads], [g[width // 2 :] for g in grads]

    gate_up = []
    stages = Stages(backward())
    for k in range(5):
        stages.turn(down_sums)
    gate_up_sums = Scatter(ring, *halves(gate_up), piece)
    while down_sums.left:
        stages.turn(down_sums, gate_up_sums)
        stages.turn(gate_up_sums, down_sums)
    down_grad = whole(*finish(down_sums)).T
    while not stages.over and gate_up_sums.left:
        down_grad = stages.turn(gate_up_sums, None, down_grad)
    assert stages.over
    activations, gain_mlp_part, delta_middle, delta_qkv, attn_grads = stages.finish()
    attn_sums = Scatter(ring, *halves(attn_grads), piece)

    def closing():
        delta_normed = scatter_group(
            ring,
            lax.dot_general(
                together((delta_qkv, attn_sums.now))[0],
                qkv_proj,
                over_last,
                preferred_element_type=f32,
            ),
        )
        yield ()
        yield ()
        yield ()
        delta_normed = yield Held(delta_normed)
        gain_attn_part = jnp.sum(delta_normed * own_rows * attn_scale, axis=0)
        weighted_attn = attn_gain * delta_normed
        input_grad = (
            delta_middle
            + attn_scale * weighted_attn
            - own_rows * attn_scale**3 * jnp.mean(own_rows * weighted_attn, axis=-1, keepdims=True)
        )
        natural = jnp.stack([gain_mlp_part, gain_attn_part], axis=0).reshape(2, devices, piece)[
            :, to_natural
        ]
        sums = jnp.concatenate(
            [natural.reshape(2 * devices, piece), jnp.full((8, piece), squared)], axis=0
        )
        input_grad = input_grad.astype(bf16)
        sums, input_grad = yield Held(sums + other_tensor(sums), input_grad)
        step = 1
        while step < devices:
            pairs = [(d, d ^ step) for d in range(devices)]
            sums = yield Held(sums + lax.ppermute(sums, "dp", pairs))
            step *= 2
        return reorder(input_grad, to_natural), sums

    stages = Stages(closing())
    while gate_up_sums.left:
        down_grad = stages.turn(gate_up_sums, attn_sums, down_grad)
        stages.turn(attn_sums, gate_up_sums)
    kept, taken = finish(gate_up_sums)
    gate_width = w_gate.shape[1] // 2
    gate_grad = whole(kept[:, :gate_width], taken[:, :gate_width])
    up_grad = whole(kept[:, gate_width:], taken[:, gate_width:])
    stages.turn(attn_sums)
    while attn_sums.left:
        gate_grad, up_grad = stages.turn(attn_sums, None, (gate_grad, up_grad))
    input_grad, totals = stages.finish()
    gain_mlp_grad = lax.dynamic_slice_in_dim(totals, me, 1, 0)[0]
    gain_attn_grad = lax.dynamic_slice_in_dim(totals, devices + me, 1, 0)[0]
    distill_loss = totals[2 * devices, 0] / (2.0 * width * count)
    attn_kept, attn_taken = finish(attn_sums)
    cuts = [0, q_width, q_width + kv_width, qkv_width, attn_kept.shape[1]]
    query_grad, key_grad, value_grad, out_grad_t = [
        whole(attn_kept[:, a:b], attn_taken[:, a:b]) for a, b in zip(cuts[:-1], cuts[1:])
    ]
    return (
        activations,
        input_grad,
        gain_attn_grad,
        query_grad,
        key_grad,
        value_grad,
        out_grad_t.T,
        gain_mlp_grad,
        gate_grad,
        up_grad,
        down_grad,
        distill_loss,
    )


def solution(mesh):
    placed = (
        P(("dp", "tensor"), None),
        P(("dp", "tensor"), None),
        P(),
        P(),
        P("dp"),
        P("dp", "tensor"),
        P("dp", "tensor"),
        P("dp", "tensor"),
        P("tensor", "dp"),
        P("dp"),
        P("dp", "tensor"),
        P("dp", "tensor"),
        P("tensor", "dp"),
    )
    return jax.shard_map(
        per_device,
        mesh=mesh,
        in_specs=placed,
        out_specs=(
            P(("dp", "tensor"), None),
            P(("dp", "tensor"), None),
            P("dp"),
            P("dp", "tensor"),
            P("dp", "tensor"),
            P("dp", "tensor"),
            P("tensor", "dp"),
            P("dp"),
            P("dp", "tensor"),
            P("dp", "tensor"),
            P("tensor", "dp"),
            P(),
        ),
        check_vma=False,
    )
```

```python
import jax
import jax.numpy as jnp
from jax import lax
from jax.experimental import pallas as pl
from jax.experimental.pallas import tpu as pltpu
from jax.sharding import PartitionSpec as P

HEAD_SIZE = 256
LANES = 128
EPS = 1e-06
ROPE_BASE = 1000042.0
over_rows = (((0,), (0,)), ((), ()))
over_last = (((1,), (1,)), ((), ()))
plain = (((1,), (0,)), ((), ()))
f32 = jnp.float32
bf16 = jnp.bfloat16


def rms_scale(value_rows):
    return lax.rsqrt(jnp.mean(value_rows * value_rows, axis=-1, keepdims=True) + EPS)


def rope_tables(position, width):
    half = width // 2
    exponent = jnp.arange(half, dtype=f32) * (-2.0 / width)
    frequency = jnp.exp(exponent * jnp.log(f32(ROPE_BASE)))
    angle = position.astype(f32)[..., None] * frequency
    return (jnp.cos(angle), jnp.sin(angle))


def ring_order(chips):
    column = chips // 2
    return [2 * i for i in range(column)] + [2 * i + 1 for i in reversed(range(column))]


class Ring:
    def __init__(self, chips):
        self.chips = chips
        order = ring_order(chips)
        self.place = [order.index(c) for c in range(chips)]
        hop = [(order[i], order[(i + 1) % chips]) for i in range(chips)]
        self.up = [(2 * a + c, 2 * b + c) for a, b in hop for c in range(2)]
        self.down = [(b, a) for a, b in self.up]
        self.swap = [(d, d ^ 1) for d in range(2 * chips)]

    def ahead(self, v):
        return lax.ppermute(v, "dp", self.up)

    def back(self, v):
        return lax.ppermute(v, "dp", self.down)

    def other_core(self, v):
        return lax.ppermute(v, "dp", self.swap)


def other_tensor(v):
    return lax.ppermute(v, "tensor", [(0, 1), (1, 0)])


def together(values):
    return lax.optimization_barrier(values)


def unfilled(shape, name):
    return pl.pallas_call(
        lambda out: None,
        out_shape=jax.ShapeDtypeStruct(shape, bf16),
        out_specs=pl.BlockSpec(memory_space=pl.ANY),
        name=name,
    )()


class Gather:
    def __init__(self, ring, name, low, high, rows, cuts=None, split=False, below=0):
        self.ring, self.size, self.split, self.below = ring, rows, split, below
        self.now = (low, high)
        self.cuts = cuts or [(0, low.shape[1])]
        height = 2 * ring.chips * rows
        shapes = [(height, b - a) for a, b in self.cuts]
        if split:
            shapes = [(height // 2, low.shape[1])] * 2
        if below:
            shapes.append((below, height))
        self.buffers = [unfilled(v, f"{name}_{i}") for i, v in enumerate(shapes)]
        self.hops = 0
        self.store()

    def store(self):
        half = self.ring.chips // 2
        k, self.hops = self.hops, self.hops + 1
        for side, rows in enumerate(self.now):
            at = k + (side - 1) * half if k >= half else k + (side + 2) * half
            if self.split:
                which = int(k < half)
                start = (at - which * 2 * half) * self.size
                self.buffers[which] = lax.dynamic_update_slice(
                    self.buffers[which], rows[: self.size], (start, 0)
                )
                continue
            for i, (a, b) in enumerate(self.cuts):
                self.buffers[i] = lax.dynamic_update_slice(
                    self.buffers[i], rows[: self.size, a:b], (at * self.size, 0)
                )
            if self.below:
                self.buffers[-1] = lax.dynamic_update_slice(
                    self.buffers[-1],
                    rows[self.size : self.size + self.below, : self.size],
                    (0, at * self.size),
                )

    def move(self):
        return self.ring.ahead(self.now[0]), self.ring.back(self.now[1])

    def take(self, moved):
        self.now = moved
        self.store()


class Scatter:
    def __init__(self, ring, far, near, rows):
        self.ring, self.parts, self.size = ring, (near, far), rows
        self.buffers = []
        self.left = ring.chips - 1
        self.now = (self.block(0), self.block(1))

    def block(self, side):
        half = self.ring.chips // 2
        grads = self.parts[self.left // half]
        start = (side * half + self.left % half) * self.size
        return jnp.concatenate([g[start : start + self.size] for g in grads], axis=1)

    def move(self):
        return self.ring.back(self.now[0]), self.ring.ahead(self.now[1])

    def take(self, moved):
        self.left -= 1
        sums = [m.astype(f32) + self.block(side).astype(f32) for side, m in enumerate(moved)]
        self.now = tuple(sums if self.left == 0 else [v.astype(bf16) for v in sums])


class Held:
    def __init__(self, *value):
        self.value = value if len(value) > 1 else value[0]


def turn(lane, other=None, values=(), held=()):
    moved, _, held, lane.buffers = together(
        (lane.move(), other.now if other else (), held, lane.buffers)
    )
    lane.take(moved)
    values, held, _ = together((values, held, lane.now))
    return values, held


class Stages:
    def __init__(self, generator):
        self.generator = generator
        self.result = None
        self.value = ()
        self.over = False
        self.advance(None)

    def advance(self, value):
        if not self.over:
            try:
                self.value = self.generator.send(value)
            except StopIteration as end:
                self.result, self.over, self.value = end.value, True, ()

    def turn(self, lane, other=None, extra=()):
        if isinstance(self.value, Held):
            value = turn(lane, other, (), (self.value.value, extra))[1][0]
        else:
            value = turn(lane, other, self.value, extra)[0]
        self.advance(value)

    def finish(self):
        while not self.over:
            self.advance(self.value.value if isinstance(self.value, Held) else self.value)
        return self.result


def gather_group(ring, rows, before=()):
    across = together((other_tensor(rows), before))[0]
    beside = ring.other_core(rows)
    return jnp.concatenate([rows, across, beside, ring.other_core(across)], axis=0)


def core_sum(ring, parts):
    half = parts.shape[0] // 2
    return parts[:half] + ring.other_core(parts[half:].astype(bf16)).astype(f32)


def tensor_sum(rows):
    half = rows.shape[0] // 2
    return rows[:half] + other_tensor(rows[half:].astype(bf16)).astype(f32)


def scatter_group(ring, parts):
    return tensor_sum(core_sum(ring, parts))


def copy_blocks(table, source, target):
    for k in range(target.shape[1] // LANES):
        start = pl.multiple_of(table[k] * LANES, LANES)
        target[:, k * LANES : (k + 1) * LANES] = source[:, pl.ds(start, LANES)]


def reorder(rows, table):
    height, width = rows.shape
    step = height // 4
    return pl.pallas_call(
        copy_blocks,
        out_shape=jax.ShapeDtypeStruct(rows.shape, rows.dtype),
        grid_spec=pltpu.PrefetchScalarGridSpec(
            num_scalar_prefetch=1,
            grid=(height // step,),
            in_specs=[pl.BlockSpec((step, width), lambda k, t: (k, 0))],
            out_specs=pl.BlockSpec((step, width), lambda k, t: (k, 0)),
        ),
        name="reorder",
    )(table, rows)


def visible(numbers, shape):
    def slot(axis):
        offset = lax.broadcasted_iota(jnp.int32, shape, axis)
        start = numbers[2] * (shape[0] // 2)
        return jnp.where(offset < shape[0] // 2, offset + start, offset - start)

    query, key = slot(0), slot(1)
    inside = query < numbers[pl.program_id(0)]
    return jnp.where(inside, key - query, jnp.abs(key - query)) <= 0


def turned(heads, cosine, sine):
    half = heads.shape[1] // 2
    first, second = heads[:, :half], heads[:, half:]
    return first * cosine - second * sine, second * cosine + first * sine


def weights_of(queries, keys, allowed):
    scores = lax.dot_general(queries, keys, over_last, preferred_element_type=f32)
    scores = jnp.where(allowed, scores * HEAD_SIZE ** (-0.5), -1e30)
    shifted = jnp.exp(scores - jnp.max(scores, axis=-1, keepdims=True))
    return shifted / jnp.sum(shifted, axis=-1, keepdims=True)


def attend_body(numbers, qkv, cosine, sine, queries, keys, values, mixed):
    rows, width = queries.shape
    half = HEAD_SIZE // 2
    cosine, sine = cosine[...], sine[...]
    key_low, key_high = turned(qkv[:, width : width + HEAD_SIZE], cosine, sine)
    keys[:, :half] = key_low.astype(bf16)
    keys[:, half:] = key_high.astype(bf16)
    values[...] = qkv[:, width + HEAD_SIZE :].astype(bf16)
    allowed = visible(numbers, (rows, rows))
    for start in range(0, width, HEAD_SIZE):
        low, high = turned(qkv[:, start : start + HEAD_SIZE], cosine, sine)
        queries[:, start : start + half] = low.astype(bf16)
        queries[:, start + half : start + HEAD_SIZE] = high.astype(bf16)
        probs = weights_of(queries[:, start : start + HEAD_SIZE], keys[...], allowed)
        mixed[:, start : start + HEAD_SIZE] = jnp.dot(
            probs.astype(bf16), values[...], preferred_element_type=f32
        ).astype(bf16)


def attend_back_body(numbers, queries, keys, values, delta, cosine, sine, out):
    rows, width = queries.shape
    half = HEAD_SIZE // 2
    scaling = HEAD_SIZE ** (-0.5)
    cosine, sine = cosine[...], sine[...]
    allowed = visible(numbers, (rows, rows))
    delta_keys = jnp.zeros((rows, HEAD_SIZE), f32)
    delta_values = jnp.zeros((rows, HEAD_SIZE), f32)
    for start in range(0, width, HEAD_SIZE):
        head = queries[:, start : start + HEAD_SIZE]
        delta_mixed = delta[:, start : start + HEAD_SIZE]
        probs = weights_of(head, keys[...], allowed)
        delta_probs = lax.dot_general(
            delta_mixed, values[...], over_last, preferred_element_type=f32
        )
        inner = jnp.sum(probs * delta_probs, axis=-1, keepdims=True)
        delta_scores = (probs * (delta_probs - inner)).astype(bf16)
        delta_values += lax.dot_general(
            probs.astype(bf16), delta_mixed, over_rows, preferred_element_type=f32
        )
        delta_keys += lax.dot_general(delta_scores, head, over_rows, preferred_element_type=f32)
        delta_head = jnp.dot(delta_scores, keys[...], preferred_element_type=f32) * scaling
        low, high = turned(delta_head, cosine, -sine)
        out[:, start : start + half] = low.astype(bf16)
        out[:, start + half : start + HEAD_SIZE] = high.astype(bf16)
    low, high = turned(delta_keys * scaling, cosine, -sine)
    out[:, width : width + half] = low.astype(bf16)
    out[:, width + half : width + HEAD_SIZE] = high.astype(bf16)
    out[:, width + HEAD_SIZE :] = delta_values.astype(bf16)


def by_sequence(body, numbers, arrays, widths, name):
    rows = arrays[0].shape[0] // 2

    def spec(columns):
        return pl.BlockSpec((rows, columns), lambda b, n: (b, 0))

    return pl.pallas_call(
        body,
        out_shape=[jax.ShapeDtypeStruct((2 * rows, w), bf16) for w in widths],
        grid_spec=pltpu.PrefetchScalarGridSpec(
            num_scalar_prefetch=1,
            grid=(2,),
            in_specs=[spec(v.shape[1]) for v in arrays],
            out_specs=[spec(w) for w in widths],
        ),
        name=name,
    )(numbers, *arrays)


def per_device(
    layer_input,
    teacher,
    lengths,
    seq_order,
    gain_attn,
    w_query,
    key_projection_weight,
    value_projection_weight,
    w_out,
    gain_mlp,
    w_gate,
    w_up,
    w_down,
):
    token_rows, width = layer_input.shape
    slots = token_rows * lax.axis_size("tensor")
    devices = lax.axis_size("dp")
    tokens_all = slots * devices
    chips = devices // 2
    ring = Ring(chips)
    me = lax.axis_index("dp")
    side = lax.axis_index("tensor")
    chip, core = me // 2, me % 2
    first_core = core == 0
    place = jnp.array(ring.place, dtype=jnp.int32)
    here = place[chip]
    piece = gain_attn.shape[0]

    numbers = jnp.arange(chips, dtype=jnp.int32)
    order = jnp.array(ring_order(chips), dtype=jnp.int32)
    from_low = 2 * order[(here - numbers) % chips]
    from_high = 2 * order[(here + numbers) % chips] + 1
    half = chips // 2
    to_relative = jnp.concatenate(
        [from_low[half:], from_high[half:], from_low[:half], from_high[:half]]
    )
    behind, before = (here - place) % chips, (place - here) % chips
    to_natural = jnp.stack(
        [
            jnp.where(behind < half, behind + 2 * half, behind - half),
            jnp.where(before < half, before + 3 * half, before),
        ],
        axis=1,
    ).reshape(devices)

    def split_cores(w):
        quarter = w.shape[1] // 2
        mine = lax.dynamic_slice_in_dim(w, core * quarter, quarter, 1)
        given = lax.dynamic_slice_in_dim(w, (1 - core) * quarter, quarter, 1)
        return mine, given

    def both_rows(weights, gains=None):
        mine, given = zip(*[split_cores(w) for w in weights])
        mine, given = jnp.concatenate(mine, axis=1), jnp.concatenate(given, axis=1)
        if gains is not None:
            extra = jnp.pad(gains, ((0, 16 - gains.shape[0]), (0, mine.shape[1] - gains.shape[1])))
            mine = jnp.concatenate([mine, extra], axis=0)
            given = jnp.concatenate([given, extra], axis=0)
        taken = ring.other_core(given)
        return (
            jnp.where(first_core, mine, taken),
            jnp.where(first_core, taken, mine),
        )

    gains = jnp.stack([gain_attn, gain_mlp])
    hops = ring.chips - 1
    q_width = w_query.shape[1] // 2
    kv_width = key_projection_weight.shape[1] // 2
    qkv_width = q_width + 2 * kv_width
    out_width = w_out.shape[0] // 2
    attn_weights = Gather(
        ring,
        "attn_rows",
        *both_rows([w_query, key_projection_weight, value_projection_weight, w_out.T], gains),
        piece,
        [(0, qkv_width), (qkv_width, qkv_width + out_width)],
        below=16,
    )
    w_gate, layer_input, to_relative, lengths, _ = together(
        (w_gate, layer_input, to_relative, lengths, attn_weights.now)
    )
    gate_weights = Gather(ring, "gate_rows", *both_rows([w_gate]), piece)
    own_input = reorder(layer_input, to_relative)
    group_rows = gather_group(ring, own_input)
    for k in range(hops):
        turn(attn_weights, gate_weights)
        turn(gate_weights, attn_weights)
    up_weights = Gather(
        ring, "up_rows", *together((both_rows([w_up]), attn_weights.now))[0], piece
    )
    down_weights = Gather(
        ring, "down_rows", *together((both_rows([w_down.T]), gate_weights.now))[0], piece, split=True
    )

    sequence_numbers = jnp.stack([me, me + 1 - 2 * core])
    length = jnp.sum(
        jnp.where(seq_order[None, :] == sequence_numbers[:, None], lengths[None, :], 0), axis=1
    )
    offsets = jnp.arange(token_rows, dtype=jnp.int32)
    slot = jnp.concatenate([side * token_rows + offsets, (1 - side) * token_rows + offsets])
    inside = slot[None, :] < length[:, None]
    position = jnp.where(inside, slot[None, :], 0)
    own_valid = inside[0, :token_rows].astype(f32)[:, None]
    cosine, sine = rope_tables(position.reshape(-1), HEAD_SIZE)
    numbers = jnp.concatenate([length, side[None]]).astype(jnp.int32)
    own_rows = own_input.astype(f32)
    attn_scale = rms_scale(own_rows)

    qkv_proj, out_proj_t, gain_rows = attn_weights.buffers
    gain_rows = gain_rows[:2].astype(f32)
    attn_gain, mlp_gain = gain_rows[:1], gain_rows[1:]
    gate_proj = gate_weights.buffers[0]

    def forward():
        group_input = group_rows.astype(f32)
        normed = (group_input * rms_scale(group_input) * attn_gain).astype(bf16)
        qkv = jnp.dot(normed, qkv_proj, preferred_element_type=f32)
        normed, qkv = yield Held(normed, qkv)
        attended = by_sequence(
            attend_body,
            numbers,
            [qkv, cosine, sine],
            [q_width, kv_width, kv_width, q_width],
            "attend",
        )
        attended = yield Held(attended)
        parts = lax.dot_general(attended[3], out_proj_t, over_last, preferred_element_type=f32)
        parts = yield Held(parts)
        shared = scatter_group(ring, parts)
        own_teacher = yield Held(reorder(teacher, to_relative))
        yield ()
        shared = yield Held(shared)
        middle = own_rows + shared
        mlp_scale = rms_scale(middle)
        normed_mlp = gather_group(ring, (middle * mlp_scale * mlp_gain).astype(bf16))
        yield ()
        yield ()
        normed_mlp = yield Held(normed_mlp)
        gate = jnp.dot(normed_mlp, gate_proj, preferred_element_type=f32)
        gate = yield Held(gate)
        return (
            own_teacher,
            (normed, *attended),
            (middle, mlp_scale, normed_mlp, gate),
        )

    stages = Stages(forward())
    for k in range(hops):
        stages.turn(up_weights, down_weights)
        stages.turn(down_weights, up_weights)
    own_teacher, attn_kept, mlp_kept = stages.finish()
    normed, rot_queries, rot_keys, values, mixed = attn_kept
    middle, mlp_scale, normed_mlp, gate = mlp_kept
    up_proj = up_weights.buffers[0]
    down_far, down_near = down_weights.buffers
    count = jnp.sum(lengths).astype(f32)

    up = jnp.dot(normed_mlp, up_proj, preferred_element_type=f32)
    sigmoid_gate = jax.nn.sigmoid(gate)
    hidden = (gate * sigmoid_gate * up).astype(bf16)
    cut = width // 2

    def half_sum(rows, proj_t):
        parts = lax.dot_general(rows, proj_t, over_last, preferred_element_type=f32)
        return core_sum(ring, parts)

    def output(shared, columns):
        result = middle[:, columns] + shared
        error = (result - own_teacher[:, columns].astype(f32)) * own_valid
        delta = error * (tokens_all / count)
        return result, error, delta, delta.astype(bf16)

    def down_grad_of(branch):
        return lax.dot_general(branch, hidden, over_rows, preferred_element_type=f32).astype(bf16)

    half_far = half_sum(hidden, down_far)
    half_near = half_sum(together((hidden, half_far))[0], down_near)
    result_far, error_far, delta_far, low_far = output(tensor_sum(half_far), slice(0, cut))
    shared_near = together((tensor_sum(half_near), low_far))[0]
    result_near, error_near, delta_near, low_near = output(shared_near, slice(cut, width))
    branch_far = gather_group(ring, low_far, low_near)
    grad_far = down_grad_of(branch_far)
    branch_near = gather_group(ring, low_near)
    down_sums = Scatter(ring, [grad_far], None, piece)
    result = jnp.concatenate([result_far, result_near], axis=1)
    delta_result = jnp.concatenate([delta_far, delta_near], axis=1)
    squared = jnp.sum(error_far * error_far) + jnp.sum(error_near * error_near)

    def backward():
        branch = together((branch_far, grad_far))[0]
        first = jnp.dot(branch, down_far, preferred_element_type=f32)
        first = yield Held(first)
        delta_hidden = first + jnp.dot(branch_near, down_near, preferred_element_type=f32)
        delta_gate = (
            delta_hidden * up * sigmoid_gate * (1.0 + gate * (1.0 - sigmoid_gate))
        ).astype(bf16)
        delta_up = (delta_hidden * gate * sigmoid_gate).astype(bf16)
        delta_gate, delta_up = yield Held(delta_gate, delta_up)
        grad_gate = lax.dot_general(
            normed_mlp, delta_gate, over_rows, preferred_element_type=f32
        ).astype(bf16)
        grad_gate, delta_up = yield Held(grad_gate, delta_up)
        grad_up = lax.dot_general(
            normed_mlp, delta_up, over_rows, preferred_element_type=f32
        ).astype(bf16)
        gate_up.extend([grad_gate, grad_up])
        delta_gate, delta_up = yield Held(delta_gate, delta_up)
        def from_hidden(rows):
            return lax.dot_general(
                delta_gate[rows], gate_proj, over_last, preferred_element_type=f32
            ) + lax.dot_general(delta_up[rows], up_proj, over_last, preferred_element_type=f32)

        given, delta_gate, delta_up = yield Held(
            from_hidden(slice(slots, None)).astype(bf16), delta_gate, delta_up
        )
        taken = ring.other_core(given)
        parts = yield Held(from_hidden(slice(0, slots)))
        delta_normed_mlp = tensor_sum(parts + taken.astype(f32))
        placed = together((result.astype(bf16), parts))[0]
        activations = yield Held(reorder(placed, to_natural))
        delta_normed_mlp = yield Held(delta_normed_mlp)
        gain_mlp_part = jnp.sum(delta_normed_mlp * middle * mlp_scale, axis=0)
        weighted_mlp = mlp_gain * delta_normed_mlp
        delta_middle = (
            delta_result
            + mlp_scale * weighted_mlp
            - middle * mlp_scale**3 * jnp.mean(middle * weighted_mlp, axis=-1, keepdims=True)
        )
        attn_low_rows = gather_group(ring, delta_middle.astype(bf16))
        yield ()
        attn_low_rows = yield Held(attn_low_rows)
        grad_out_t = lax.dot_general(attn_low_rows, mixed, over_rows, preferred_element_type=f32)
        delta_mixed = jnp.dot(attn_low_rows, out_proj_t, preferred_element_type=f32).astype(bf16)
        grad_out_t = grad_out_t.astype(bf16)
        delta_qkv = by_sequence(
            attend_back_body,
            numbers,
            [rot_queries, rot_keys, values, delta_mixed, cosine, sine],
            [qkv_width],
            "attend_back",
        )[0]
        delta_qkv, grad_out_t = yield Held(delta_qkv, grad_out_t)
        grad_qkv = lax.dot_general(normed, delta_qkv, over_rows, preferred_element_type=f32)
        return (
            activations,
            gain_mlp_part,
            delta_middle,
            delta_qkv,
            [jnp.concatenate([grad_qkv.astype(bf16), grad_out_t], axis=1)],
        )

    def finish(sums):
        low, high = sums.now
        kept = jnp.where(first_core, low, high)
        taken = ring.other_core(jnp.where(first_core, high, low).astype(bf16)).astype(f32)
        return kept, taken

    def whole(kept, taken):
        return jnp.concatenate(
            [jnp.where(first_core, kept, taken), jnp.where(first_core, taken, kept)], axis=1
        )

    def halves(grads):
        return [g[: width // 2] for g in grads], [g[width // 2 :] for g in grads]

    gate_up = []
    stages = Stages(backward())
    for k in range(3):
        stages.turn(down_sums)
    gate_up_sums = Scatter(ring, *halves(gate_up), piece)
    grad_near = down_grad_of(together((branch_near, gate_up_sums.now))[0])
    down_sums.parts = ([grad_near], down_sums.parts[1])
    stages.turn(down_sums, gate_up_sums)
    while down_sums.left:
        stages.turn(gate_up_sums, down_sums)
        stages.turn(down_sums, gate_up_sums)
    down_grad = whole(*finish(down_sums)).T
    while not stages.over and gate_up_sums.left:
        stages.turn(gate_up_sums, None, down_grad)
    assert stages.over
    activations, gain_mlp_part, delta_middle, delta_qkv, attn_grads = stages.finish()
    attn_sums = Scatter(ring, *halves(attn_grads), piece)

    def closing():
        delta_normed = scatter_group(
            ring,
            lax.dot_general(
                together((delta_qkv, attn_sums.now))[0],
                qkv_proj,
                over_last,
                preferred_element_type=f32,
            ),
        )
        yield ()
        yield ()
        yield ()
        delta_normed = yield Held(delta_normed)
        gain_attn_part = jnp.sum(delta_normed * own_rows * attn_scale, axis=0)
        weighted_attn = attn_gain * delta_normed
        input_grad = (
            delta_middle
            + attn_scale * weighted_attn
            - own_rows * attn_scale**3 * jnp.mean(own_rows * weighted_attn, axis=-1, keepdims=True)
        )
        natural = jnp.stack([gain_mlp_part, gain_attn_part], axis=0).reshape(2, devices, piece)[
            :, to_natural
        ]
        sums = jnp.concatenate(
            [natural.reshape(2 * devices, piece), jnp.full((8, piece), squared)], axis=0
        )
        sums, input_grad = yield Held(sums + other_tensor(sums), input_grad.astype(bf16))
        input_grad = reorder(input_grad, to_natural)
        step = 1
        while step < devices:
            pairs = [(d, d ^ step) for d in range(devices)]
            sums, _ = yield Held(sums + lax.ppermute(sums, "dp", pairs), input_grad)
            step *= 2
        return input_grad, sums

    stages = Stages(closing())
    while gate_up_sums.left:
        stages.turn(gate_up_sums, attn_sums, down_grad)
        stages.turn(attn_sums, gate_up_sums)
    kept, taken = finish(gate_up_sums)
    gate_width = w_gate.shape[1] // 2
    gate_grad = whole(kept[:, :gate_width], taken[:, :gate_width])
    up_grad = whole(kept[:, gate_width:], taken[:, gate_width:])
    stages.turn(attn_sums)
    while attn_sums.left:
        stages.turn(attn_sums, None, (gate_grad, up_grad))
    input_grad, totals = stages.finish()
    gain_mlp_grad = lax.dynamic_slice_in_dim(totals, me, 1, 0)[0]
    gain_attn_grad = lax.dynamic_slice_in_dim(totals, devices + me, 1, 0)[0]
    distill_loss = totals[2 * devices, 0] / (2.0 * width * count)
    attn_kept, attn_taken = finish(attn_sums)
    cuts = [0, q_width, q_width + kv_width, qkv_width, attn_kept.shape[1]]
    query_grad, key_grad, value_grad, out_grad_t = [
        whole(attn_kept[:, a:b], attn_taken[:, a:b]) for a, b in zip(cuts[:-1], cuts[1:])
    ]
    return (
        activations,
        input_grad,
        gain_attn_grad,
        query_grad,
        key_grad,
        value_grad,
        out_grad_t.T,
        gain_mlp_grad,
        gate_grad,
        up_grad,
        down_grad,
        distill_loss,
    )


def solution(mesh):
    placed = (
        P(("dp", "tensor"), None),
        P(("dp", "tensor"), None),
        P(),
        P(),
        P("dp"),
        P("dp", "tensor"),
        P("dp", "tensor"),
        P("dp", "tensor"),
        P("tensor", "dp"),
        P("dp"),
        P("dp", "tensor"),
        P("dp", "tensor"),
        P("tensor", "dp"),
    )
    return jax.shard_map(
        per_device,
        mesh=mesh,
        in_specs=placed,
        out_specs=(
            P(("dp", "tensor"), None),
            P(("dp", "tensor"), None),
            P("dp"),
            P("dp", "tensor"),
            P("dp", "tensor"),
            P("dp", "tensor"),
            P("tensor", "dp"),
            P("dp"),
            P("dp", "tensor"),
            P("dp", "tensor"),
            P("tensor", "dp"),
            P(),
        ),
        check_vma=False,
    )
```

```python
import jax
import jax.numpy as jnp
from jax import lax
from jax.experimental import pallas as pl
from jax.experimental.pallas import tpu as pltpu
from jax.sharding import PartitionSpec as P

HEAD_SIZE = 256
LANES = 128
EPS = 1e-06
ROPE_BASE = 1000042.0
over_rows = (((0,), (0,)), ((), ()))
over_last = (((1,), (1,)), ((), ()))
plain = (((1,), (0,)), ((), ()))
f32 = jnp.float32
bf16 = jnp.bfloat16


def rms_scale(value_rows):
    return lax.rsqrt(jnp.mean(value_rows * value_rows, axis=-1, keepdims=True) + EPS)


def rope_tables(position, width):
    half = width // 2
    exponent = jnp.arange(half, dtype=f32) * (-2.0 / width)
    frequency = jnp.exp(exponent * jnp.log(f32(ROPE_BASE)))
    angle = position.astype(f32)[..., None] * frequency
    return (jnp.cos(angle), jnp.sin(angle))


def ring_order(chips):
    column = chips // 2
    return [2 * i for i in range(column)] + [2 * i + 1 for i in reversed(range(column))]


class Ring:
    def __init__(self, chips):
        self.chips = chips
        order = ring_order(chips)
        self.place = [order.index(c) for c in range(chips)]
        hop = [(order[i], order[(i + 1) % chips]) for i in range(chips)]
        self.up = [(2 * a + c, 2 * b + c) for a, b in hop for c in range(2)]
        self.down = [(b, a) for a, b in self.up]
        self.swap = [(d, d ^ 1) for d in range(2 * chips)]

    def ahead(self, v):
        return lax.ppermute(v, "dp", self.up)

    def back(self, v):
        return lax.ppermute(v, "dp", self.down)

    def other_core(self, v):
        return lax.ppermute(v, "dp", self.swap)


def other_tensor(v):
    return lax.ppermute(v, "tensor", [(0, 1), (1, 0)])


def together(values):
    return lax.optimization_barrier(values)


def unfilled(shape, name):
    return pl.pallas_call(
        lambda out: None,
        out_shape=jax.ShapeDtypeStruct(shape, bf16),
        out_specs=pl.BlockSpec(memory_space=pl.ANY),
        name=name,
    )()


class Gather:
    def __init__(self, ring, name, low, high, rows, cuts=None, split=False, below=0):
        self.ring, self.size, self.split, self.below = ring, rows, split, below
        self.now = (low, high)
        self.cuts = cuts or [(0, low.shape[1])]
        height = 2 * ring.chips * rows
        shapes = [(height, b - a) for a, b in self.cuts]
        if split:
            shapes = [(height // 2, low.shape[1])] * 2
        if below:
            shapes.append((below, height))
        self.buffers = [unfilled(v, f"{name}_{i}") for i, v in enumerate(shapes)]
        self.hops = 0
        self.store()

    def store(self):
        half = self.ring.chips // 2
        k, self.hops = self.hops, self.hops + 1
        for side, rows in enumerate(self.now):
            at = k + (side - 1) * half if k >= half else k + (side + 2) * half
            if self.split:
                which = int(k < half)
                start = (at - which * 2 * half) * self.size
                self.buffers[which] = lax.dynamic_update_slice(
                    self.buffers[which], rows[: self.size], (start, 0)
                )
                continue
            for i, (a, b) in enumerate(self.cuts):
                self.buffers[i] = lax.dynamic_update_slice(
                    self.buffers[i], rows[: self.size, a:b], (at * self.size, 0)
                )
            if self.below:
                self.buffers[-1] = lax.dynamic_update_slice(
                    self.buffers[-1],
                    rows[self.size : self.size + self.below, : self.size],
                    (0, at * self.size),
                )

    def move(self):
        return self.ring.ahead(self.now[0]), self.ring.back(self.now[1])

    def take(self, moved):
        self.now = moved
        self.store()


class Scatter:
    def __init__(self, ring, far, near, rows):
        self.ring, self.parts, self.size = ring, (near, far), rows
        self.buffers = []
        self.left = ring.chips - 1
        self.now = (self.block(0), self.block(1))

    def block(self, side):
        half = self.ring.chips // 2
        grads = self.parts[self.left // half]
        start = (side * half + self.left % half) * self.size
        return jnp.concatenate([g[start : start + self.size] for g in grads], axis=1)

    def move(self):
        return self.ring.back(self.now[0]), self.ring.ahead(self.now[1])

    def take(self, moved):
        self.left -= 1
        sums = [m.astype(f32) + self.block(side).astype(f32) for side, m in enumerate(moved)]
        self.now = tuple(sums if self.left == 0 else [v.astype(bf16) for v in sums])


class Held:
    def __init__(self, *value):
        self.value = value if len(value) > 1 else value[0]


def turn(lane, other=None, values=(), held=()):
    moved, _, held, lane.buffers = together(
        (lane.move(), other.now if other else (), held, lane.buffers)
    )
    lane.take(moved)
    values, held, _ = together((values, held, lane.now))
    return values, held


class Stages:
    def __init__(self, generator):
        self.generator = generator
        self.result = None
        self.value = ()
        self.over = False
        self.advance(None)

    def advance(self, value):
        if not self.over:
            try:
                self.value = self.generator.send(value)
            except StopIteration as end:
                self.result, self.over, self.value = end.value, True, ()

    def turn(self, lane, other=None, extra=()):
        if isinstance(self.value, Held):
            value = turn(lane, other, (), (self.value.value, extra))[1][0]
        else:
            value = turn(lane, other, self.value, extra)[0]
        self.advance(value)

    def finish(self):
        while not self.over:
            self.advance(self.value.value if isinstance(self.value, Held) else self.value)
        return self.result


def gather_group(ring, rows, before=()):
    across = together((other_tensor(rows), before))[0]
    beside = ring.other_core(rows)
    return jnp.concatenate([rows, across, beside, ring.other_core(across)], axis=0)


def core_sum(ring, parts):
    half = parts.shape[0] // 2
    return parts[:half] + ring.other_core(parts[half:].astype(bf16)).astype(f32)


def tensor_sum(rows):
    half = rows.shape[0] // 2
    return rows[:half] + other_tensor(rows[half:].astype(bf16)).astype(f32)


def scatter_group(ring, parts):
    return tensor_sum(core_sum(ring, parts))


def copy_blocks(table, source, target):
    for k in range(target.shape[1] // LANES):
        start = pl.multiple_of(table[k] * LANES, LANES)
        target[:, k * LANES : (k + 1) * LANES] = source[:, pl.ds(start, LANES)]


def reorder(rows, table):
    height, width = rows.shape
    step = height // 4
    return pl.pallas_call(
        copy_blocks,
        out_shape=jax.ShapeDtypeStruct(rows.shape, rows.dtype),
        grid_spec=pltpu.PrefetchScalarGridSpec(
            num_scalar_prefetch=1,
            grid=(height // step,),
            in_specs=[pl.BlockSpec((step, width), lambda k, t: (k, 0))],
            out_specs=pl.BlockSpec((step, width), lambda k, t: (k, 0)),
        ),
        name="reorder",
    )(table, rows)


def visible(numbers, shape):
    def slot(axis):
        offset = lax.broadcasted_iota(jnp.int32, shape, axis)
        start = numbers[2] * (shape[0] // 2)
        return jnp.where(offset < shape[0] // 2, offset + start, offset - start)

    query, key = slot(0), slot(1)
    inside = query < numbers[pl.program_id(0)]
    return jnp.where(inside, key - query, jnp.abs(key - query)) <= 0


def turned(heads, cosine, sine):
    half = heads.shape[1] // 2
    first, second = heads[:, :half], heads[:, half:]
    return first * cosine - second * sine, second * cosine + first * sine


def weights_of(queries, keys, allowed):
    scores = lax.dot_general(queries, keys, over_last, preferred_element_type=f32)
    scores = jnp.where(allowed, scores * HEAD_SIZE ** (-0.5), -1e30)
    shifted = jnp.exp(scores - jnp.max(scores, axis=-1, keepdims=True))
    return shifted / jnp.sum(shifted, axis=-1, keepdims=True)


def attend_body(numbers, qkv, cosine, sine, queries, keys, values, mixed):
    rows, width = queries.shape
    half = HEAD_SIZE // 2
    cosine, sine = cosine[...], sine[...]
    key_low, key_high = turned(qkv[:, width : width + HEAD_SIZE], cosine, sine)
    keys[:, :half] = key_low.astype(bf16)
    keys[:, half:] = key_high.astype(bf16)
    values[...] = qkv[:, width + HEAD_SIZE :].astype(bf16)
    allowed = visible(numbers, (rows, rows))
    for start in range(0, width, HEAD_SIZE):
        low, high = turned(qkv[:, start : start + HEAD_SIZE], cosine, sine)
        queries[:, start : start + half] = low.astype(bf16)
        queries[:, start + half : start + HEAD_SIZE] = high.astype(bf16)
        probs = weights_of(queries[:, start : start + HEAD_SIZE], keys[...], allowed)
        mixed[:, start : start + HEAD_SIZE] = jnp.dot(
            probs.astype(bf16), values[...], preferred_element_type=f32
        ).astype(bf16)


def attend_back_body(numbers, queries, keys, values, delta, cosine, sine, out):
    rows, width = queries.shape
    half = HEAD_SIZE // 2
    scaling = HEAD_SIZE ** (-0.5)
    cosine, sine = cosine[...], sine[...]
    allowed = visible(numbers, (rows, rows))
    delta_keys = jnp.zeros((rows, HEAD_SIZE), f32)
    delta_values = jnp.zeros((rows, HEAD_SIZE), f32)
    for start in range(0, width, HEAD_SIZE):
        head = queries[:, start : start + HEAD_SIZE]
        delta_mixed = delta[:, start : start + HEAD_SIZE]
        probs = weights_of(head, keys[...], allowed)
        delta_probs = lax.dot_general(
            delta_mixed, values[...], over_last, preferred_element_type=f32
        )
        inner = jnp.sum(probs * delta_probs, axis=-1, keepdims=True)
        delta_scores = (probs * (delta_probs - inner)).astype(bf16)
        delta_values += lax.dot_general(
            probs.astype(bf16), delta_mixed, over_rows, preferred_element_type=f32
        )
        delta_keys += lax.dot_general(delta_scores, head, over_rows, preferred_element_type=f32)
        delta_head = jnp.dot(delta_scores, keys[...], preferred_element_type=f32) * scaling
        low, high = turned(delta_head, cosine, -sine)
        out[:, start : start + half] = low.astype(bf16)
        out[:, start + half : start + HEAD_SIZE] = high.astype(bf16)
    low, high = turned(delta_keys * scaling, cosine, -sine)
    out[:, width : width + half] = low.astype(bf16)
    out[:, width + half : width + HEAD_SIZE] = high.astype(bf16)
    out[:, width + HEAD_SIZE :] = delta_values.astype(bf16)


def by_sequence(body, numbers, arrays, widths, name):
    rows = arrays[0].shape[0] // 2

    def spec(columns):
        return pl.BlockSpec((rows, columns), lambda b, n: (b, 0))

    return pl.pallas_call(
        body,
        out_shape=[jax.ShapeDtypeStruct((2 * rows, w), bf16) for w in widths],
        grid_spec=pltpu.PrefetchScalarGridSpec(
            num_scalar_prefetch=1,
            grid=(2,),
            in_specs=[spec(v.shape[1]) for v in arrays],
            out_specs=[spec(w) for w in widths],
        ),
        name=name,
    )(numbers, *arrays)


def per_device(
    layer_input,
    teacher,
    lengths,
    seq_order,
    gain_attn,
    w_query,
    key_projection_weight,
    value_projection_weight,
    w_out,
    gain_mlp,
    w_gate,
    w_up,
    w_down,
):
    token_rows, width = layer_input.shape
    slots = token_rows * lax.axis_size("tensor")
    devices = lax.axis_size("dp")
    tokens_all = slots * devices
    chips = devices // 2
    ring = Ring(chips)
    me = lax.axis_index("dp")
    side = lax.axis_index("tensor")
    chip, core = me // 2, me % 2
    first_core = core == 0
    place = jnp.array(ring.place, dtype=jnp.int32)
    here = place[chip]
    piece = gain_attn.shape[0]

    numbers = jnp.arange(chips, dtype=jnp.int32)
    order = jnp.array(ring_order(chips), dtype=jnp.int32)
    from_low = 2 * order[(here - numbers) % chips]
    from_high = 2 * order[(here + numbers) % chips] + 1
    half = chips // 2
    to_relative = jnp.concatenate(
        [from_low[half:], from_high[half:], from_low[:half], from_high[:half]]
    )
    behind, before = (here - place) % chips, (place - here) % chips
    to_natural = jnp.stack(
        [
            jnp.where(behind < half, behind + 2 * half, behind - half),
            jnp.where(before < half, before + 3 * half, before),
        ],
        axis=1,
    ).reshape(devices)

    def split_cores(w):
        quarter = w.shape[1] // 2
        mine = lax.dynamic_slice_in_dim(w, core * quarter, quarter, 1)
        given = lax.dynamic_slice_in_dim(w, (1 - core) * quarter, quarter, 1)
        return mine, given

    def both_rows(weights, gains=None):
        mine, given = zip(*[split_cores(w) for w in weights])
        mine, given = jnp.concatenate(mine, axis=1), jnp.concatenate(given, axis=1)
        if gains is not None:
            extra = jnp.pad(gains, ((0, 16 - gains.shape[0]), (0, mine.shape[1] - gains.shape[1])))
            mine = jnp.concatenate([mine, extra], axis=0)
            given = jnp.concatenate([given, extra], axis=0)
        taken = ring.other_core(given)
        return (
            jnp.where(first_core, mine, taken),
            jnp.where(first_core, taken, mine),
        )

    gains = jnp.stack([gain_attn, gain_mlp])
    hops = ring.chips - 1
    q_width = w_query.shape[1] // 2
    kv_width = key_projection_weight.shape[1] // 2
    qkv_width = q_width + 2 * kv_width
    out_width = w_out.shape[0] // 2
    attn_weights = Gather(
        ring,
        "attn_rows",
        *both_rows([w_query, key_projection_weight, value_projection_weight, w_out.T], gains),
        piece,
        [(0, qkv_width), (qkv_width, qkv_width + out_width)],
        below=16,
    )
    w_gate, layer_input, to_relative, lengths, _ = together(
        (w_gate, layer_input, to_relative, lengths, attn_weights.now)
    )
    gate_weights = Gather(ring, "gate_rows", *both_rows([w_gate]), piece)
    own_input = reorder(layer_input, to_relative)
    group_rows = gather_group(ring, own_input)
    for k in range(hops):
        turn(attn_weights, gate_weights)
        if k == hops - 2:
            group_rows = together((group_rows, attn_weights.now))[0]
        turn(gate_weights, attn_weights)
    up_weights = Gather(
        ring, "up_rows", *together((both_rows([w_up]), attn_weights.now))[0], piece
    )
    down_weights = Gather(
        ring, "down_rows", *together((both_rows([w_down.T]), gate_weights.now))[0], piece, split=True
    )

    sequence_numbers = jnp.stack([me, me + 1 - 2 * core])
    length = jnp.sum(
        jnp.where(seq_order[None, :] == sequence_numbers[:, None], lengths[None, :], 0), axis=1
    )
    offsets = jnp.arange(token_rows, dtype=jnp.int32)
    slot = jnp.concatenate([side * token_rows + offsets, (1 - side) * token_rows + offsets])
    inside = slot[None, :] < length[:, None]
    position = jnp.where(inside, slot[None, :], 0)
    own_valid = inside[0, :token_rows].astype(f32)[:, None]
    cosine, sine = rope_tables(position.reshape(-1), HEAD_SIZE)
    numbers = jnp.concatenate([length, side[None]]).astype(jnp.int32)
    own_rows = own_input.astype(f32)
    attn_scale = rms_scale(own_rows)

    qkv_proj, out_proj_t, gain_rows = attn_weights.buffers
    gain_rows = gain_rows[:2].astype(f32)
    attn_gain, mlp_gain = gain_rows[:1], gain_rows[1:]
    gate_proj = gate_weights.buffers[0]

    def forward():
        group_input = group_rows.astype(f32)
        normed = (group_input * rms_scale(group_input) * attn_gain).astype(bf16)
        qkv = jnp.dot(normed, qkv_proj, preferred_element_type=f32)
        normed, qkv = yield Held(normed, qkv)
        attended = by_sequence(
            attend_body,
            numbers,
            [qkv, cosine, sine],
            [q_width, kv_width, kv_width, q_width],
            "attend",
        )
        attended = yield Held(attended)
        parts = lax.dot_general(attended[3], out_proj_t, over_last, preferred_element_type=f32)
        parts = yield Held(parts)
        shared = scatter_group(ring, parts)
        own_teacher = yield Held(reorder(teacher, to_relative))
        yield ()
        shared = yield Held(shared)
        middle = own_rows + shared
        mlp_scale = rms_scale(middle)
        normed_mlp = gather_group(ring, (middle * mlp_scale * mlp_gain).astype(bf16))
        yield ()
        yield ()
        normed_mlp = yield Held(normed_mlp)
        gate = jnp.dot(normed_mlp, gate_proj, preferred_element_type=f32)
        gate = yield Held(gate)
        return (
            own_teacher,
            (normed, *attended),
            (middle, mlp_scale, normed_mlp, gate),
        )

    stages = Stages(forward())
    for k in range(hops):
        stages.turn(up_weights, down_weights)
        stages.turn(down_weights, up_weights)
    own_teacher, attn_kept, mlp_kept = stages.finish()
    normed, rot_queries, rot_keys, values, mixed = attn_kept
    middle, mlp_scale, normed_mlp, gate = mlp_kept
    up_proj = up_weights.buffers[0]
    down_far, down_near = down_weights.buffers
    count = jnp.sum(lengths).astype(f32)

    up = jnp.dot(normed_mlp, up_proj, preferred_element_type=f32)
    sigmoid_gate = jax.nn.sigmoid(gate)
    hidden = (gate * sigmoid_gate * up).astype(bf16)
    cut = width // 2

    def half_sum(rows, proj_t):
        parts = lax.dot_general(rows, proj_t, over_last, preferred_element_type=f32)
        return core_sum(ring, parts)

    def output(shared, columns):
        result = middle[:, columns] + shared
        error = (result - own_teacher[:, columns].astype(f32)) * own_valid
        delta = error * (tokens_all / count)
        return result, error, delta, delta.astype(bf16)

    def down_grad_of(branch):
        return lax.dot_general(branch, hidden, over_rows, preferred_element_type=f32).astype(bf16)

    half_far = half_sum(hidden, down_far)
    half_near = half_sum(together((hidden, half_far))[0], down_near)
    result_far, error_far, delta_far, low_far = output(tensor_sum(half_far), slice(0, cut))
    branch_far = gather_group(ring, low_far)
    grad_far = down_grad_of(branch_far)
    shared_near = together((tensor_sum(half_near), low_far))[0]
    result_near, error_near, delta_near, low_near = output(shared_near, slice(cut, width))
    branch_near = gather_group(ring, low_near)
    down_sums = Scatter(ring, [grad_far], None, piece)
    result = jnp.concatenate([result_far, result_near], axis=1)
    delta_result = jnp.concatenate([delta_far, delta_near], axis=1)
    squared = jnp.sum(error_far * error_far) + jnp.sum(error_near * error_near)

    def backward():
        branch = together((branch_far, grad_far))[0]
        first = jnp.dot(branch, down_far, preferred_element_type=f32)
        first = yield Held(first)
        delta_hidden = first + jnp.dot(branch_near, down_near, preferred_element_type=f32)
        delta_gate = (
            delta_hidden * up * sigmoid_gate * (1.0 + gate * (1.0 - sigmoid_gate))
        ).astype(bf16)
        delta_up = (delta_hidden * gate * sigmoid_gate).astype(bf16)
        delta_gate, delta_up = yield Held(delta_gate, delta_up)
        grad_gate = lax.dot_general(
            normed_mlp, delta_gate, over_rows, preferred_element_type=f32
        ).astype(bf16)
        grad_gate, delta_up = yield Held(grad_gate, delta_up)
        grad_up = lax.dot_general(
            normed_mlp, delta_up, over_rows, preferred_element_type=f32
        ).astype(bf16)
        gate_up.extend([grad_gate, grad_up])
        delta_gate, delta_up = yield Held(delta_gate, delta_up)
        def from_hidden(rows):
            return lax.dot_general(
                delta_gate[rows], gate_proj, over_last, preferred_element_type=f32
            ) + lax.dot_general(delta_up[rows], up_proj, over_last, preferred_element_type=f32)

        given, delta_gate, delta_up = yield Held(
            from_hidden(slice(slots, None)).astype(bf16), delta_gate, delta_up
        )
        taken = ring.other_core(given)
        parts = yield Held(from_hidden(slice(0, slots)))
        parts = parts + taken.astype(f32)
        delta_normed_mlp = tensor_sum(parts)
        activations = reorder(together((result.astype(bf16), parts))[0], to_natural)
        yield ()
        delta_normed_mlp, activations = yield Held(delta_normed_mlp, activations)
        gain_mlp_part = jnp.sum(delta_normed_mlp * middle * mlp_scale, axis=0)
        weighted_mlp = mlp_gain * delta_normed_mlp
        delta_middle = (
            delta_result
            + mlp_scale * weighted_mlp
            - middle * mlp_scale**3 * jnp.mean(middle * weighted_mlp, axis=-1, keepdims=True)
        )
        attn_low_rows = gather_group(ring, delta_middle.astype(bf16))
        yield ()
        yield ()
        attn_low_rows = yield Held(attn_low_rows)
        grad_out_t = lax.dot_general(attn_low_rows, mixed, over_rows, preferred_element_type=f32)
        delta_mixed = jnp.dot(attn_low_rows, out_proj_t, preferred_element_type=f32).astype(bf16)
        grad_out_t = grad_out_t.astype(bf16)
        delta_qkv = by_sequence(
            attend_back_body,
            numbers,
            [rot_queries, rot_keys, values, delta_mixed, cosine, sine],
            [qkv_width],
            "attend_back",
        )[0]
        delta_qkv, grad_out_t = yield Held(delta_qkv, grad_out_t)
        grad_qkv = lax.dot_general(normed, delta_qkv, over_rows, preferred_element_type=f32)
        return (
            activations,
            gain_mlp_part,
            delta_middle,
            delta_qkv,
            [jnp.concatenate([grad_qkv.astype(bf16), grad_out_t], axis=1)],
        )

    def finish(sums):
        low, high = sums.now
        kept = jnp.where(first_core, low, high)
        taken = ring.other_core(jnp.where(first_core, high, low).astype(bf16)).astype(f32)
        return kept, taken

    def whole(kept, taken):
        return jnp.concatenate(
            [jnp.where(first_core, kept, taken), jnp.where(first_core, taken, kept)], axis=1
        )

    def halves(grads):
        return [g[: width // 2] for g in grads], [g[width // 2 :] for g in grads]

    gate_up = []
    stages = Stages(backward())
    for k in range(3):
        stages.turn(down_sums)
    gate_up_sums = Scatter(ring, *halves(gate_up), piece)
    grad_near = down_grad_of(together((branch_near, gate_up_sums.now))[0])
    down_sums.parts = ([grad_near], down_sums.parts[1])
    stages.turn(down_sums, gate_up_sums)
    while down_sums.left > 1:
        stages.turn(gate_up_sums, down_sums)
        stages.turn(down_sums, gate_up_sums)
    stages.turn(gate_up_sums, down_sums)
    stages.turn(gate_up_sums, down_sums)
    stages.turn(down_sums, gate_up_sums)
    down_grad = whole(*finish(down_sums)).T
    while not stages.over and gate_up_sums.left:
        stages.turn(gate_up_sums, None, down_grad)
    assert stages.over
    activations, gain_mlp_part, delta_middle, delta_qkv, attn_grads = stages.finish()
    attn_sums = Scatter(ring, *halves(attn_grads), piece)

    def closing():
        delta_normed = scatter_group(
            ring,
            lax.dot_general(
                together((delta_qkv, attn_sums.now))[0],
                qkv_proj,
                over_last,
                preferred_element_type=f32,
            ),
        )
        yield ()
        yield ()
        yield ()
        delta_normed = yield Held(delta_normed)
        gain_attn_part = jnp.sum(delta_normed * own_rows * attn_scale, axis=0)
        weighted_attn = attn_gain * delta_normed
        input_grad = (
            delta_middle
            + attn_scale * weighted_attn
            - own_rows * attn_scale**3 * jnp.mean(own_rows * weighted_attn, axis=-1, keepdims=True)
        )
        natural = jnp.stack([gain_mlp_part, gain_attn_part], axis=0).reshape(2, devices, piece)[
            :, to_natural
        ]
        sums = jnp.concatenate(
            [natural.reshape(2 * devices, piece), jnp.full((8, piece), squared)], axis=0
        )
        sums, input_grad = yield Held(sums + other_tensor(sums), input_grad.astype(bf16))
        input_grad = reorder(input_grad, to_natural)
        step = 1
        while step < devices:
            pairs = [(d, d ^ step) for d in range(devices)]
            sums, _ = yield Held(sums + lax.ppermute(sums, "dp", pairs), input_grad)
            step *= 2
        return input_grad, sums

    stages = Stages(closing())
    while gate_up_sums.left:
        stages.turn(gate_up_sums, attn_sums, down_grad)
        stages.turn(attn_sums, gate_up_sums)
    kept, taken = finish(gate_up_sums)
    gate_width = w_gate.shape[1] // 2
    gate_grad = whole(kept[:, :gate_width], taken[:, :gate_width])
    up_grad = whole(kept[:, gate_width:], taken[:, gate_width:])
    stages.turn(attn_sums)
    while attn_sums.left:
        stages.turn(attn_sums, None, (gate_grad, up_grad))
    input_grad, totals = stages.finish()
    gain_mlp_grad = lax.dynamic_slice_in_dim(totals, me, 1, 0)[0]
    gain_attn_grad = lax.dynamic_slice_in_dim(totals, devices + me, 1, 0)[0]
    distill_loss = totals[2 * devices, 0] / (2.0 * width * count)
    attn_kept, attn_taken = finish(attn_sums)
    cuts = [0, q_width, q_width + kv_width, qkv_width, attn_kept.shape[1]]
    query_grad, key_grad, value_grad, out_grad_t = [
        whole(attn_kept[:, a:b], attn_taken[:, a:b]) for a, b in zip(cuts[:-1], cuts[1:])
    ]
    return (
        activations,
        input_grad,
        gain_attn_grad,
        query_grad,
        key_grad,
        value_grad,
        out_grad_t.T,
        gain_mlp_grad,
        gate_grad,
        up_grad,
        down_grad,
        distill_loss,
    )


def solution(mesh):
    placed = (
        P(("dp", "tensor"), None),
        P(("dp", "tensor"), None),
        P(),
        P(),
        P("dp"),
        P("dp", "tensor"),
        P("dp", "tensor"),
        P("dp", "tensor"),
        P("tensor", "dp"),
        P("dp"),
        P("dp", "tensor"),
        P("dp", "tensor"),
        P("tensor", "dp"),
    )
    return jax.shard_map(
        per_device,
        mesh=mesh,
        in_specs=placed,
        out_specs=(
            P(("dp", "tensor"), None),
            P(("dp", "tensor"), None),
            P("dp"),
            P("dp", "tensor"),
            P("dp", "tensor"),
            P("dp", "tensor"),
            P("tensor", "dp"),
            P("dp"),
            P("dp", "tensor"),
            P("dp", "tensor"),
            P("tensor", "dp"),
            P(),
        ),
        check_vma=False,
    )
```

```python
import jax
import jax.numpy as jnp
from jax import lax
from jax.experimental import pallas as pl
from jax.experimental.pallas import tpu as pltpu
from jax.sharding import PartitionSpec as P

HEAD_SIZE = 256
LANES = 128
EPS = 1e-06
ROPE_BASE = 1000042.0
over_rows = (((0,), (0,)), ((), ()))
over_last = (((1,), (1,)), ((), ()))
plain = (((1,), (0,)), ((), ()))
f32 = jnp.float32
bf16 = jnp.bfloat16


def rms_scale(value_rows):
    return lax.rsqrt(jnp.mean(value_rows * value_rows, axis=-1, keepdims=True) + EPS)


def rope_tables(position, width):
    half = width // 2
    exponent = jnp.arange(half, dtype=f32) * (-2.0 / width)
    frequency = jnp.exp(exponent * jnp.log(f32(ROPE_BASE)))
    angle = position.astype(f32)[..., None] * frequency
    return (jnp.cos(angle), jnp.sin(angle))


def ring_order(chips):
    column = chips // 2
    return [2 * i for i in range(column)] + [2 * i + 1 for i in reversed(range(column))]


class Ring:
    def __init__(self, chips):
        self.chips = chips
        order = ring_order(chips)
        self.place = [order.index(c) for c in range(chips)]
        hop = [(order[i], order[(i + 1) % chips]) for i in range(chips)]
        self.up = [(2 * a + c, 2 * b + c) for a, b in hop for c in range(2)]
        self.down = [(b, a) for a, b in self.up]
        self.swap = [(d, d ^ 1) for d in range(2 * chips)]

    def ahead(self, v):
        return lax.ppermute(v, "dp", self.up)

    def back(self, v):
        return lax.ppermute(v, "dp", self.down)

    def other_core(self, v):
        return lax.ppermute(v, "dp", self.swap)


def other_tensor(v):
    return lax.ppermute(v, "tensor", [(0, 1), (1, 0)])


def together(values):
    return lax.optimization_barrier(values)


def unfilled(shape, name):
    return pl.pallas_call(
        lambda out: None,
        out_shape=jax.ShapeDtypeStruct(shape, bf16),
        out_specs=pl.BlockSpec(memory_space=pl.ANY),
        name=name,
    )()


class Gather:
    def __init__(self, ring, name, low, high, rows, cuts=None, split=False, below=0):
        self.ring, self.size, self.split, self.below = ring, rows, split, below
        self.now = (low, high)
        self.cuts = cuts or [(0, low.shape[1])]
        height = 2 * ring.chips * rows
        shapes = [(height, b - a) for a, b in self.cuts]
        if split:
            shapes = [(height // 2, low.shape[1])] * 2
        if below:
            shapes.append((below, height))
        self.buffers = [unfilled(v, f"{name}_{i}") for i, v in enumerate(shapes)]
        self.hops = 0
        self.store()

    def store(self):
        half = self.ring.chips // 2
        k, self.hops = self.hops, self.hops + 1
        for side, rows in enumerate(self.now):
            at = k + (side - 1) * half if k >= half else k + (side + 2) * half
            if self.split:
                which = int(k < half)
                start = (at - which * 2 * half) * self.size
                self.buffers[which] = lax.dynamic_update_slice(
                    self.buffers[which], rows[: self.size], (start, 0)
                )
                continue
            for i, (a, b) in enumerate(self.cuts):
                self.buffers[i] = lax.dynamic_update_slice(
                    self.buffers[i], rows[: self.size, a:b], (at * self.size, 0)
                )
            if self.below:
                self.buffers[-1] = lax.dynamic_update_slice(
                    self.buffers[-1],
                    rows[self.size : self.size + self.below, : self.size],
                    (0, at * self.size),
                )

    def move(self):
        return self.ring.ahead(self.now[0]), self.ring.back(self.now[1])

    def take(self, moved):
        self.now = moved
        self.store()


class Scatter:
    def __init__(self, ring, far, near, rows):
        self.ring, self.parts, self.size = ring, (near, far), rows
        self.buffers = []
        self.left = ring.chips - 1
        self.now = (self.block(0), self.block(1))

    def block(self, side):
        half = self.ring.chips // 2
        grads = self.parts[self.left // half]
        start = (side * half + self.left % half) * self.size
        return jnp.concatenate([g[start : start + self.size] for g in grads], axis=1)

    def move(self):
        return self.ring.back(self.now[0]), self.ring.ahead(self.now[1])

    def take(self, moved):
        self.left -= 1
        sums = [m.astype(f32) + self.block(side).astype(f32) for side, m in enumerate(moved)]
        self.now = tuple(sums if self.left == 0 else [v.astype(bf16) for v in sums])


class Held:
    def __init__(self, *value):
        self.value = value if len(value) > 1 else value[0]


def turn(lane, other=None, values=(), held=()):
    moved, _, held, lane.buffers = together(
        (lane.move(), other.now if other else (), held, lane.buffers)
    )
    lane.take(moved)
    values, held, _ = together((values, held, lane.now))
    return values, held


class Stages:
    def __init__(self, generator):
        self.generator = generator
        self.result = None
        self.value = ()
        self.over = False
        self.advance(None)

    def advance(self, value):
        if not self.over:
            try:
                self.value = self.generator.send(value)
            except StopIteration as end:
                self.result, self.over, self.value = end.value, True, ()

    def turn(self, lane, other=None, extra=()):
        if isinstance(self.value, Held):
            value = turn(lane, other, (), (self.value.value, extra))[1][0]
        else:
            value = turn(lane, other, self.value, extra)[0]
        self.advance(value)

    def finish(self):
        while not self.over:
            self.advance(self.value.value if isinstance(self.value, Held) else self.value)
        return self.result


def gather_group(ring, rows, before=()):
    across = together((other_tensor(rows), before))[0]
    beside = ring.other_core(rows)
    return jnp.concatenate([rows, across, beside, ring.other_core(across)], axis=0)


def core_sum(ring, parts):
    half = parts.shape[0] // 2
    return parts[:half] + ring.other_core(parts[half:].astype(bf16)).astype(f32)


def tensor_sum(rows):
    half = rows.shape[0] // 2
    return rows[:half] + other_tensor(rows[half:].astype(bf16)).astype(f32)


def scatter_group(ring, parts):
    return tensor_sum(core_sum(ring, parts))


def copy_blocks(table, source, target):
    for k in range(target.shape[1] // LANES):
        start = pl.multiple_of(table[k] * LANES, LANES)
        target[:, k * LANES : (k + 1) * LANES] = source[:, pl.ds(start, LANES)]


def reorder(rows, table):
    height, width = rows.shape
    step = height // 4
    return pl.pallas_call(
        copy_blocks,
        out_shape=jax.ShapeDtypeStruct(rows.shape, rows.dtype),
        grid_spec=pltpu.PrefetchScalarGridSpec(
            num_scalar_prefetch=1,
            grid=(height // step,),
            in_specs=[pl.BlockSpec((step, width), lambda k, t: (k, 0))],
            out_specs=pl.BlockSpec((step, width), lambda k, t: (k, 0)),
        ),
        name="reorder",
    )(table, rows)


def visible(numbers, shape):
    def slot(axis):
        offset = lax.broadcasted_iota(jnp.int32, shape, axis)
        start = numbers[2] * (shape[0] // 2)
        return jnp.where(offset < shape[0] // 2, offset + start, offset - start)

    query, key = slot(0), slot(1)
    inside = query < numbers[pl.program_id(0)]
    return jnp.where(inside, key - query, jnp.abs(key - query)) <= 0


def turned(heads, cosine, sine):
    half = heads.shape[1] // 2
    first, second = heads[:, :half], heads[:, half:]
    return first * cosine - second * sine, second * cosine + first * sine


def weights_of(queries, keys, allowed):
    scores = lax.dot_general(queries, keys, over_last, preferred_element_type=f32)
    scores = jnp.where(allowed, scores * HEAD_SIZE ** (-0.5), -1e30)
    shifted = jnp.exp(scores - jnp.max(scores, axis=-1, keepdims=True))
    return shifted / jnp.sum(shifted, axis=-1, keepdims=True)


def attend_body(numbers, qkv, cosine, sine, queries, keys, values, mixed):
    rows, width = queries.shape
    half = HEAD_SIZE // 2
    cosine, sine = cosine[...], sine[...]
    key_low, key_high = turned(qkv[:, width : width + HEAD_SIZE], cosine, sine)
    keys[:, :half] = key_low.astype(bf16)
    keys[:, half:] = key_high.astype(bf16)
    values[...] = qkv[:, width + HEAD_SIZE :].astype(bf16)
    allowed = visible(numbers, (rows, rows))
    for start in range(0, width, HEAD_SIZE):
        low, high = turned(qkv[:, start : start + HEAD_SIZE], cosine, sine)
        queries[:, start : start + half] = low.astype(bf16)
        queries[:, start + half : start + HEAD_SIZE] = high.astype(bf16)
        probs = weights_of(queries[:, start : start + HEAD_SIZE], keys[...], allowed)
        mixed[:, start : start + HEAD_SIZE] = jnp.dot(
            probs.astype(bf16), values[...], preferred_element_type=f32
        ).astype(bf16)


def attend_back_body(numbers, queries, keys, values, delta, cosine, sine, out):
    rows, width = queries.shape
    half = HEAD_SIZE // 2
    scaling = HEAD_SIZE ** (-0.5)
    cosine, sine = cosine[...], sine[...]
    allowed = visible(numbers, (rows, rows))
    delta_keys = jnp.zeros((rows, HEAD_SIZE), f32)
    delta_values = jnp.zeros((rows, HEAD_SIZE), f32)
    for start in range(0, width, HEAD_SIZE):
        head = queries[:, start : start + HEAD_SIZE]
        delta_mixed = delta[:, start : start + HEAD_SIZE]
        probs = weights_of(head, keys[...], allowed)
        delta_probs = lax.dot_general(
            delta_mixed, values[...], over_last, preferred_element_type=f32
        )
        inner = jnp.sum(probs * delta_probs, axis=-1, keepdims=True)
        delta_scores = (probs * (delta_probs - inner)).astype(bf16)
        delta_values += lax.dot_general(
            probs.astype(bf16), delta_mixed, over_rows, preferred_element_type=f32
        )
        delta_keys += lax.dot_general(delta_scores, head, over_rows, preferred_element_type=f32)
        delta_head = jnp.dot(delta_scores, keys[...], preferred_element_type=f32) * scaling
        low, high = turned(delta_head, cosine, -sine)
        out[:, start : start + half] = low.astype(bf16)
        out[:, start + half : start + HEAD_SIZE] = high.astype(bf16)
    low, high = turned(delta_keys * scaling, cosine, -sine)
    out[:, width : width + half] = low.astype(bf16)
    out[:, width + half : width + HEAD_SIZE] = high.astype(bf16)
    out[:, width + HEAD_SIZE :] = delta_values.astype(bf16)


def by_sequence(body, numbers, arrays, widths, name):
    rows = arrays[0].shape[0] // 2

    def spec(columns):
        return pl.BlockSpec((rows, columns), lambda b, n: (b, 0))

    return pl.pallas_call(
        body,
        out_shape=[jax.ShapeDtypeStruct((2 * rows, w), bf16) for w in widths],
        grid_spec=pltpu.PrefetchScalarGridSpec(
            num_scalar_prefetch=1,
            grid=(2,),
            in_specs=[spec(v.shape[1]) for v in arrays],
            out_specs=[spec(w) for w in widths],
        ),
        name=name,
    )(numbers, *arrays)


def per_device(
    layer_input,
    teacher,
    lengths,
    seq_order,
    gain_attn,
    w_query,
    key_projection_weight,
    value_projection_weight,
    w_out,
    gain_mlp,
    w_gate,
    w_up,
    w_down,
):
    token_rows, width = layer_input.shape
    slots = token_rows * lax.axis_size("tensor")
    devices = lax.axis_size("dp")
    tokens_all = slots * devices
    chips = devices // 2
    ring = Ring(chips)
    me = lax.axis_index("dp")
    side = lax.axis_index("tensor")
    chip, core = me // 2, me % 2
    first_core = core == 0
    place = jnp.array(ring.place, dtype=jnp.int32)
    here = place[chip]
    piece = gain_attn.shape[0]

    numbers = jnp.arange(chips, dtype=jnp.int32)
    order = jnp.array(ring_order(chips), dtype=jnp.int32)
    from_low = 2 * order[(here - numbers) % chips]
    from_high = 2 * order[(here + numbers) % chips] + 1
    half = chips // 2
    to_relative = jnp.concatenate(
        [from_low[half:], from_high[half:], from_low[:half], from_high[:half]]
    )
    behind, before = (here - place) % chips, (place - here) % chips
    to_natural = jnp.stack(
        [
            jnp.where(behind < half, behind + 2 * half, behind - half),
            jnp.where(before < half, before + 3 * half, before),
        ],
        axis=1,
    ).reshape(devices)

    def split_cores(w):
        quarter = w.shape[1] // 2
        mine = lax.dynamic_slice_in_dim(w, core * quarter, quarter, 1)
        given = lax.dynamic_slice_in_dim(w, (1 - core) * quarter, quarter, 1)
        return mine, given

    def both_rows(weights, gains=None):
        mine, given = zip(*[split_cores(w) for w in weights])
        mine, given = jnp.concatenate(mine, axis=1), jnp.concatenate(given, axis=1)
        if gains is not None:
            extra = jnp.pad(gains, ((0, 16 - gains.shape[0]), (0, mine.shape[1] - gains.shape[1])))
            mine = jnp.concatenate([mine, extra], axis=0)
            given = jnp.concatenate([given, extra], axis=0)
        taken = ring.other_core(given)
        return (
            jnp.where(first_core, mine, taken),
            jnp.where(first_core, taken, mine),
        )

    gains = jnp.stack([gain_attn, gain_mlp])
    hops = ring.chips - 1
    q_width = w_query.shape[1] // 2
    kv_width = key_projection_weight.shape[1] // 2
    qkv_width = q_width + 2 * kv_width
    out_width = w_out.shape[0] // 2
    attn_weights = Gather(
        ring,
        "attn_rows",
        *both_rows([w_query, key_projection_weight, value_projection_weight, w_out.T], gains),
        piece,
        [(0, qkv_width), (qkv_width, qkv_width + out_width)],
        below=16,
    )
    w_gate, layer_input, to_relative, lengths, _ = together(
        (w_gate, layer_input, to_relative, lengths, attn_weights.now)
    )
    gate_weights = Gather(ring, "gate_rows", *both_rows([w_gate]), piece)
    own_input = reorder(layer_input, to_relative)
    group_rows = gather_group(ring, own_input)
    for k in range(hops):
        turn(attn_weights, gate_weights)
        if k == hops - 2:
            group_rows = together((group_rows, attn_weights.now))[0]
        turn(gate_weights, attn_weights)
    up_weights = Gather(
        ring, "up_rows", *together((both_rows([w_up]), attn_weights.now))[0], piece
    )
    down_weights = Gather(
        ring, "down_rows", *together((both_rows([w_down.T]), gate_weights.now))[0], piece, split=True
    )

    sequence_numbers = jnp.stack([me, me + 1 - 2 * core])
    length = jnp.sum(
        jnp.where(seq_order[None, :] == sequence_numbers[:, None], lengths[None, :], 0), axis=1
    )
    offsets = jnp.arange(token_rows, dtype=jnp.int32)
    slot = jnp.concatenate([side * token_rows + offsets, (1 - side) * token_rows + offsets])
    inside = slot[None, :] < length[:, None]
    position = jnp.where(inside, slot[None, :], 0)
    own_valid = inside[0, :token_rows].astype(f32)[:, None]
    cosine, sine = rope_tables(position.reshape(-1), HEAD_SIZE)
    numbers = jnp.concatenate([length, side[None]]).astype(jnp.int32)
    own_rows = own_input.astype(f32)
    attn_scale = rms_scale(own_rows)

    qkv_proj, out_proj_t, gain_rows = attn_weights.buffers
    gain_rows = gain_rows[:2].astype(f32)
    attn_gain, mlp_gain = gain_rows[:1], gain_rows[1:]
    gate_proj = gate_weights.buffers[0]

    def forward():
        group_input = group_rows.astype(f32)
        normed = (group_input * rms_scale(group_input) * attn_gain).astype(bf16)
        qkv = jnp.dot(normed, qkv_proj, preferred_element_type=f32)
        normed, qkv = yield Held(normed, qkv)
        attended = by_sequence(
            attend_body,
            numbers,
            [qkv, cosine, sine],
            [q_width, kv_width, kv_width, q_width],
            "attend",
        )
        attended = yield Held(attended)
        parts = lax.dot_general(attended[3], out_proj_t, over_last, preferred_element_type=f32)
        parts = yield Held(parts)
        shared = scatter_group(ring, parts)
        own_teacher = yield Held(reorder(teacher, to_relative))
        yield ()
        shared = yield Held(shared)
        middle = own_rows + shared
        mlp_scale = rms_scale(middle)
        normed_mlp = gather_group(ring, (middle * mlp_scale * mlp_gain).astype(bf16))
        yield ()
        yield ()
        normed_mlp = yield Held(normed_mlp)
        gate = jnp.dot(normed_mlp, gate_proj, preferred_element_type=f32)
        gate = yield Held(gate)
        return (
            own_teacher,
            (normed, *attended),
            (middle, mlp_scale, normed_mlp, gate),
        )

    stages = Stages(forward())
    for k in range(hops):
        stages.turn(up_weights, down_weights)
        if k % 2:
            stages.turn(down_weights, up_weights)
    own_teacher, attn_kept, mlp_kept = stages.finish()
    normed, rot_queries, rot_keys, values, mixed = attn_kept
    middle, mlp_scale, normed_mlp, gate = mlp_kept
    up_proj = up_weights.buffers[0]
    down_near = down_weights.buffers.pop()
    count = jnp.sum(lengths).astype(f32)
    cut = width // 2

    def half_sum(rows, proj_t):
        parts = lax.dot_general(rows, proj_t, over_last, preferred_element_type=f32)
        return core_sum(ring, parts)

    def output(shared, columns):
        result = middle[:, columns] + shared
        error = (result - own_teacher[:, columns].astype(f32)) * own_valid
        delta = error * (tokens_all / count)
        return result, error, delta, delta.astype(bf16)

    def down_grad_of(branch):
        return lax.dot_general(branch, hidden, over_rows, preferred_element_type=f32).astype(bf16)

    def near_half():
        up = jnp.dot(normed_mlp, up_proj, preferred_element_type=f32)
        sigmoid_gate = jax.nn.sigmoid(gate)
        hidden = yield Held((gate * sigmoid_gate * up).astype(bf16))
        half = yield Held(half_sum(hidden, down_near))
        result, error, delta, low = output(tensor_sum(half), slice(cut, width))
        low = yield Held(low)
        across, beside = yield Held(other_tensor(low), ring.other_core(low))
        branch = jnp.concatenate([low, across, beside, ring.other_core(across)], axis=0)
        first = jnp.dot(branch, down_near, preferred_element_type=f32)
        return up, sigmoid_gate, hidden, result, error, delta, branch, first

    stages = Stages(near_half())
    while down_weights.hops < ring.chips:
        stages.turn(down_weights)
    up, sigmoid_gate, hidden, result_near, error_near, delta_near, branch_near, first = (
        stages.finish()
    )
    down_far = down_weights.buffers[0]
    half_far = half_sum(hidden, down_far)
    result_far, error_far, delta_far, low_far = output(tensor_sum(half_far), slice(0, cut))
    branch_far = gather_group(ring, low_far)
    grad_far = down_grad_of(branch_far)
    down_sums = Scatter(ring, [grad_far], None, piece)
    result = jnp.concatenate([result_far, result_near], axis=1)
    delta_result = jnp.concatenate([delta_far, delta_near], axis=1)
    squared = jnp.sum(error_far * error_far) + jnp.sum(error_near * error_near)

    def backward():
        branch, near_part, _ = together((branch_far, first, grad_far))
        delta_hidden = yield Held(
            near_part + jnp.dot(branch, down_far, preferred_element_type=f32)
        )
        delta_gate = (
            delta_hidden * up * sigmoid_gate * (1.0 + gate * (1.0 - sigmoid_gate))
        ).astype(bf16)
        delta_up = (delta_hidden * gate * sigmoid_gate).astype(bf16)
        delta_gate, delta_up = yield Held(delta_gate, delta_up)
        grad_gate = lax.dot_general(
            normed_mlp, delta_gate, over_rows, preferred_element_type=f32
        ).astype(bf16)
        grad_gate, delta_up = yield Held(grad_gate, delta_up)
        grad_up = lax.dot_general(
            normed_mlp, delta_up, over_rows, preferred_element_type=f32
        ).astype(bf16)
        gate_up.extend([grad_gate, grad_up])
        delta_gate, delta_up = yield Held(delta_gate, delta_up)
        def from_hidden(rows):
            return lax.dot_general(
                delta_gate[rows], gate_proj, over_last, preferred_element_type=f32
            ) + lax.dot_general(delta_up[rows], up_proj, over_last, preferred_element_type=f32)

        given, delta_gate, delta_up = yield Held(
            from_hidden(slice(slots, None)).astype(bf16), delta_gate, delta_up
        )
        taken = ring.other_core(given)
        parts = yield Held(from_hidden(slice(0, slots)))
        parts = parts + taken.astype(f32)
        delta_normed_mlp = tensor_sum(parts)
        activations = reorder(together((result.astype(bf16), parts))[0], to_natural)
        yield ()
        delta_normed_mlp, activations = yield Held(delta_normed_mlp, activations)
        gain_mlp_part = jnp.sum(delta_normed_mlp * middle * mlp_scale, axis=0)
        weighted_mlp = mlp_gain * delta_normed_mlp
        delta_middle = (
            delta_result
            + mlp_scale * weighted_mlp
            - middle * mlp_scale**3 * jnp.mean(middle * weighted_mlp, axis=-1, keepdims=True)
        )
        attn_low_rows = gather_group(ring, delta_middle.astype(bf16))
        yield ()
        yield ()
        attn_low_rows = yield Held(attn_low_rows)
        grad_out_t = lax.dot_general(attn_low_rows, mixed, over_rows, preferred_element_type=f32)
        delta_mixed = jnp.dot(attn_low_rows, out_proj_t, preferred_element_type=f32).astype(bf16)
        grad_out_t = grad_out_t.astype(bf16)
        delta_qkv = by_sequence(
            attend_back_body,
            numbers,
            [rot_queries, rot_keys, values, delta_mixed, cosine, sine],
            [qkv_width],
            "attend_back",
        )[0]
        delta_qkv, grad_out_t = yield Held(delta_qkv, grad_out_t)
        grad_qkv = lax.dot_general(normed, delta_qkv, over_rows, preferred_element_type=f32)
        return (
            activations,
            gain_mlp_part,
            delta_middle,
            delta_qkv,
            [jnp.concatenate([grad_qkv.astype(bf16), grad_out_t], axis=1)],
        )

    def finish(sums):
        low, high = sums.now
        kept = jnp.where(first_core, low, high)
        taken = ring.other_core(jnp.where(first_core, high, low).astype(bf16)).astype(f32)
        return kept, taken

    def whole(kept, taken):
        return jnp.concatenate(
            [jnp.where(first_core, kept, taken), jnp.where(first_core, taken, kept)], axis=1
        )

    def halves(grads):
        return [g[: width // 2] for g in grads], [g[width // 2 :] for g in grads]

    gate_up = []
    stages = Stages(backward())
    for k in range(3):
        stages.turn(down_sums)
    gate_up_sums = Scatter(ring, *halves(gate_up), piece)
    grad_near = down_grad_of(together((branch_near, gate_up_sums.now))[0])
    down_sums.parts = ([grad_near], down_sums.parts[1])
    stages.turn(down_sums, gate_up_sums)
    while down_sums.left > 1:
        stages.turn(gate_up_sums, down_sums)
        stages.turn(down_sums, gate_up_sums)
    stages.turn(gate_up_sums, down_sums)
    stages.turn(gate_up_sums, down_sums)
    stages.turn(down_sums, gate_up_sums)
    while not stages.over and gate_up_sums.left:
        stages.turn(gate_up_sums, down_sums)
    assert stages.over
    activations, gain_mlp_part, delta_middle, delta_qkv, attn_grads = stages.finish()
    attn_sums = Scatter(ring, *halves(attn_grads), piece)

    def closing():
        delta_normed = scatter_group(
            ring,
            lax.dot_general(
                together((delta_qkv, attn_sums.now))[0],
                qkv_proj,
                over_last,
                preferred_element_type=f32,
            ),
        )
        yield ()
        yield ()
        yield ()
        delta_normed = yield Held(delta_normed)
        gain_attn_part = jnp.sum(delta_normed * own_rows * attn_scale, axis=0)
        weighted_attn = attn_gain * delta_normed
        input_grad = (
            delta_middle
            + attn_scale * weighted_attn
            - own_rows * attn_scale**3 * jnp.mean(own_rows * weighted_attn, axis=-1, keepdims=True)
        )
        natural = jnp.stack([gain_mlp_part, gain_attn_part], axis=0).reshape(2, devices, piece)[
            :, to_natural
        ]
        sums = jnp.concatenate(
            [natural.reshape(2 * devices, piece), jnp.full((8, piece), squared)], axis=0
        )
        sums, input_grad = yield Held(sums + other_tensor(sums), input_grad.astype(bf16))
        input_grad = reorder(input_grad, to_natural)
        step = 1
        while step < devices:
            pairs = [(d, d ^ step) for d in range(devices)]
            sums, _ = yield Held(sums + lax.ppermute(sums, "dp", pairs), input_grad)
            step *= 2
        return input_grad, sums

    stages = Stages(closing())
    while down_sums.left:
        stages.turn(down_sums, gate_up_sums)
    down_grad = whole(*finish(down_sums)).T
    while gate_up_sums.left:
        stages.turn(gate_up_sums, attn_sums, down_grad)
        stages.turn(attn_sums, gate_up_sums)
    kept, taken = finish(gate_up_sums)
    gate_width = w_gate.shape[1] // 2
    gate_grad = whole(kept[:, :gate_width], taken[:, :gate_width])
    up_grad = whole(kept[:, gate_width:], taken[:, gate_width:])
    stages.turn(attn_sums)
    while attn_sums.left:
        stages.turn(attn_sums, None, (gate_grad, up_grad))
    input_grad, totals = stages.finish()
    gain_mlp_grad = lax.dynamic_slice_in_dim(totals, me, 1, 0)[0]
    gain_attn_grad = lax.dynamic_slice_in_dim(totals, devices + me, 1, 0)[0]
    distill_loss = totals[2 * devices, 0] / (2.0 * width * count)
    attn_kept, attn_taken = finish(attn_sums)
    cuts = [0, q_width, q_width + kv_width, qkv_width, attn_kept.shape[1]]
    query_grad, key_grad, value_grad, out_grad_t = [
        whole(attn_kept[:, a:b], attn_taken[:, a:b]) for a, b in zip(cuts[:-1], cuts[1:])
    ]
    return (
        activations,
        input_grad,
        gain_attn_grad,
        query_grad,
        key_grad,
        value_grad,
        out_grad_t.T,
        gain_mlp_grad,
        gate_grad,
        up_grad,
        down_grad,
        distill_loss,
    )


def solution(mesh):
    placed = (
        P(("dp", "tensor"), None),
        P(("dp", "tensor"), None),
        P(),
        P(),
        P("dp"),
        P("dp", "tensor"),
        P("dp", "tensor"),
        P("dp", "tensor"),
        P("tensor", "dp"),
        P("dp"),
        P("dp", "tensor"),
        P("dp", "tensor"),
        P("tensor", "dp"),
    )
    return jax.shard_map(
        per_device,
        mesh=mesh,
        in_specs=placed,
        out_specs=(
            P(("dp", "tensor"), None),
            P(("dp", "tensor"), None),
            P("dp"),
            P("dp", "tensor"),
            P("dp", "tensor"),
            P("dp", "tensor"),
            P("tensor", "dp"),
            P("dp"),
            P("dp", "tensor"),
            P("dp", "tensor"),
            P("tensor", "dp"),
            P(),
        ),
        check_vma=False,
    )
```

```python
import jax
import jax.numpy as jnp
from jax import lax
from jax.experimental import pallas as pl
from jax.experimental.pallas import tpu as pltpu
from jax.sharding import PartitionSpec as P

HEAD_SIZE = 256
LANES = 128
EPS = 1e-06
ROPE_BASE = 1000042.0
over_rows = (((0,), (0,)), ((), ()))
over_last = (((1,), (1,)), ((), ()))
plain = (((1,), (0,)), ((), ()))
f32 = jnp.float32
bf16 = jnp.bfloat16


def rms_scale(value_rows):
    return lax.rsqrt(jnp.mean(value_rows * value_rows, axis=-1, keepdims=True) + EPS)


def rope_tables(position, width):
    half = width // 2
    exponent = jnp.arange(half, dtype=f32) * (-2.0 / width)
    frequency = jnp.exp(exponent * jnp.log(f32(ROPE_BASE)))
    angle = position.astype(f32)[..., None] * frequency
    return (jnp.cos(angle), jnp.sin(angle))


def ring_order(chips):
    column = chips // 2
    return [2 * i for i in range(column)] + [2 * i + 1 for i in reversed(range(column))]


class Ring:
    def __init__(self, chips):
        self.chips = chips
        order = ring_order(chips)
        self.place = [order.index(c) for c in range(chips)]
        hop = [(order[i], order[(i + 1) % chips]) for i in range(chips)]
        self.up = [(2 * a + c, 2 * b + c) for a, b in hop for c in range(2)]
        self.down = [(b, a) for a, b in self.up]
        self.swap = [(d, d ^ 1) for d in range(2 * chips)]

    def ahead(self, v):
        return lax.ppermute(v, "dp", self.up)

    def back(self, v):
        return lax.ppermute(v, "dp", self.down)

    def other_core(self, v):
        return lax.ppermute(v, "dp", self.swap)


def other_tensor(v):
    return lax.ppermute(v, "tensor", [(0, 1), (1, 0)])


def together(values):
    return lax.optimization_barrier(values)


def unfilled(shape, name):
    return pl.pallas_call(
        lambda out: None,
        out_shape=jax.ShapeDtypeStruct(shape, bf16),
        out_specs=pl.BlockSpec(memory_space=pl.ANY),
        name=name,
    )()


class Gather:
    def __init__(self, ring, name, low, high, rows, cuts=None, split=False, below=0):
        self.ring, self.size, self.split, self.below = ring, rows, split, below
        self.now = (low, high)
        self.cuts = cuts or [(0, low.shape[1])]
        height = 2 * ring.chips * rows
        shapes = [(height, b - a) for a, b in self.cuts]
        if split:
            shapes = [(height // 2, low.shape[1])] * 2
        if below:
            shapes.append((below, height))
        self.buffers = [unfilled(v, f"{name}_{i}") for i, v in enumerate(shapes)]
        self.hops = 0
        self.store()

    def store(self):
        half = self.ring.chips // 2
        k, self.hops = self.hops, self.hops + 1
        for side, rows in enumerate(self.now):
            at = k + (side - 1) * half if k >= half else k + (side + 2) * half
            if self.split:
                which = int(k < half)
                start = (at - which * 2 * half) * self.size
                self.buffers[which] = lax.dynamic_update_slice(
                    self.buffers[which], rows[: self.size], (start, 0)
                )
                continue
            for i, (a, b) in enumerate(self.cuts):
                self.buffers[i] = lax.dynamic_update_slice(
                    self.buffers[i], rows[: self.size, a:b], (at * self.size, 0)
                )
            if self.below:
                self.buffers[-1] = lax.dynamic_update_slice(
                    self.buffers[-1],
                    rows[self.size : self.size + self.below, : self.size],
                    (0, at * self.size),
                )

    def move(self):
        return self.ring.ahead(self.now[0]), self.ring.back(self.now[1])

    def take(self, moved):
        self.now = moved
        self.store()


class Scatter:
    def __init__(self, ring, far, near, rows):
        self.ring, self.parts, self.size = ring, (near, far), rows
        self.buffers = []
        self.left = ring.chips - 1
        self.now = tuple(jnp.concatenate(self.block(side), axis=1) for side in range(2))

    def block(self, side):
        half = self.ring.chips // 2
        grads = self.parts[self.left // half]
        start = (side * half + self.left % half) * self.size
        return [g[start : start + self.size] for g in grads]

    def move(self):
        return self.ring.back(self.now[0]), self.ring.ahead(self.now[1])

    def take(self, moved):
        self.left -= 1
        kind = f32 if self.left == 0 else bf16

        def added(side):
            column, sums = 0, []
            for part in self.block(side):
                taken = moved[side][:, column : column + part.shape[1]]
                sums.append((taken.astype(f32) + part.astype(f32)).astype(kind))
                column += part.shape[1]
            return jnp.concatenate(sums, axis=1)

        self.now = (added(0), added(1))


class Held:
    def __init__(self, *value):
        self.value = value if len(value) > 1 else value[0]


def turn(lane, other=None, values=(), held=()):
    moved, _, held, lane.buffers = together(
        (lane.move(), other.now if other else (), held, lane.buffers)
    )
    lane.take(moved)
    values, held, _ = together((values, held, lane.now))
    return values, held


class Stages:
    def __init__(self, generator):
        self.generator = generator
        self.result = None
        self.value = ()
        self.over = False
        self.advance(None)

    def advance(self, value):
        if not self.over:
            try:
                self.value = self.generator.send(value)
            except StopIteration as end:
                self.result, self.over, self.value = end.value, True, ()

    def turn(self, lane, other=None, extra=()):
        if isinstance(self.value, Held):
            value = turn(lane, other, (), (self.value.value, extra))[1][0]
        else:
            value = turn(lane, other, self.value, extra)[0]
        self.advance(value)

    def finish(self):
        while not self.over:
            self.advance(self.value.value if isinstance(self.value, Held) else self.value)
        return self.result


def gather_group(ring, rows, before=()):
    across = together((other_tensor(rows), before))[0]
    beside = ring.other_core(rows)
    return jnp.concatenate([rows, across, beside, ring.other_core(across)], axis=0)


def core_sum(ring, parts):
    half = parts.shape[0] // 2
    return parts[:half] + ring.other_core(parts[half:].astype(bf16)).astype(f32)


def tensor_sum(rows):
    half = rows.shape[0] // 2
    return rows[:half] + other_tensor(rows[half:].astype(bf16)).astype(f32)


def scatter_group(ring, parts):
    return tensor_sum(core_sum(ring, parts))


def copy_blocks(table, source, target):
    for k in range(target.shape[1] // LANES):
        start = pl.multiple_of(table[k] * LANES, LANES)
        target[:, k * LANES : (k + 1) * LANES] = source[:, pl.ds(start, LANES)]


def reorder(rows, table):
    height, width = rows.shape
    step = height // 4
    return pl.pallas_call(
        copy_blocks,
        out_shape=jax.ShapeDtypeStruct(rows.shape, rows.dtype),
        grid_spec=pltpu.PrefetchScalarGridSpec(
            num_scalar_prefetch=1,
            grid=(height // step,),
            in_specs=[pl.BlockSpec((step, width), lambda k, t: (k, 0))],
            out_specs=pl.BlockSpec((step, width), lambda k, t: (k, 0)),
        ),
        name="reorder",
    )(table, rows)


def visible(numbers, shape):
    def slot(axis):
        offset = lax.broadcasted_iota(jnp.int32, shape, axis)
        start = numbers[2] * (shape[0] // 2)
        return jnp.where(offset < shape[0] // 2, offset + start, offset - start)

    query, key = slot(0), slot(1)
    inside = query < numbers[pl.program_id(0)]
    return jnp.where(inside, key - query, jnp.abs(key - query)) <= 0


def turned(heads, cosine, sine):
    half = heads.shape[1] // 2
    first, second = heads[:, :half], heads[:, half:]
    return first * cosine - second * sine, second * cosine + first * sine


def weights_of(queries, keys, allowed):
    scores = lax.dot_general(queries, keys, over_last, preferred_element_type=f32)
    scores = jnp.where(allowed, scores * HEAD_SIZE ** (-0.5), -1e30)
    shifted = jnp.exp(scores - jnp.max(scores, axis=-1, keepdims=True))
    return shifted / jnp.sum(shifted, axis=-1, keepdims=True)


def attend_body(numbers, qkv, cosine, sine, queries, keys, values, mixed):
    rows, width = queries.shape
    half = HEAD_SIZE // 2
    cosine, sine = cosine[...], sine[...]
    key_low, key_high = turned(qkv[:, width : width + HEAD_SIZE], cosine, sine)
    keys[:, :half] = key_low.astype(bf16)
    keys[:, half:] = key_high.astype(bf16)
    values[...] = qkv[:, width + HEAD_SIZE :].astype(bf16)
    allowed = visible(numbers, (rows, rows))
    for start in range(0, width, HEAD_SIZE):
        low, high = turned(qkv[:, start : start + HEAD_SIZE], cosine, sine)
        queries[:, start : start + half] = low.astype(bf16)
        queries[:, start + half : start + HEAD_SIZE] = high.astype(bf16)
        probs = weights_of(queries[:, start : start + HEAD_SIZE], keys[...], allowed)
        mixed[:, start : start + HEAD_SIZE] = jnp.dot(
            probs.astype(bf16), values[...], preferred_element_type=f32
        ).astype(bf16)


def attend_back_body(numbers, queries, keys, values, delta, cosine, sine, out):
    rows, width = queries.shape
    half = HEAD_SIZE // 2
    scaling = HEAD_SIZE ** (-0.5)
    cosine, sine = cosine[...], sine[...]
    allowed = visible(numbers, (rows, rows))
    delta_keys = jnp.zeros((rows, HEAD_SIZE), f32)
    delta_values = jnp.zeros((rows, HEAD_SIZE), f32)
    for start in range(0, width, HEAD_SIZE):
        head = queries[:, start : start + HEAD_SIZE]
        delta_mixed = delta[:, start : start + HEAD_SIZE]
        probs = weights_of(head, keys[...], allowed)
        delta_probs = lax.dot_general(
            delta_mixed, values[...], over_last, preferred_element_type=f32
        )
        inner = jnp.sum(probs * delta_probs, axis=-1, keepdims=True)
        delta_scores = (probs * (delta_probs - inner)).astype(bf16)
        delta_values += lax.dot_general(
            probs.astype(bf16), delta_mixed, over_rows, preferred_element_type=f32
        )
        delta_keys += lax.dot_general(delta_scores, head, over_rows, preferred_element_type=f32)
        delta_head = jnp.dot(delta_scores, keys[...], preferred_element_type=f32) * scaling
        low, high = turned(delta_head, cosine, -sine)
        out[:, start : start + half] = low.astype(bf16)
        out[:, start + half : start + HEAD_SIZE] = high.astype(bf16)
    low, high = turned(delta_keys * scaling, cosine, -sine)
    out[:, width : width + half] = low.astype(bf16)
    out[:, width + half : width + HEAD_SIZE] = high.astype(bf16)
    out[:, width + HEAD_SIZE :] = delta_values.astype(bf16)


def by_sequence(body, numbers, arrays, widths, name):
    rows = arrays[0].shape[0] // 2

    def spec(columns):
        return pl.BlockSpec((rows, columns), lambda b, n: (b, 0))

    return pl.pallas_call(
        body,
        out_shape=[jax.ShapeDtypeStruct((2 * rows, w), bf16) for w in widths],
        grid_spec=pltpu.PrefetchScalarGridSpec(
            num_scalar_prefetch=1,
            grid=(2,),
            in_specs=[spec(v.shape[1]) for v in arrays],
            out_specs=[spec(w) for w in widths],
        ),
        name=name,
    )(numbers, *arrays)


def per_device(
    layer_input,
    teacher,
    lengths,
    seq_order,
    gain_attn,
    w_query,
    key_projection_weight,
    value_projection_weight,
    w_out,
    gain_mlp,
    w_gate,
    w_up,
    w_down,
):
    token_rows, width = layer_input.shape
    slots = token_rows * lax.axis_size("tensor")
    devices = lax.axis_size("dp")
    tokens_all = slots * devices
    chips = devices // 2
    ring = Ring(chips)
    me = lax.axis_index("dp")
    side = lax.axis_index("tensor")
    chip, core = me // 2, me % 2
    first_core = core == 0
    place = jnp.array(ring.place, dtype=jnp.int32)
    here = place[chip]
    piece = gain_attn.shape[0]

    numbers = jnp.arange(chips, dtype=jnp.int32)
    order = jnp.array(ring_order(chips), dtype=jnp.int32)
    from_low = 2 * order[(here - numbers) % chips]
    from_high = 2 * order[(here + numbers) % chips] + 1
    half = chips // 2
    to_relative = jnp.concatenate(
        [from_low[half:], from_high[half:], from_low[:half], from_high[:half]]
    )
    behind, before = (here - place) % chips, (place - here) % chips
    to_natural = jnp.stack(
        [
            jnp.where(behind < half, behind + 2 * half, behind - half),
            jnp.where(before < half, before + 3 * half, before),
        ],
        axis=1,
    ).reshape(devices)

    def split_cores(w):
        quarter = w.shape[1] // 2
        mine = lax.dynamic_slice_in_dim(w, core * quarter, quarter, 1)
        given = lax.dynamic_slice_in_dim(w, (1 - core) * quarter, quarter, 1)
        return mine, given

    def both_rows(weights, gains=None):
        mine, given = zip(*[split_cores(w) for w in weights])
        mine, given = jnp.concatenate(mine, axis=1), jnp.concatenate(given, axis=1)
        if gains is not None:
            extra = jnp.pad(gains, ((0, 16 - gains.shape[0]), (0, mine.shape[1] - gains.shape[1])))
            mine = jnp.concatenate([mine, extra], axis=0)
            given = jnp.concatenate([given, extra], axis=0)
        taken = ring.other_core(given)
        return (
            jnp.where(first_core, mine, taken),
            jnp.where(first_core, taken, mine),
        )

    gains = jnp.stack([gain_attn, gain_mlp])
    hops = ring.chips - 1
    q_width = w_query.shape[1] // 2
    kv_width = key_projection_weight.shape[1] // 2
    qkv_width = q_width + 2 * kv_width
    out_width = w_out.shape[0] // 2
    attn_weights = Gather(
        ring,
        "attn_rows",
        *both_rows([w_query, key_projection_weight, value_projection_weight, w_out.T], gains),
        piece,
        [(0, qkv_width), (qkv_width, qkv_width + out_width)],
        below=16,
    )
    w_gate, layer_input, to_relative, lengths, _ = together(
        (w_gate, layer_input, to_relative, lengths, attn_weights.now)
    )
    gate_weights = Gather(ring, "gate_rows", *both_rows([w_gate]), piece)
    own_input = reorder(layer_input, to_relative)
    group_rows = gather_group(ring, own_input)
    for k in range(hops):
        turn(attn_weights, gate_weights)
        if k == hops - 2:
            group_rows = together((group_rows, attn_weights.now))[0]
        turn(gate_weights, attn_weights)
    up_weights = Gather(
        ring, "up_rows", *together((both_rows([w_up]), attn_weights.now))[0], piece
    )
    down_weights = Gather(
        ring, "down_rows", *together((both_rows([w_down.T]), gate_weights.now))[0], piece, split=True
    )

    sequence_numbers = jnp.stack([me, me + 1 - 2 * core])
    length = jnp.sum(
        jnp.where(seq_order[None, :] == sequence_numbers[:, None], lengths[None, :], 0), axis=1
    )
    offsets = jnp.arange(token_rows, dtype=jnp.int32)
    slot = jnp.concatenate([side * token_rows + offsets, (1 - side) * token_rows + offsets])
    inside = slot[None, :] < length[:, None]
    position = jnp.where(inside, slot[None, :], 0)
    own_valid = inside[0, :token_rows].astype(f32)[:, None]
    cosine, sine = rope_tables(position.reshape(-1), HEAD_SIZE)
    numbers = jnp.concatenate([length, side[None]]).astype(jnp.int32)
    own_rows = own_input.astype(f32)
    attn_scale = rms_scale(own_rows)

    qkv_proj, out_proj_t, gain_rows = attn_weights.buffers
    gain_rows = gain_rows[:2].astype(f32)
    attn_gain, mlp_gain = gain_rows[:1], gain_rows[1:]
    gate_proj = gate_weights.buffers[0]

    def forward():
        group_input = group_rows.astype(f32)
        normed = (group_input * rms_scale(group_input) * attn_gain).astype(bf16)
        qkv = jnp.dot(normed, qkv_proj, preferred_element_type=f32)
        normed, qkv = yield Held(normed, qkv)
        attended = by_sequence(
            attend_body,
            numbers,
            [qkv, cosine, sine],
            [q_width, kv_width, kv_width, q_width],
            "attend",
        )
        attended = yield Held(attended)
        parts = lax.dot_general(attended[3], out_proj_t, over_last, preferred_element_type=f32)
        parts = yield Held(parts)
        shared = scatter_group(ring, parts)
        own_teacher = yield Held(reorder(teacher, to_relative))
        yield ()
        shared = yield Held(shared)
        middle = own_rows + shared
        mlp_scale = rms_scale(middle)
        normed_mlp = gather_group(ring, (middle * mlp_scale * mlp_gain).astype(bf16))
        yield ()
        yield ()
        normed_mlp = yield Held(normed_mlp)
        gate = jnp.dot(normed_mlp, gate_proj, preferred_element_type=f32)
        gate = yield Held(gate)
        return (
            own_teacher,
            (normed, *attended),
            (middle, mlp_scale, normed_mlp, gate),
        )

    stages = Stages(forward())
    for k in range(hops):
        stages.turn(up_weights, down_weights)
        stages.turn(down_weights, up_weights)
    own_teacher, attn_kept, mlp_kept = stages.finish()
    normed, rot_queries, rot_keys, values, mixed = attn_kept
    middle, mlp_scale, normed_mlp, gate = mlp_kept
    up_proj = up_weights.buffers[0]
    down_far, down_near = down_weights.buffers
    count = jnp.sum(lengths).astype(f32)

    up = jnp.dot(normed_mlp, up_proj, preferred_element_type=f32)
    sigmoid_gate = jax.nn.sigmoid(gate)
    hidden = (gate * sigmoid_gate * up).astype(bf16)
    cut = width // 2

    def half_sum(rows, proj_t):
        parts = lax.dot_general(rows, proj_t, over_last, preferred_element_type=f32)
        return core_sum(ring, parts)

    def output(shared, columns):
        result = middle[:, columns] + shared
        error = (result - own_teacher[:, columns].astype(f32)) * own_valid
        delta = error * (tokens_all / count)
        return result, error, delta, delta.astype(bf16)

    def down_grad_of(branch):
        return lax.dot_general(branch, hidden, over_rows, preferred_element_type=f32).astype(bf16)

    half_far = half_sum(hidden, down_far)
    half_near = half_sum(together((hidden, half_far))[0], down_near)
    result_far, error_far, delta_far, low_far = output(tensor_sum(half_far), slice(0, cut))
    branch_far = gather_group(ring, low_far)
    grad_far = down_grad_of(branch_far)
    shared_near = together((tensor_sum(half_near), low_far))[0]
    result_near, error_near, delta_near, low_near = output(shared_near, slice(cut, width))
    branch_near = gather_group(ring, low_near)
    down_sums = Scatter(ring, [grad_far], None, piece)
    result = jnp.concatenate([result_far, result_near], axis=1)
    delta_result = jnp.concatenate([delta_far, delta_near], axis=1)
    squared = jnp.sum(error_far * error_far) + jnp.sum(error_near * error_near)

    def backward():
        branch = together((branch_far, grad_far))[0]
        first = jnp.dot(branch, down_far, preferred_element_type=f32)
        first = yield Held(first)
        delta_hidden = first + jnp.dot(branch_near, down_near, preferred_element_type=f32)
        delta_gate = (
            delta_hidden * up * sigmoid_gate * (1.0 + gate * (1.0 - sigmoid_gate))
        ).astype(bf16)
        delta_up = (delta_hidden * gate * sigmoid_gate).astype(bf16)
        delta_gate, delta_up = yield Held(delta_gate, delta_up)
        grad_gate = lax.dot_general(
            normed_mlp, delta_gate, over_rows, preferred_element_type=f32
        ).astype(bf16)
        grad_gate, delta_up = yield Held(grad_gate, delta_up)
        grad_up = lax.dot_general(
            normed_mlp, delta_up, over_rows, preferred_element_type=f32
        ).astype(bf16)
        gate_up.extend([grad_gate, grad_up])
        delta_gate, delta_up = yield Held(delta_gate, delta_up)
        def from_hidden(rows):
            return lax.dot_general(
                delta_gate[rows], gate_proj, over_last, preferred_element_type=f32
            ) + lax.dot_general(delta_up[rows], up_proj, over_last, preferred_element_type=f32)

        given, delta_gate, delta_up = yield Held(
            from_hidden(slice(slots, None)).astype(bf16), delta_gate, delta_up
        )
        taken = ring.other_core(given)
        parts = yield Held(from_hidden(slice(0, slots)))
        parts = parts + taken.astype(f32)
        delta_normed_mlp = tensor_sum(parts)
        activations = reorder(together((result.astype(bf16), parts))[0], to_natural)
        yield ()
        delta_normed_mlp, activations = yield Held(delta_normed_mlp, activations)
        gain_mlp_part = jnp.sum(delta_normed_mlp * middle * mlp_scale, axis=0)
        weighted_mlp = mlp_gain * delta_normed_mlp
        delta_middle = (
            delta_result
            + mlp_scale * weighted_mlp
            - middle * mlp_scale**3 * jnp.mean(middle * weighted_mlp, axis=-1, keepdims=True)
        )
        attn_low_rows = gather_group(ring, delta_middle.astype(bf16))
        yield ()
        yield ()
        attn_low_rows = yield Held(attn_low_rows)
        grad_out_t = lax.dot_general(attn_low_rows, mixed, over_rows, preferred_element_type=f32)
        delta_mixed = jnp.dot(attn_low_rows, out_proj_t, preferred_element_type=f32).astype(bf16)
        grad_out_t = grad_out_t.astype(bf16)
        delta_qkv = by_sequence(
            attend_back_body,
            numbers,
            [rot_queries, rot_keys, values, delta_mixed, cosine, sine],
            [qkv_width],
            "attend_back",
        )[0]
        delta_qkv, grad_out_t = yield Held(delta_qkv, grad_out_t)
        grad_qkv = lax.dot_general(normed, delta_qkv, over_rows, preferred_element_type=f32)
        return (
            activations,
            gain_mlp_part,
            delta_middle,
            delta_qkv,
            [jnp.concatenate([grad_qkv.astype(bf16), grad_out_t], axis=1)],
        )

    def finish(sums):
        low, high = sums.now
        kept = jnp.where(first_core, low, high)
        taken = ring.other_core(jnp.where(first_core, high, low).astype(bf16)).astype(f32)
        return kept, taken

    def whole(kept, taken):
        return jnp.concatenate(
            [jnp.where(first_core, kept, taken), jnp.where(first_core, taken, kept)], axis=1
        )

    def halves(grads):
        return [g[: width // 2] for g in grads], [g[width // 2 :] for g in grads]

    gate_up = []
    stages = Stages(backward())
    for k in range(3):
        stages.turn(down_sums)
    gate_up_sums = Scatter(ring, *halves(gate_up), piece)
    grad_near = down_grad_of(together((branch_near, gate_up_sums.now))[0])
    down_sums.parts = ([grad_near], down_sums.parts[1])
    stages.turn(down_sums, gate_up_sums)
    while down_sums.left > 1:
        stages.turn(gate_up_sums, down_sums)
        stages.turn(down_sums, gate_up_sums)
    stages.turn(gate_up_sums, down_sums)
    stages.turn(gate_up_sums, down_sums)
    stages.turn(down_sums, gate_up_sums)
    down_grad = whole(*finish(down_sums)).T
    while not stages.over and gate_up_sums.left:
        stages.turn(gate_up_sums, None, down_grad)
    assert stages.over
    activations, gain_mlp_part, delta_middle, delta_qkv, attn_grads = stages.finish()
    attn_sums = Scatter(ring, *halves(attn_grads), piece)

    def closing():
        delta_normed = scatter_group(
            ring,
            lax.dot_general(
                together((delta_qkv, attn_sums.now))[0],
                qkv_proj,
                over_last,
                preferred_element_type=f32,
            ),
        )
        yield ()
        yield ()
        yield ()
        delta_normed = yield Held(delta_normed)
        gain_attn_part = jnp.sum(delta_normed * own_rows * attn_scale, axis=0)
        weighted_attn = attn_gain * delta_normed
        input_grad = (
            delta_middle
            + attn_scale * weighted_attn
            - own_rows * attn_scale**3 * jnp.mean(own_rows * weighted_attn, axis=-1, keepdims=True)
        )
        natural = jnp.stack([gain_mlp_part, gain_attn_part], axis=0).reshape(2, devices, piece)[
            :, to_natural
        ]
        sums = jnp.concatenate(
            [natural.reshape(2 * devices, piece), jnp.full((8, piece), squared)], axis=0
        )
        sums, input_grad = yield Held(sums + other_tensor(sums), input_grad.astype(bf16))
        input_grad = reorder(input_grad, to_natural)
        step = 1
        while step < devices:
            pairs = [(d, d ^ step) for d in range(devices)]
            sums, _ = yield Held(sums + lax.ppermute(sums, "dp", pairs), input_grad)
            step *= 2
        return input_grad, sums

    stages = Stages(closing())
    while gate_up_sums.left:
        stages.turn(gate_up_sums, attn_sums, down_grad)
        stages.turn(attn_sums, gate_up_sums)
    kept, taken = finish(gate_up_sums)
    gate_width = w_gate.shape[1] // 2
    gate_grad = whole(kept[:, :gate_width], taken[:, :gate_width])
    up_grad = whole(kept[:, gate_width:], taken[:, gate_width:])
    stages.turn(attn_sums)
    while attn_sums.left:
        stages.turn(attn_sums, None, (gate_grad, up_grad))
    input_grad, totals = stages.finish()
    gain_mlp_grad = lax.dynamic_slice_in_dim(totals, me, 1, 0)[0]
    gain_attn_grad = lax.dynamic_slice_in_dim(totals, devices + me, 1, 0)[0]
    distill_loss = totals[2 * devices, 0] / (2.0 * width * count)
    attn_kept, attn_taken = finish(attn_sums)
    cuts = [0, q_width, q_width + kv_width, qkv_width, attn_kept.shape[1]]
    query_grad, key_grad, value_grad, out_grad_t = [
        whole(attn_kept[:, a:b], attn_taken[:, a:b]) for a, b in zip(cuts[:-1], cuts[1:])
    ]
    return (
        activations,
        input_grad,
        gain_attn_grad,
        query_grad,
        key_grad,
        value_grad,
        out_grad_t.T,
        gain_mlp_grad,
        gate_grad,
        up_grad,
        down_grad,
        distill_loss,
    )


def solution(mesh):
    placed = (
        P(("dp", "tensor"), None),
        P(("dp", "tensor"), None),
        P(),
        P(),
        P("dp"),
        P("dp", "tensor"),
        P("dp", "tensor"),
        P("dp", "tensor"),
        P("tensor", "dp"),
        P("dp"),
        P("dp", "tensor"),
        P("dp", "tensor"),
        P("tensor", "dp"),
    )
    return jax.shard_map(
        per_device,
        mesh=mesh,
        in_specs=placed,
        out_specs=(
            P(("dp", "tensor"), None),
            P(("dp", "tensor"), None),
            P("dp"),
            P("dp", "tensor"),
            P("dp", "tensor"),
            P("dp", "tensor"),
            P("tensor", "dp"),
            P("dp"),
            P("dp", "tensor"),
            P("dp", "tensor"),
            P("tensor", "dp"),
            P(),
        ),
        check_vma=False,
    )
```

```python
import jax
import jax.numpy as jnp
from jax import lax
from jax.experimental import pallas as pl
from jax.experimental.pallas import tpu as pltpu
from jax.sharding import PartitionSpec as P

HEAD_SIZE = 256
LANES = 128
EPS = 1e-06
ROPE_BASE = 1000042.0
over_rows = (((0,), (0,)), ((), ()))
over_last = (((1,), (1,)), ((), ()))
plain = (((1,), (0,)), ((), ()))
f32 = jnp.float32
bf16 = jnp.bfloat16


def rms_scale(value_rows):
    return lax.rsqrt(jnp.mean(value_rows * value_rows, axis=-1, keepdims=True) + EPS)


def rope_tables(position, width):
    half = width // 2
    exponent = jnp.arange(half, dtype=f32) * (-2.0 / width)
    frequency = jnp.exp(exponent * jnp.log(f32(ROPE_BASE)))
    angle = position.astype(f32)[..., None] * frequency
    return (jnp.cos(angle), jnp.sin(angle))


def ring_order(chips):
    column = chips // 2
    return [2 * i for i in range(column)] + [2 * i + 1 for i in reversed(range(column))]


class Ring:
    def __init__(self, chips):
        self.chips = chips
        order = ring_order(chips)
        self.place = [order.index(c) for c in range(chips)]
        hop = [(order[i], order[(i + 1) % chips]) for i in range(chips)]
        self.up = [(2 * a + c, 2 * b + c) for a, b in hop for c in range(2)]
        self.down = [(b, a) for a, b in self.up]
        self.swap = [(d, d ^ 1) for d in range(2 * chips)]

    def ahead(self, v):
        return lax.ppermute(v, "dp", self.up)

    def back(self, v):
        return lax.ppermute(v, "dp", self.down)

    def other_core(self, v):
        return lax.ppermute(v, "dp", self.swap)


def other_tensor(v):
    return lax.ppermute(v, "tensor", [(0, 1), (1, 0)])


def together(values):
    return lax.optimization_barrier(values)


def unfilled(shape, name):
    return pl.pallas_call(
        lambda out: None,
        out_shape=jax.ShapeDtypeStruct(shape, bf16),
        out_specs=pl.BlockSpec(memory_space=pl.ANY),
        name=name,
    )()


class Gather:
    def __init__(self, ring, name, low, high, rows, cuts=None, split=False, below=0):
        self.ring, self.size, self.split, self.below = ring, rows, split, below
        self.now = (low, high)
        self.cuts = cuts or [(0, low.shape[1])]
        height = 2 * ring.chips * rows
        shapes = [(height, b - a) for a, b in self.cuts]
        if split:
            shapes = [(height // 2, low.shape[1])] * 2
        if below:
            shapes.append((below, height))
        self.buffers = [unfilled(v, f"{name}_{i}") for i, v in enumerate(shapes)]
        self.hops = 0
        self.store()

    def store(self):
        half = self.ring.chips // 2
        k, self.hops = self.hops, self.hops + 1
        for side, rows in enumerate(self.now):
            at = k + (side - 1) * half if k >= half else k + (side + 2) * half
            if self.split:
                which = int(k < half)
                start = (at - which * 2 * half) * self.size
                self.buffers[which] = lax.dynamic_update_slice(
                    self.buffers[which], rows[: self.size], (start, 0)
                )
                continue
            for i, (a, b) in enumerate(self.cuts):
                self.buffers[i] = lax.dynamic_update_slice(
                    self.buffers[i], rows[: self.size, a:b], (at * self.size, 0)
                )
            if self.below:
                self.buffers[-1] = lax.dynamic_update_slice(
                    self.buffers[-1],
                    rows[self.size : self.size + self.below, : self.size],
                    (0, at * self.size),
                )

    def move(self):
        return self.ring.ahead(self.now[0]), self.ring.back(self.now[1])

    def take(self, moved):
        self.now = moved
        self.store()


class Scatter:
    def __init__(self, ring, far, near, rows):
        self.ring, self.parts, self.size = ring, (near, far), rows
        self.buffers = []
        self.left = ring.chips - 1
        self.now = tuple(jnp.concatenate(self.block(side), axis=1) for side in range(2))

    def block(self, side):
        half = self.ring.chips // 2
        grads = self.parts[self.left // half]
        start = (side * half + self.left % half) * self.size
        return [g[start : start + self.size] for g in grads]

    def move(self):
        return self.ring.back(self.now[0]), self.ring.ahead(self.now[1])

    def take(self, moved):
        self.left -= 1
        kind = f32 if self.left == 0 else bf16

        def added(side):
            column, sums = 0, []
            for part in self.block(side):
                taken = moved[side][:, column : column + part.shape[1]]
                sums.append((taken.astype(f32) + part.astype(f32)).astype(kind))
                column += part.shape[1]
            return jnp.concatenate(sums, axis=1)

        self.now = (added(0), added(1))


class Held:
    def __init__(self, *value):
        self.value = value if len(value) > 1 else value[0]


def turn(lane, other=None, values=(), held=()):
    moved, _, held, lane.buffers = together(
        (lane.move(), other.now if other else (), held, lane.buffers)
    )
    lane.take(moved)
    values, held, _ = together((values, held, lane.now))
    return values, held


class Stages:
    def __init__(self, generator):
        self.generator = generator
        self.result = None
        self.value = ()
        self.over = False
        self.advance(None)

    def advance(self, value):
        if not self.over:
            try:
                self.value = self.generator.send(value)
            except StopIteration as end:
                self.result, self.over, self.value = end.value, True, ()

    def turn(self, lane, other=None, extra=()):
        if isinstance(self.value, Held):
            value = turn(lane, other, (), (self.value.value, extra))[1][0]
        else:
            value = turn(lane, other, self.value, extra)[0]
        self.advance(value)

    def finish(self):
        while not self.over:
            self.advance(self.value.value if isinstance(self.value, Held) else self.value)
        return self.result


def gather_group(ring, rows, before=()):
    across = together((other_tensor(rows), before))[0]
    beside = ring.other_core(rows)
    return jnp.concatenate([rows, across, beside, ring.other_core(across)], axis=0)


def core_sum(ring, parts):
    half = parts.shape[0] // 2
    return parts[:half] + ring.other_core(parts[half:].astype(bf16)).astype(f32)


def tensor_sum(rows):
    half = rows.shape[0] // 2
    return rows[:half] + other_tensor(rows[half:].astype(bf16)).astype(f32)


def scatter_group(ring, parts):
    return tensor_sum(core_sum(ring, parts))


def copy_blocks(table, source, target):
    for k in range(target.shape[1] // LANES):
        start = pl.multiple_of(table[k] * LANES, LANES)
        target[:, k * LANES : (k + 1) * LANES] = source[:, pl.ds(start, LANES)]


def reorder(rows, table):
    height, width = rows.shape
    step = height // 4
    return pl.pallas_call(
        copy_blocks,
        out_shape=jax.ShapeDtypeStruct(rows.shape, rows.dtype),
        grid_spec=pltpu.PrefetchScalarGridSpec(
            num_scalar_prefetch=1,
            grid=(height // step,),
            in_specs=[pl.BlockSpec((step, width), lambda k, t: (k, 0))],
            out_specs=pl.BlockSpec((step, width), lambda k, t: (k, 0)),
        ),
        name="reorder",
    )(table, rows)


def visible(numbers, shape):
    def slot(axis):
        offset = lax.broadcasted_iota(jnp.int32, shape, axis)
        start = numbers[2] * (shape[0] // 2)
        return jnp.where(offset < shape[0] // 2, offset + start, offset - start)

    query, key = slot(0), slot(1)
    inside = query < numbers[pl.program_id(0)]
    return jnp.where(inside, key - query, jnp.abs(key - query)) <= 0


def turned(heads, cosine, sine):
    half = heads.shape[1] // 2
    first, second = heads[:, :half], heads[:, half:]
    return first * cosine - second * sine, second * cosine + first * sine


def weights_of(queries, keys, allowed):
    scores = lax.dot_general(queries, keys, over_last, preferred_element_type=f32)
    scores = jnp.where(allowed, scores * HEAD_SIZE ** (-0.5), -1e30)
    shifted = jnp.exp(scores - jnp.max(scores, axis=-1, keepdims=True))
    return shifted / jnp.sum(shifted, axis=-1, keepdims=True)


def attend_body(numbers, qkv, cosine, sine, queries, keys, values, mixed):
    rows, width = queries.shape
    half = HEAD_SIZE // 2
    cosine, sine = cosine[...], sine[...]
    key_low, key_high = turned(qkv[:, width : width + HEAD_SIZE], cosine, sine)
    keys[:, :half] = key_low.astype(bf16)
    keys[:, half:] = key_high.astype(bf16)
    values[...] = qkv[:, width + HEAD_SIZE :].astype(bf16)
    allowed = visible(numbers, (rows, rows))
    for start in range(0, width, HEAD_SIZE):
        low, high = turned(qkv[:, start : start + HEAD_SIZE], cosine, sine)
        queries[:, start : start + half] = low.astype(bf16)
        queries[:, start + half : start + HEAD_SIZE] = high.astype(bf16)
        probs = weights_of(queries[:, start : start + HEAD_SIZE], keys[...], allowed)
        mixed[:, start : start + HEAD_SIZE] = jnp.dot(
            probs.astype(bf16), values[...], preferred_element_type=f32
        ).astype(bf16)


def attend_back_body(numbers, queries, keys, values, delta, cosine, sine, out):
    rows, width = queries.shape
    half = HEAD_SIZE // 2
    scaling = HEAD_SIZE ** (-0.5)
    cosine, sine = cosine[...], sine[...]
    allowed = visible(numbers, (rows, rows))
    delta_keys = jnp.zeros((rows, HEAD_SIZE), f32)
    delta_values = jnp.zeros((rows, HEAD_SIZE), f32)
    for start in range(0, width, HEAD_SIZE):
        head = queries[:, start : start + HEAD_SIZE]
        delta_mixed = delta[:, start : start + HEAD_SIZE]
        probs = weights_of(head, keys[...], allowed)
        delta_probs = lax.dot_general(
            delta_mixed, values[...], over_last, preferred_element_type=f32
        )
        inner = jnp.sum(probs * delta_probs, axis=-1, keepdims=True)
        delta_scores = (probs * (delta_probs - inner)).astype(bf16)
        delta_values += lax.dot_general(
            probs.astype(bf16), delta_mixed, over_rows, preferred_element_type=f32
        )
        delta_keys += lax.dot_general(delta_scores, head, over_rows, preferred_element_type=f32)
        delta_head = jnp.dot(delta_scores, keys[...], preferred_element_type=f32) * scaling
        low, high = turned(delta_head, cosine, -sine)
        out[:, start : start + half] = low.astype(bf16)
        out[:, start + half : start + HEAD_SIZE] = high.astype(bf16)
    low, high = turned(delta_keys * scaling, cosine, -sine)
    out[:, width : width + half] = low.astype(bf16)
    out[:, width + half : width + HEAD_SIZE] = high.astype(bf16)
    out[:, width + HEAD_SIZE :] = delta_values.astype(bf16)


def by_sequence(body, numbers, arrays, widths, name):
    rows = arrays[0].shape[0] // 2

    def spec(columns):
        return pl.BlockSpec((rows, columns), lambda b, n: (b, 0))

    return pl.pallas_call(
        body,
        out_shape=[jax.ShapeDtypeStruct((2 * rows, w), bf16) for w in widths],
        grid_spec=pltpu.PrefetchScalarGridSpec(
            num_scalar_prefetch=1,
            grid=(2,),
            in_specs=[spec(v.shape[1]) for v in arrays],
            out_specs=[spec(w) for w in widths],
        ),
        name=name,
    )(numbers, *arrays)


def per_device(
    layer_input,
    teacher,
    lengths,
    seq_order,
    gain_attn,
    w_query,
    key_projection_weight,
    value_projection_weight,
    w_out,
    gain_mlp,
    w_gate,
    w_up,
    w_down,
):
    token_rows, width = layer_input.shape
    slots = token_rows * lax.axis_size("tensor")
    devices = lax.axis_size("dp")
    tokens_all = slots * devices
    chips = devices // 2
    ring = Ring(chips)
    me = lax.axis_index("dp")
    side = lax.axis_index("tensor")
    chip, core = me // 2, me % 2
    first_core = core == 0
    place = jnp.array(ring.place, dtype=jnp.int32)
    here = place[chip]
    piece = gain_attn.shape[0]

    numbers = jnp.arange(chips, dtype=jnp.int32)
    order = jnp.array(ring_order(chips), dtype=jnp.int32)
    from_low = 2 * order[(here - numbers) % chips]
    from_high = 2 * order[(here + numbers) % chips] + 1
    half = chips // 2
    to_relative = jnp.concatenate(
        [from_low[half:], from_high[half:], from_low[:half], from_high[:half]]
    )
    behind, before = (here - place) % chips, (place - here) % chips
    to_natural = jnp.stack(
        [
            jnp.where(behind < half, behind + 2 * half, behind - half),
            jnp.where(before < half, before + 3 * half, before),
        ],
        axis=1,
    ).reshape(devices)

    def split_cores(w):
        quarter = w.shape[1] // 2
        mine = lax.dynamic_slice_in_dim(w, core * quarter, quarter, 1)
        given = lax.dynamic_slice_in_dim(w, (1 - core) * quarter, quarter, 1)
        return mine, given

    def both_rows(weights, gains=None):
        mine, given = zip(*[split_cores(w) for w in weights])
        mine, given = jnp.concatenate(mine, axis=1), jnp.concatenate(given, axis=1)
        if gains is not None:
            extra = jnp.pad(gains, ((0, 16 - gains.shape[0]), (0, mine.shape[1] - gains.shape[1])))
            mine = jnp.concatenate([mine, extra], axis=0)
            given = jnp.concatenate([given, extra], axis=0)
        taken = ring.other_core(given)
        return (
            jnp.where(first_core, mine, taken),
            jnp.where(first_core, taken, mine),
        )

    gains = jnp.stack([gain_attn, gain_mlp])
    hops = ring.chips - 1
    q_width = w_query.shape[1] // 2
    kv_width = key_projection_weight.shape[1] // 2
    qkv_width = q_width + 2 * kv_width
    out_width = w_out.shape[0] // 2
    attn_weights = Gather(
        ring,
        "attn_rows",
        *both_rows([w_query, key_projection_weight, value_projection_weight, w_out.T], gains),
        piece,
        [(0, qkv_width), (qkv_width, qkv_width + out_width)],
        below=16,
    )
    w_gate, layer_input, to_relative, lengths, _ = together(
        (w_gate, layer_input, to_relative, lengths, attn_weights.now)
    )
    gate_weights = Gather(ring, "gate_rows", *both_rows([w_gate]), piece)
    own_input = reorder(layer_input, to_relative)
    group_rows = gather_group(ring, own_input)
    for k in range(hops):
        turn(attn_weights, gate_weights)
        if k == hops - 2:
            group_rows = together((group_rows, attn_weights.now))[0]
        turn(gate_weights, attn_weights)
    up_weights = Gather(
        ring, "up_rows", *together((both_rows([w_up]), attn_weights.now))[0], piece
    )
    down_weights = Gather(
        ring, "down_rows", *together((both_rows([w_down.T]), gate_weights.now))[0], piece, split=True
    )

    sequence_numbers = jnp.stack([me, me + 1 - 2 * core])
    length = jnp.sum(
        jnp.where(seq_order[None, :] == sequence_numbers[:, None], lengths[None, :], 0), axis=1
    )
    offsets = jnp.arange(token_rows, dtype=jnp.int32)
    slot = jnp.concatenate([side * token_rows + offsets, (1 - side) * token_rows + offsets])
    inside = slot[None, :] < length[:, None]
    position = jnp.where(inside, slot[None, :], 0)
    own_valid = inside[0, :token_rows].astype(f32)[:, None]
    cosine, sine = rope_tables(position.reshape(-1), HEAD_SIZE)
    numbers = jnp.concatenate([length, side[None]]).astype(jnp.int32)
    own_rows = own_input.astype(f32)
    attn_scale = rms_scale(own_rows)

    qkv_proj, out_proj_t, gain_rows = attn_weights.buffers
    gain_rows = gain_rows[:2].astype(f32)
    attn_gain, mlp_gain = gain_rows[:1], gain_rows[1:]
    gate_proj = gate_weights.buffers[0]

    def forward():
        group_input = group_rows.astype(f32)
        normed = (group_input * rms_scale(group_input) * attn_gain).astype(bf16)
        qkv = jnp.dot(normed, qkv_proj, preferred_element_type=f32)
        normed, qkv = yield Held(normed, qkv)
        attended = by_sequence(
            attend_body,
            numbers,
            [qkv, cosine, sine],
            [q_width, kv_width, kv_width, q_width],
            "attend",
        )
        attended = yield Held(attended)
        parts = lax.dot_general(attended[3], out_proj_t, over_last, preferred_element_type=f32)
        parts = yield Held(parts)
        shared = scatter_group(ring, parts)
        own_teacher = yield Held(reorder(teacher, to_relative))
        yield ()
        shared = yield Held(shared)
        middle = own_rows + shared
        mlp_scale = rms_scale(middle)
        normed_mlp = gather_group(ring, (middle * mlp_scale * mlp_gain).astype(bf16))
        yield ()
        yield ()
        normed_mlp = yield Held(normed_mlp)
        gate = jnp.dot(normed_mlp, gate_proj, preferred_element_type=f32)
        gate = yield Held(gate)
        return (
            own_teacher,
            (normed, *attended),
            (middle, mlp_scale, normed_mlp, gate),
        )

    stages = Stages(forward())
    for k in range(hops):
        stages.turn(up_weights, down_weights)
        stages.turn(down_weights, up_weights)
    own_teacher, attn_kept, mlp_kept = stages.finish()
    normed, rot_queries, rot_keys, values, mixed = attn_kept
    middle, mlp_scale, normed_mlp, gate = mlp_kept
    up_proj = up_weights.buffers[0]
    down_far, down_near = down_weights.buffers
    count = jnp.sum(lengths).astype(f32)

    up = jnp.dot(normed_mlp, up_proj, preferred_element_type=f32)
    sigmoid_gate = jax.nn.sigmoid(gate)
    hidden = (gate * sigmoid_gate * up).astype(bf16)
    cut = width // 2

    def half_sum(rows, proj_t):
        parts = lax.dot_general(rows, proj_t, over_last, preferred_element_type=f32)
        return core_sum(ring, parts)

    def output(shared, columns):
        result = middle[:, columns] + shared
        error = (result - own_teacher[:, columns].astype(f32)) * own_valid
        delta = error * (tokens_all / count)
        return result, error, delta, delta.astype(bf16)

    def down_grad_of(branch):
        return lax.dot_general(branch, hidden, over_rows, preferred_element_type=f32).astype(bf16)

    half_far = half_sum(hidden, down_far)
    half_near = half_sum(together((hidden, half_far))[0], down_near)
    result_far, error_far, delta_far, low_far = output(tensor_sum(half_far), slice(0, cut))
    branch_far = gather_group(ring, low_far)
    grad_far = down_grad_of(branch_far)
    shared_near = together((tensor_sum(half_near), low_far))[0]
    result_near, error_near, delta_near, low_near = output(shared_near, slice(cut, width))
    branch_near = gather_group(ring, low_near)
    down_sums = Scatter(ring, [grad_far], None, piece)
    result = jnp.concatenate([result_far, result_near], axis=1)
    delta_result = jnp.concatenate([delta_far, delta_near], axis=1)
    squared = jnp.sum(error_far * error_far) + jnp.sum(error_near * error_near)

    def backward():
        branch = together((branch_far, grad_far))[0]
        first = jnp.dot(branch, down_far, preferred_element_type=f32)
        first = yield Held(first)
        delta_hidden = first + jnp.dot(branch_near, down_near, preferred_element_type=f32)
        delta_gate = (
            delta_hidden * up * sigmoid_gate * (1.0 + gate * (1.0 - sigmoid_gate))
        ).astype(bf16)
        delta_up = (delta_hidden * gate * sigmoid_gate).astype(bf16)
        delta_gate, delta_up = yield Held(delta_gate, delta_up)
        grad_gate = lax.dot_general(
            normed_mlp, delta_gate, over_rows, preferred_element_type=f32
        ).astype(bf16)
        grad_gate, delta_up = yield Held(grad_gate, delta_up)
        grad_up = lax.dot_general(
            normed_mlp, delta_up, over_rows, preferred_element_type=f32
        ).astype(bf16)
        gate_up.extend([grad_gate, grad_up])
        delta_gate, delta_up = yield Held(delta_gate, delta_up)
        def from_hidden(rows):
            return lax.dot_general(
                delta_gate[rows], gate_proj, over_last, preferred_element_type=f32
            ) + lax.dot_general(delta_up[rows], up_proj, over_last, preferred_element_type=f32)

        given, delta_gate, delta_up = yield Held(
            from_hidden(slice(slots, None)).astype(bf16), delta_gate, delta_up
        )
        taken = ring.other_core(given)
        parts = yield Held(from_hidden(slice(0, slots)))
        parts = parts + taken.astype(f32)
        delta_normed_mlp = tensor_sum(parts)
        activations = reorder(together((result.astype(bf16), parts))[0], to_natural)
        yield ()
        delta_normed_mlp, activations = yield Held(delta_normed_mlp, activations)
        gain_mlp_part = jnp.sum(delta_normed_mlp * middle * mlp_scale, axis=0)
        weighted_mlp = mlp_gain * delta_normed_mlp
        delta_middle = (
            delta_result
            + mlp_scale * weighted_mlp
            - middle * mlp_scale**3 * jnp.mean(middle * weighted_mlp, axis=-1, keepdims=True)
        )
        attn_low_rows = gather_group(ring, delta_middle.astype(bf16))
        yield ()
        yield ()
        attn_low_rows = yield Held(attn_low_rows)
        grad_out_t = lax.dot_general(attn_low_rows, mixed, over_rows, preferred_element_type=f32)
        delta_mixed = jnp.dot(attn_low_rows, out_proj_t, preferred_element_type=f32).astype(bf16)
        grad_out_t = grad_out_t.astype(bf16)
        delta_qkv = by_sequence(
            attend_back_body,
            numbers,
            [rot_queries, rot_keys, values, delta_mixed, cosine, sine],
            [qkv_width],
            "attend_back",
        )[0]
        delta_qkv, grad_out_t = yield Held(delta_qkv, grad_out_t)
        grad_qkv = lax.dot_general(normed, delta_qkv, over_rows, preferred_element_type=f32)
        return (
            activations,
            gain_mlp_part,
            delta_middle,
            delta_qkv,
            [jnp.concatenate([grad_qkv.astype(bf16), grad_out_t], axis=1)],
        )

    def finish(sums):
        low, high = sums.now
        kept = jnp.where(first_core, low, high)
        taken = ring.other_core(jnp.where(first_core, high, low).astype(bf16)).astype(f32)
        return kept, taken

    def whole(kept, taken):
        return jnp.concatenate(
            [jnp.where(first_core, kept, taken), jnp.where(first_core, taken, kept)], axis=1
        )

    def halves(grads):
        return [g[: width // 2] for g in grads], [g[width // 2 :] for g in grads]

    gate_up = []
    stages = Stages(backward())
    for k in range(3):
        stages.turn(down_sums)
    gate_up_sums = Scatter(ring, *halves(gate_up), piece)
    grad_near = down_grad_of(together((branch_near, gate_up_sums.now))[0])
    down_sums.parts = ([grad_near], down_sums.parts[1])
    stages.turn(down_sums, gate_up_sums)
    while down_sums.left > 1:
        stages.turn(gate_up_sums, down_sums)
        stages.turn(down_sums, gate_up_sums)
    stages.turn(gate_up_sums, down_sums)
    stages.turn(gate_up_sums, down_sums)
    stages.turn(down_sums, gate_up_sums)
    down_grad = whole(*finish(down_sums)).T
    while not stages.over and gate_up_sums.left:
        stages.turn(gate_up_sums, None, down_grad)
    assert stages.over
    activations, gain_mlp_part, delta_middle, delta_qkv, attn_grads = stages.finish()
    attn_sums = Scatter(ring, *halves(attn_grads), piece)

    def closing():
        delta_normed = scatter_group(
            ring,
            lax.dot_general(
                together((delta_qkv, attn_sums.now))[0],
                qkv_proj,
                over_last,
                preferred_element_type=f32,
            ),
        )
        yield ()
        yield ()
        yield ()
        delta_normed = yield Held(delta_normed)
        gain_attn_part = jnp.sum(delta_normed * own_rows * attn_scale, axis=0)
        weighted_attn = attn_gain * delta_normed
        input_grad = (
            delta_middle
            + attn_scale * weighted_attn
            - own_rows * attn_scale**3 * jnp.mean(own_rows * weighted_attn, axis=-1, keepdims=True)
        )
        natural = jnp.stack([gain_mlp_part, gain_attn_part], axis=0).reshape(2, devices, piece)[
            :, to_natural
        ]
        sums = jnp.concatenate(
            [natural.reshape(2 * devices, piece), jnp.full((8, piece), squared)], axis=0
        )
        sums, input_grad = yield Held(sums + other_tensor(sums), input_grad.astype(bf16))
        input_grad = reorder(input_grad, to_natural)
        step = 1
        while step < devices:
            pairs = [(d, d ^ step) for d in range(devices)]
            sums, _ = yield Held(sums + lax.ppermute(sums, "dp", pairs), input_grad)
            step *= 2
        return input_grad, sums

    stages = Stages(closing())
    while gate_up_sums.left:
        stages.turn(gate_up_sums, attn_sums, down_grad)
        stages.turn(attn_sums, gate_up_sums)
    kept, taken = finish(gate_up_sums)
    gate_width = w_gate.shape[1] // 2
    gate_grad = whole(kept[:, :gate_width], taken[:, :gate_width])
    up_grad = whole(kept[:, gate_width:], taken[:, gate_width:])
    stages.turn(attn_sums)
    stages.turn(attn_sums)
    finished = [gate_grad, up_grad]
    while attn_sums.left:
        stages.turn(attn_sums, None, finished.pop(0) if finished else ())
    input_grad, totals = stages.finish()
    gain_mlp_grad = lax.dynamic_slice_in_dim(totals, me, 1, 0)[0]
    gain_attn_grad = lax.dynamic_slice_in_dim(totals, devices + me, 1, 0)[0]
    distill_loss = totals[2 * devices, 0] / (2.0 * width * count)
    attn_kept, attn_taken = finish(attn_sums)
    cuts = [0, q_width, q_width + kv_width, qkv_width, attn_kept.shape[1]]
    query_grad, key_grad, value_grad, out_grad_t = [
        whole(attn_kept[:, a:b], attn_taken[:, a:b]) for a, b in zip(cuts[:-1], cuts[1:])
    ]
    return (
        activations,
        input_grad,
        gain_attn_grad,
        query_grad,
        key_grad,
        value_grad,
        out_grad_t.T,
        gain_mlp_grad,
        gate_grad,
        up_grad,
        down_grad,
        distill_loss,
    )


def solution(mesh):
    placed = (
        P(("dp", "tensor"), None),
        P(("dp", "tensor"), None),
        P(),
        P(),
        P("dp"),
        P("dp", "tensor"),
        P("dp", "tensor"),
        P("dp", "tensor"),
        P("tensor", "dp"),
        P("dp"),
        P("dp", "tensor"),
        P("dp", "tensor"),
        P("tensor", "dp"),
    )
    return jax.shard_map(
        per_device,
        mesh=mesh,
        in_specs=placed,
        out_specs=(
            P(("dp", "tensor"), None),
            P(("dp", "tensor"), None),
            P("dp"),
            P("dp", "tensor"),
            P("dp", "tensor"),
            P("dp", "tensor"),
            P("tensor", "dp"),
            P("dp"),
            P("dp", "tensor"),
            P("dp", "tensor"),
            P("tensor", "dp"),
            P(),
        ),
        check_vma=False,
    )
```
